8 devices in a mesh: dp: 2 (over z, y), tp: 4 (over x, core).
Axes of the slice: x: 2, y: 2, z: 1, core: 2. Of those that a mesh axis runs over, the one named last changes fastest.
Arguments:
- hidden: bfloat16 [12, 1024, 2048], P('dp', 'tp'), parts along dimension 0
- grad_out: bfloat16 [12, 1024, 2048], P('dp', 'tp'), parts along dimension 0
- prefix_len: int32 [12], P('dp'), parts along dimension 0
- valid_len: int32 [12], P('dp'), parts along dimension 0
- attn_norm: bfloat16 [2048], replicated
- w_query: bfloat16 [2048, 2048], P(None, 'tp')
- w_key: bfloat16 [2048, 256], replicated
- w_value: bfloat16 [2048, 256], replicated
- w_out: bfloat16 [2048, 2048], P('tp')
- mlp_norm: bfloat16 [2048], replicated
- w_gate: bfloat16 [2048, 16384], P(None, 'tp')
- w_up: bfloat16 [2048, 16384], P(None, 'tp')
- w_down: bfloat16 [16384, 2048], P('tp')
Outputs:
- output 1: bfloat16 [12, 1024, 2048], P('dp', 'tp'), parts along dimension 0
- output 2: bfloat16 [12, 1024, 2048], P('dp', 'tp'), parts along dimension 0
- output 3: float32 [4096], P('dp'), parts along dimension 0
- output 4: float32 [4096, 2048], P('dp', 'tp'), parts along dimension 0
- output 5: float32 [4096, 256], P('dp'), parts along dimension 0
- output 6: float32 [4096, 256], P('dp'), parts along dimension 0
- output 7: float32 [4096, 2048], P(('dp', 'tp')), parts along dimension 0
- output 8: float32 [4096], P('dp'), parts along dimension 0
- output 9: float32 [4096, 16384], P('dp', 'tp'), parts along dimension 0
- output 10: float32 [4096, 16384], P('dp', 'tp'), parts along dimension 0
- output 11: float32 [32768, 2048], P(('dp', 'tp')), parts along dimension 0
There are 2 independent parts. The reference program is written for one: setup_inputs(seed, part) draws one part's arguments, and reference() takes and returns one part's arrays. A program takes and returns all parts, laid end to end along the dimension named above; an argument that names none is the same for every part.
All inputs are finite; a program needn't handle non-finite values.
Results may differ from the reference program's by a relative error of at most 0.02.
Values are sent between devices in bfloat16 or wider.
A program may use at most 1 GiB of HBM per device.

```python
import math
import jax
import jax.numpy as jnp
from jax import lax

BATCH_SIZE = 6
SEQ_LEN = 1024
MODEL_DIM = 2048
NUM_HEADS = 8
HEAD_DIM = 256
FFN_DIM = 16384


def rms_norm(x_in, gain):
    x_f = x_in.astype(jnp.float32)
    inv_rms = lax.rsqrt(jnp.mean(x_f * x_f, axis=-1, keepdims=True) + 1e-6)
    return (x_f * inv_rms * (1.0 + gain.astype(jnp.float32))).astype(jnp.bfloat16)


def rope_tables(positions, head_dim):
    half_dim = head_dim // 2
    exponent = jnp.arange(half_dim, dtype=jnp.float32) * (2.0 / head_dim)
    inv_freq = jnp.exp(exponent * (-math.log(10000.0)))
    angles = positions.astype(jnp.float32)[:, None] * inv_freq[None, :]
    return jnp.cos(angles), jnp.sin(angles)


def apply_rope(x_f, cos_t, sin_t):
    half_dim = x_f.shape[-1] // 2
    first = x_f[..., :half_dim]
    second = x_f[..., half_dim:]
    return jnp.concatenate([first * cos_t - second * sin_t, second * cos_t + first * sin_t], axis=-1)


def attend_one(operands):
    query, keys, values, prefix_count, valid_count = operands
    seq_len = query.shape[0]
    scale = query.shape[-1] ** -0.5
    scores = jnp.einsum("qhd,kd->hqk", query.astype(jnp.float32), keys.astype(jnp.float32)) * scale
    q_pos = jnp.arange(seq_len)[:, None]
    k_pos = jnp.arange(seq_len)[None, :]
    visible = (k_pos < valid_count) & ((k_pos < prefix_count) | (k_pos <= q_pos))
    scores = jnp.where(visible[None], scores, -1e30)
    probs = jax.nn.softmax(scores, axis=-1).astype(jnp.bfloat16)
    mixed = jnp.einsum("hqk,kd->qhd", probs.astype(jnp.float32), values.astype(jnp.float32))
    return mixed.astype(jnp.bfloat16)


def layer_forward(hidden, prefix_len, valid_len, weights):
    attn_norm, w_query, w_key, w_value, w_out, mlp_norm, w_gate, w_up, w_down = weights
    batch, seq_len, model_dim = hidden.shape
    head_dim = w_key.shape[1]
    num_heads = w_query.shape[1] // head_dim
    num_rows = batch * seq_len
    normed = rms_norm(hidden, attn_norm).reshape(num_rows, model_dim)
    cos_t, sin_t = rope_tables(jnp.arange(seq_len), head_dim)
    q_raw = jnp.dot(normed, w_query, preferred_element_type=jnp.float32).reshape(batch, seq_len, num_heads, head_dim)
    query = apply_rope(q_raw, cos_t[:, None, :], sin_t[:, None, :]).astype(jnp.bfloat16)
    k_raw = jnp.dot(normed, w_key, preferred_element_type=jnp.float32).reshape(batch, seq_len, head_dim)
    keys = apply_rope(k_raw, cos_t, sin_t).astype(jnp.bfloat16)
    values = jnp.dot(normed, w_value, preferred_element_type=jnp.float32).astype(jnp.bfloat16).reshape(batch, seq_len, head_dim)
    mixed = lax.map(jax.checkpoint(attend_one), (query, keys, values, prefix_len, valid_len))
    attn_out = jnp.dot(mixed.reshape(num_rows, num_heads * head_dim), w_out, preferred_element_type=jnp.float32)
    resid = (hidden.astype(jnp.float32) + attn_out.reshape(batch, seq_len, model_dim)).astype(jnp.bfloat16)
    gated_in = rms_norm(resid, mlp_norm).reshape(num_rows, model_dim)
    gate = jnp.dot(gated_in, w_gate, preferred_element_type=jnp.float32)
    upper = jnp.dot(gated_in, w_up, preferred_element_type=jnp.float32)
    act = (jax.nn.gelu(gate, approximate=True) * upper).astype(jnp.bfloat16)
    mlp_out = jnp.dot(act, w_down, preferred_element_type=jnp.float32)
    return (resid.astype(jnp.float32) + mlp_out.reshape(batch, seq_len, model_dim)).astype(jnp.bfloat16)


def setup_inputs(seed: int = 0, part: int = 0) -> dict:
    base_key = jax.random.key(seed)
    part_keys = jax.random.split(jax.random.fold_in(base_key, part), 4)
    shared_keys = jax.random.split(base_key, 9)
    q_dim = NUM_HEADS * HEAD_DIM
    act_shape = (BATCH_SIZE, SEQ_LEN, MODEL_DIM)
    hidden = (0.25 * jax.random.normal(part_keys[0], act_shape, jnp.float32)).astype(jnp.bfloat16)
    grad_out = jax.random.normal(part_keys[1], act_shape, jnp.float32).astype(jnp.bfloat16)
    valid_len = jax.random.randint(part_keys[2], (BATCH_SIZE,), (3 * SEQ_LEN) // 4, SEQ_LEN + 1, dtype=jnp.int32)
    valid_len = valid_len.at[0].set(SEQ_LEN)
    prefix_len = jax.random.randint(part_keys[3], (BATCH_SIZE,), SEQ_LEN // 8, (3 * SEQ_LEN) // 4 + 1, dtype=jnp.int32)
    in_scale = 1.0 / math.sqrt(MODEL_DIM)
    out_scale = math.sqrt(SEQ_LEN / (64.0 * q_dim))
    down_scale = 1.0 / math.sqrt(FFN_DIM)
    attn_norm = (0.3 * jax.random.normal(shared_keys[0], (MODEL_DIM,), jnp.float32)).astype(jnp.bfloat16)
    w_query = (in_scale * jax.random.normal(shared_keys[1], (MODEL_DIM, q_dim), jnp.float32)).astype(jnp.bfloat16)
    w_key = (in_scale * jax.random.normal(shared_keys[2], (MODEL_DIM, HEAD_DIM), jnp.float32)).astype(jnp.bfloat16)
    w_value = (in_scale * jax.random.normal(shared_keys[3], (MODEL_DIM, HEAD_DIM), jnp.float32)).astype(jnp.bfloat16)
    w_out = (out_scale * jax.random.normal(shared_keys[4], (q_dim, MODEL_DIM), jnp.float32)).astype(jnp.bfloat16)
    mlp_norm = (0.3 * jax.random.normal(shared_keys[5], (MODEL_DIM,), jnp.float32)).astype(jnp.bfloat16)
    w_gate = (in_scale * jax.random.normal(shared_keys[6], (MODEL_DIM, FFN_DIM), jnp.float32)).astype(jnp.bfloat16)
    w_up = (in_scale * jax.random.normal(shared_keys[7], (MODEL_DIM, FFN_DIM), jnp.float32)).astype(jnp.bfloat16)
    w_down = (down_scale * jax.random.normal(shared_keys[8], (FFN_DIM, MODEL_DIM), jnp.float32)).astype(jnp.bfloat16)
    return {"hidden": hidden, "grad_out": grad_out, "prefix_len": prefix_len, "valid_len": valid_len, "attn_norm": attn_norm, "w_query": w_query, "w_key": w_key, "w_value": w_value, "w_out": w_out, "mlp_norm": mlp_norm, "w_gate": w_gate, "w_up": w_up, "w_down": w_down}


def reference(hidden, grad_out, prefix_len, valid_len, attn_norm, w_query, w_key, w_value, w_out, mlp_norm, w_gate, w_up, w_down):
    weights = (attn_norm, w_query, w_key, w_value, w_out, mlp_norm, w_gate, w_up, w_down)

    def forward(hidden_in, weights_in):
        return layer_forward(hidden_in, prefix_len, valid_len, weights_in)

    hidden_out, pullback = jax.vjp(forward, hidden, weights)
    grad_hidden, grad_weights = pullback(grad_out)
    g_attn_norm, g_query, g_key, g_value, g_out, g_mlp_norm, g_gate, g_up, g_down = grad_weights
    return (hidden_out, grad_hidden, g_attn_norm.astype(jnp.float32), g_query.astype(jnp.float32), g_key.astype(jnp.float32), g_value.astype(jnp.float32), g_out.astype(jnp.float32), g_mlp_norm.astype(jnp.float32), g_gate.astype(jnp.float32), g_up.astype(jnp.float32), g_down.astype(jnp.float32))
```

```python
import functools
import math

import jax
import jax.numpy as jnp
from jax import lax
from jax.experimental import pallas as pl
from jax.experimental.pallas import tpu as pltpu
from jax.sharding import PartitionSpec as P

EPS = 1e-6
BF = jnp.bfloat16
F32 = jnp.float32
MIB = 1024 * 1024
ANY = pl.BlockSpec(memory_space=pl.ANY)


def dot_nn(a, b):
    return lax.dot_general(a, b, (((1,), (0,)), ((), ())), preferred_element_type=F32)


def dot_nt(a, b):
    return lax.dot_general(a, b, (((1,), (1,)), ((), ())), preferred_element_type=F32)


def dot_tn(a, b):
    return lax.dot_general(a, b, (((0,), (0,)), ((), ())), preferred_element_type=F32)


def const_spec(shape):
    zeros = (0,) * len(shape)
    return pl.BlockSpec(shape, lambda *_: zeros, pipeline_mode=pl.Buffered(1))


def run(kernel, name, grid, in_specs, out_specs, out_shape, args, scratch=(), prefetch=0, aliases=None, flops=0, nbytes=0, limit=60):
    spec = pltpu.PrefetchScalarGridSpec(num_scalar_prefetch=prefetch, grid=grid, in_specs=in_specs, out_specs=out_specs, scratch_shapes=scratch)
    return pl.pallas_call(
        kernel,
        name=name,
        grid_spec=spec,
        out_shape=out_shape,
        input_output_aliases=aliases or {},
        compiler_params=pltpu.CompilerParams(dimension_semantics=("arbitrary",) * len(grid), vmem_limit_bytes=limit * MIB),
        cost_estimate=pl.CostEstimate(flops=int(flops), bytes_accessed=int(nbytes), transcendentals=0),
    )(*args)


def rope_fwd(x, cos_t, sin_t):
    half = x.shape[-1] // 2
    a, b = x[:, :half], x[:, half:]
    return a * cos_t - b * sin_t, b * cos_t + a * sin_t


def rope_bwd(a, b, cos_t, sin_t):
    return a * cos_t + b * sin_t, b * cos_t - a * sin_t


def pre_kernel(h_ref, gain_ref, wk_ref, wv_ref, cos_ref, sin_ref, u_ref, kv_ref):
    x = h_ref[0].astype(F32)
    inv = lax.rsqrt(jnp.mean(x * x, axis=-1, keepdims=True) + EPS)
    u = (x * inv * gain_ref[...]).astype(BF)
    u_ref[0] = u
    hd = wk_ref.shape[1]
    first, second = rope_fwd(dot_nn(u, wk_ref[...]), cos_ref[...], sin_ref[...])
    kv_ref[0, :, : hd // 2] = first.astype(BF)
    kv_ref[0, :, hd // 2 : hd] = second.astype(BF)
    kv_ref[0, :, hd:] = dot_nn(u, wv_ref[...]).astype(BF)


def attn_fwd_kernel(meta_ref, u_ref, wq_ref, kv_ref, cos_ref, sin_ref, token_ref, q_ref, pt_ref, mix_ref, vt_ref, s_ref):
    b = pl.program_id(0)
    tp_n, _, cols = wq_ref.shape
    hd = kv_ref.shape[-1] // 2
    seq = kv_ref.shape[0] * kv_ref.shape[2]
    sl = u_ref.shape[1]
    heads = tp_n * cols // hd
    u = u_ref[0]
    cos_t, sin_t = cos_ref[...], sin_ref[...]
    keys = kv_ref[:, 0, :, :hd].reshape(seq, hd)
    vt_ref[...] = kv_ref[:, 0, :, hd:].reshape(seq, hd).astype(F32).T.astype(BF)
    for s in range(tp_n):
        qs = dot_nn(u, wq_ref[s])
        for j in range(cols // hd):
            base = (s * (cols // hd) + j) * hd
            first, second = rope_fwd(qs[:, j * hd : (j + 1) * hd], cos_t, sin_t)
            q_ref[0, :, base : base + hd // 2] = first.astype(BF)
            q_ref[0, :, base + hd // 2 : base + hd] = second.astype(BF)
    prefix, valid = meta_ref[4 + b], meta_ref[4 + pl.num_programs(0) + b]
    q_end = lax.broadcasted_iota(jnp.int32, (1, sl), 1) + (meta_ref[2] * sl + 1)
    limit = jnp.minimum(valid, jnp.maximum(prefix, q_end))
    visible = lax.broadcasted_iota(jnp.int32, (seq, sl), 0) < limit
    scale = (hd**-0.5) * math.log2(math.e)

    def scores(h):
        return dot_nt(keys, q_ref[0, :, h * hd : (h + 1) * hd])

    s_ref[0] = scores(0)
    for h in range(heads):
        if h + 1 < heads:
            s_ref[(h + 1) % 2] = scores(h + 1)
        sc = jnp.where(visible, s_ref[h % 2], -1e30)
        top = jnp.max(sc, axis=0, keepdims=True)
        e = jnp.exp2((sc - top) * scale)
        p = (e * (1.0 / jnp.sum(e, axis=0, keepdims=True))).astype(BF)
        pt_ref[0, :, h * sl : (h + 1) * sl] = p
        mix_ref[0, :, h * hd : (h + 1) * hd] = dot_nn(vt_ref[...], p).T.astype(BF)


def out_kernel(mix_ref, wo_ref, h_ref, gain_ref, resid_ref, z0_ref, z1_ref):
    b = pl.program_id(0)
    half = pl.num_programs(0) // 2
    x = (h_ref[0].astype(F32) + dot_nn(mix_ref[0], wo_ref[...])).astype(BF)
    resid_ref[0] = x
    x = x.astype(F32)
    inv = lax.rsqrt(jnp.mean(x * x, axis=-1, keepdims=True) + EPS)
    z = (x * inv * gain_ref[...]).astype(BF)

    @pl.when(b < half)
    def _():
        z0_ref[0] = z

    @pl.when(b >= half)
    def _():
        z1_ref[0] = z


def dact_kernel(meta_ref, ga_ref, gb_ref, wd_ref, *rest):
    da_ref, cat_ref = rest[-2:]
    core = meta_ref[1]
    rows = ga_ref.shape[0] * ga_ref.shape[1]
    dim = ga_ref.shape[2]
    for rel, ref in enumerate((ga_ref, gb_ref)):
        da_ref[rel] = dot_nt(ref[...].reshape(rows, dim), wd_ref[...]).astype(BF)

    @pl.when(pl.program_id(0) == 0)
    def _():
        cat_ref[0, core] = ga_ref[...].reshape(rows, dim)
        cat_ref[0, 1 - core] = gb_ref[...].reshape(rows, dim)


def mlp_kernel(meta_ref, za_ref, zb_ref, da_ref, wg_ref, wu_ref, *rest):
    act_ref, dg_ref, du_ref, cat_ref = rest[-4:]
    core = meta_ref[1]
    rows = za_ref.shape[0] * za_ref.shape[1]
    dim = za_ref.shape[2]
    step = rows // 2
    c0 = math.sqrt(2.0 / math.pi)
    c1 = c0 * 0.044715
    for rel, ref in enumerate((za_ref, zb_ref)):
        place = core if rel == 0 else 1 - core
        z = ref[...].reshape(rows, dim)
        for r in range(0, rows, step):
            zr = z[r : r + step]
            gate = dot_nn(zr, wg_ref[...])
            up = dot_nn(zr, wu_ref[...])
            da = da_ref[rel, r : r + step, :].astype(F32)
            x2 = gate * gate
            t = jnp.tanh(gate * (c0 + c1 * x2))
            hh = 0.5 + 0.5 * t
            gelu = gate * hh
            slope = hh + gelu * ((1.0 - hh) * (2.0 * c0 + 6.0 * c1 * x2))
            act_ref[0, place, r : r + step, :] = (gelu * up).astype(BF)
            du_ref[0, place, r : r + step, :] = (da * gelu).astype(BF)
            dg_ref[0, place, r : r + step, :] = (da * up * slope).astype(BF)

    @pl.when(pl.program_id(0) == 0)
    def _():
        cat_ref[0, core] = za_ref[...].reshape(rows, dim)
        cat_ref[0, 1 - core] = zb_ref[...].reshape(rows, dim)


def attn_bwd_kernel(dz0_ref, dz1_ref, res_ref, go_ref, gain_ref, wo_ref, kv_ref, q_ref, pt_ref, cos_ref, sin_ref,
                    dres_ref, dq_ref, dkv_ref, gn_ref, kt_ref, do_ref, qs_ref, ds_ref, dp_ref):
    b = pl.program_id(0)
    half = pl.num_programs(0) // 2
    hd = kv_ref.shape[-1] // 2
    seq = kv_ref.shape[0] * kv_ref.shape[2]
    sl = q_ref.shape[1]
    heads = q_ref.shape[2] // hd
    x = res_ref[0].astype(F32)
    dz = jnp.where(b < half, dz0_ref[0], dz1_ref[0]).astype(F32)
    inv = lax.rsqrt(jnp.mean(x * x, axis=-1, keepdims=True) + EPS)
    xn = x * inv
    part = jnp.sum(dz * xn, axis=0, keepdims=True)

    @pl.when(b == 0)
    def _():
        gn_ref[...] = part

    @pl.when(b > 0)
    def _():
        gn_ref[...] += part

    dxn = dz * gain_ref[...]
    dx = inv * (dxn - xn * jnp.mean(dxn * xn, axis=-1, keepdims=True))
    dres = (go_ref[0].astype(F32) + dx).astype(BF)
    dres_ref[0] = dres
    keys = kv_ref[:, 0, :, :hd].reshape(seq, hd)
    vals = kv_ref[:, 0, :, hd:].reshape(seq, hd)
    kt_ref[...] = keys.astype(F32).T.astype(BF)
    for h in range(heads):
        do_ref[h * sl : (h + 1) * sl, :] = dot_nt(dres, wo_ref[h * hd : (h + 1) * hd, :]).astype(BF)
        qs_ref[h * sl : (h + 1) * sl, :] = q_ref[0, :, h * hd : (h + 1) * hd]
    scale = hd**-0.5
    cos_t, sin_t = cos_ref[...], sin_ref[...]

    def dprobs(h):
        return dot_nt(vals, do_ref[h * sl : (h + 1) * sl, :])

    dp_ref[0] = dprobs(0)
    for h in range(heads):
        if h + 1 < heads:
            dp_ref[(h + 1) % 2] = dprobs(h + 1)
        p = pt_ref[0, :, h * sl : (h + 1) * sl].astype(F32)
        t = p * dp_ref[h % 2]
        ds = ((t - p * jnp.sum(t, axis=0, keepdims=True)) * scale).astype(BF)
        ds_ref[:, h * sl : (h + 1) * sl] = ds
        dq = dot_nn(kt_ref[...], ds).T
        first, second = rope_bwd(dq[:, : hd // 2], dq[:, hd // 2 :], cos_t, sin_t)
        dq_ref[0, :, h * hd : h * hd + hd // 2] = first.astype(BF)
        dq_ref[0, :, h * hd + hd // 2 : (h + 1) * hd] = second.astype(BF)
    shape = (kv_ref.shape[0], kv_ref.shape[2], hd)
    dkv_ref[:, 0, :, :hd] = dot_nn(ds_ref[...], qs_ref[...]).astype(BF).reshape(shape)
    dkv_ref[:, 0, :, hd:] = dot_nn(pt_ref[0], do_ref[...]).astype(BF).reshape(shape)


def last_kernel(dkv_ref, dq_ref, u_ref, h_ref, dres_ref, gain_ref, wq_ref, wk_ref, wv_ref, cos_ref, sin_ref, gm_ref,
                gh_ref, gkv_ref, acc_ref):
    b = pl.program_id(0)
    tp_n, dim, cols = wq_ref.shape
    hd = wk_ref.shape[1]
    raw = dkv_ref[0]
    dk = raw[:, :hd].astype(F32)
    first, second = rope_bwd(dk[:, : hd // 2], dk[:, hd // 2 :], cos_ref[...], sin_ref[...])
    dk = jnp.concatenate([first, second], axis=1).astype(BF)
    dv = raw[:, hd:]
    dn = dot_nt(dk, wk_ref[...]) + dot_nt(dv, wv_ref[...])
    for s in range(tp_n):
        dn = dn + dot_nt(dq_ref[0, :, s * cols : (s + 1) * cols], wq_ref[s])
    x = h_ref[0].astype(F32)
    inv = lax.rsqrt(jnp.mean(x * x, axis=-1, keepdims=True) + EPS)
    xn = x * inv
    part = jnp.sum(dn * xn, axis=0, keepdims=True)
    dxn = dn * gain_ref[...]
    dx = inv * (dxn - xn * jnp.mean(dxn * xn, axis=-1, keepdims=True))
    gh_ref[0] = (dres_ref[0].astype(F32) + dx).astype(BF)
    gk = dot_tn(u_ref[0], jnp.concatenate([dk, dv], axis=1))

    @pl.when(b == 0)
    def _():
        acc_ref[...] = part
        gkv_ref[:dim, :] = gk

    @pl.when(b > 0)
    def _():
        acc_ref[...] += part
        gkv_ref[:dim, :] += gk

    @pl.when(b == pl.num_programs(0) - 1)
    def _():
        width = 2 * hd
        per = dim // width
        for i in range(per):
            gkv_ref[dim + i : dim + i + 1, :] = gm_ref[:, i * width : (i + 1) * width]
            gkv_ref[dim + per + i : dim + per + i + 1, :] = acc_ref[:, i * width : (i + 1) * width]


def wgrad_kernel(x_ref, y_ref, o_ref):
    o_ref[0] = dot_tn(x_ref[...], y_ref[...])


def tie_kernel(x_ref, *rest):
    del x_ref, rest


def tie(x, *tokens):
    return pl.pallas_call(
        tie_kernel,
        name="tie",
        in_specs=[ANY] * (1 + len(tokens)),
        out_specs=ANY,
        out_shape=jax.ShapeDtypeStruct(x.shape, x.dtype),
        input_output_aliases={0: 0},
    )(x, *tokens)


def solution(mesh):
    act_spec = P("dp", "tp", None)
    in_specs = (act_spec, act_spec, P("dp"), P("dp"), P(None), P(None, "tp"), P(None, None), P(None, None), P("tp", None), P(None), P(None, "tp"), P(None, "tp"), P("tp", None))
    out_specs = (act_spec, act_spec, P("dp"), P("dp", "tp"), P("dp", None), P("dp", None), P(("dp", "tp"), None), P("dp"), P("dp", "tp"), P("dp", "tp"), P(("dp", "tp"), None))
    core_flip = [(0, 1), (1, 0), (2, 3), (3, 2)]
    chip_flip = [(0, 2), (2, 0), (1, 3), (3, 1)]

    def to_core(x):
        return lax.ppermute(x, "tp", core_flip)

    def to_chip(x):
        return lax.ppermute(x, "tp", chip_flip)

    def local_layer(hidden, grad_out, prefix_len, valid_len, attn_norm, w_query, w_key, w_value, w_out, mlp_norm, w_gate, w_up, w_down):
        batch, sl, dim = hidden.shape
        half = batch // 2
        rows = half * sl
        hd = w_key.shape[1]
        cols = w_query.shape[1]
        tp_n = mesh.shape["tp"]
        seq = sl * tp_n
        qd = cols * tp_n
        heads = qd // hd
        ffn = w_gate.shape[1]
        me = lax.axis_index("tp")
        chip, core = me // 2, me % 2
        meta_me = jnp.stack([chip, core, me, me]).astype(jnp.int32)
        meta = jnp.concatenate([meta_me, prefix_len, valid_len])
        meta_mine = meta
        meta_other = jnp.concatenate([jnp.stack([1 - chip, core, me, me]).astype(jnp.int32), prefix_len, valid_len])

        exponent = jnp.arange(hd // 2, dtype=F32) * (2.0 / hd)
        inv_freq = jnp.exp(exponent * (-math.log(10000.0)))
        angles = (me * sl + jnp.arange(sl)).astype(F32)[:, None] * inv_freq[None, :]
        cos_t, sin_t = jnp.cos(angles), jnp.sin(angles)
        gain1 = (1.0 + attn_norm.astype(F32)).reshape(1, dim)
        gain2 = (1.0 + mlp_norm.astype(F32)).reshape(1, dim)

        def sds(shape, dtype=BF):
            return jax.ShapeDtypeStruct(shape, dtype)

        tok_spec = pl.BlockSpec((1, sl, dim), lambda b, *_: (b, 0, 0))
        rope_spec = const_spec((sl, hd // 2))
        gain_spec = const_spec((1, dim))
        own = batch * sl

        wq4 = lax.all_gather(w_query, "tp", axis=0)
        u, kv = run(
            pre_kernel, "pre", (batch,),
            [tok_spec, gain_spec, const_spec((dim, hd)), const_spec((dim, hd)), rope_spec, rope_spec],
            [tok_spec, pl.BlockSpec((1, sl, 2 * hd), lambda b: (b, 0, 0))],
            [sds((batch, sl, dim)), sds((batch, sl, 2 * hd))],
            (hidden, gain1, w_key, w_value, cos_t, sin_t),
            flops=4 * own * dim * hd, nbytes=6 * own * dim)
        kv4 = lax.all_gather(kv, "tp", axis=0)
        wo_all = lax.all_gather(w_out, "tp", axis=0, tiled=True)

        g_mate = to_core(grad_out)
        half_spec = lambda c: pl.BlockSpec((half, sl, dim), lambda n, m: (c, 0, 0), pipeline_mode=pl.Buffered(1))
        bn = 512
        cat_spec = pl.BlockSpec((1, 2, rows, dim), lambda n, m: (m[0], 0, 0, 0), pipeline_mode=pl.Buffered(1))

        def dact(meta_in, ga, gb, c, prev, token):
            extra = [prev] if prev is not None else []
            tokens = [token] if token is not None else []
            return run(
                dact_kernel, "dact", (ffn // bn,),
                [half_spec(c), half_spec(c), pl.BlockSpec((bn, dim), lambda n, m: (n, 0))] + [ANY] * len(extra + tokens),
                [pl.BlockSpec((2, rows, bn), lambda n, m: (0, 0, n)), cat_spec],
                [sds((2, rows, ffn)), sds((2, 2, rows, dim))],
                (meta_in, ga, gb, w_down, *extra, *tokens),
                prefetch=1, aliases={4: 1} if extra else None,
                flops=4 * rows * dim * ffn, nbytes=2 * ffn * dim)

        fb = 256

        def mlp(meta_in, za, zb, da, prev, token):
            extra = list(prev) if prev is not None else []
            tokens = [token] if token is not None else []
            z_spec = pl.BlockSpec((half, sl, dim), lambda n, m: (0, 0, 0), pipeline_mode=pl.Buffered(1))
            w_spec = pl.BlockSpec((dim, fb), lambda n, m: (0, n))
            o_spec = pl.BlockSpec((1, 2, rows, fb), lambda n, m: (m[0], 0, 0, n))
            return run(
                mlp_kernel, "mlp", (ffn // fb,),
                [z_spec, z_spec, pl.BlockSpec((2, rows, fb), lambda n, m: (0, 0, n)), w_spec, w_spec] + [ANY] * len(extra + tokens),
                [o_spec, o_spec, o_spec, cat_spec],
                [sds((2, 2, rows, ffn))] * 3 + [sds((2, 2, rows, dim))],
                (meta_in, za, zb, da, w_gate, w_up, *extra, *tokens),
                prefetch=1, aliases={6 + i: i for i in range(4)} if extra else None,
                flops=8 * rows * dim * ffn, nbytes=4 * ffn * dim + 16 * rows * ffn)

        da_m0, gcat0 = dact(meta_mine, grad_out, g_mate, 0, None, kv)
        da_m1, gcat1 = dact(meta_mine, grad_out, g_mate, 1, None, da_m0)

        q, pt, mixed = run(
            attn_fwd_kernel, "attn_fwd", (batch,),
            [tok_spec, const_spec((tp_n, dim, cols)), pl.BlockSpec((tp_n, 1, sl, 2 * hd), lambda b, m: (0, b, 0, 0)), rope_spec, rope_spec, ANY],
            [pl.BlockSpec((1, sl, qd), lambda b, m: (b, 0, 0)), pl.BlockSpec((1, seq, heads * sl), lambda b, m: (b, 0, 0)), pl.BlockSpec((1, sl, qd), lambda b, m: (b, 0, 0))],
            [sds((batch, sl, qd)), sds((batch, seq, heads * sl)), sds((batch, sl, qd))],
            (meta, u, wq4, kv4, cos_t, sin_t, da_m1),
            scratch=[pltpu.VMEM((hd, seq), BF), pltpu.VMEM((2, seq, sl), F32)], prefetch=1,
            flops=2 * own * dim * qd + 4 * own * seq * qd, nbytes=2 * own * heads * seq)

        go_halves = [tie(grad_out[c * half : (c + 1) * half], kv4) for c in range(2)]
        g_far = [to_chip(go_halves[c]) for c in range(2)]
        g_far_mate = [to_core(x) for x in g_far]

        resid, z0, z1 = run(
            out_kernel, "out_proj", (batch,),
            [pl.BlockSpec((1, sl, qd), lambda b: (b, 0, 0)), const_spec((qd, dim)), tok_spec, gain_spec],
            [tok_spec, pl.BlockSpec((1, sl, dim), lambda b: (jnp.minimum(b, half - 1), 0, 0)), pl.BlockSpec((1, sl, dim), lambda b: (jnp.maximum(b - half, 0), 0, 0))],
            [sds((batch, sl, dim)), sds((half, sl, dim)), sds((half, sl, dim))],
            (mixed, wo_all, hidden, gain2),
            flops=2 * own * dim * qd, nbytes=8 * own * dim)
        zs = [z0, z1]
        z_mate = [to_core(z) for z in zs]
        z_far = [to_chip(z) for z in zs]
        z_far_mate = [to_core(z) for z in z_far]

        own0 = mlp(meta_mine, zs[0], z_mate[0], da_m0, None, None)
        own1 = mlp(meta_mine, zs[1], z_mate[1], da_m1, None, own0[0])

        def backward_half(full):
            act, dg, du, _ = full
            flat = (4 * rows, ffn)
            d_gated = (dot_nt(dg.reshape(flat), w_gate) + dot_nt(du.reshape(flat), w_up)).astype(BF)
            d_gated = lax.psum_scatter(d_gated.reshape(tp_n, rows, dim), "tp", scatter_dimension=0)
            part = dot_nn(act.reshape(flat), w_down).astype(BF)
            part = lax.psum_scatter(part.reshape(tp_n, rows, dim), "tp", scatter_dimension=0)
            return d_gated.reshape(half, sl, dim), part.reshape(half, sl, dim)

        da_o0, gcat0 = dact(meta_other, g_far[0], g_far_mate[0], 0, gcat0, own1[0])
        full0 = mlp(meta_other, z_far[0], z_far_mate[0], da_o0, own0, None)
        dz0, part0 = backward_half(full0)
        da_o1, gcat1 = dact(meta_other, g_far[1], g_far_mate[1], 0, gcat1, full0[3])
        full1 = mlp(meta_other, z_far[1], z_far_mate[1], da_o1, own1, None)
        dz1, part1 = backward_half(full1)
        hidden_out = (resid.astype(F32) + jnp.concatenate([part0, part1]).astype(F32)).astype(BF)

        d_resid, d_q, dkv_part, gn2 = run(
            attn_bwd_kernel, "attn_bwd", (batch,),
            [pl.BlockSpec((1, sl, dim), lambda b: (jnp.minimum(b, half - 1), 0, 0)), pl.BlockSpec((1, sl, dim), lambda b: (jnp.maximum(b - half, 0), 0, 0)),
             tok_spec, tok_spec, gain_spec, const_spec((qd, dim)), pl.BlockSpec((tp_n, 1, sl, 2 * hd), lambda b: (0, b, 0, 0)),
             pl.BlockSpec((1, sl, qd), lambda b: (b, 0, 0)), pl.BlockSpec((1, seq, heads * sl), lambda b: (b, 0, 0)), rope_spec, rope_spec],
            [tok_spec, pl.BlockSpec((1, sl, qd), lambda b: (b, 0, 0)), pl.BlockSpec((tp_n, 1, sl, 2 * hd), lambda b: (0, b, 0, 0)), pl.BlockSpec((1, dim), lambda b: (0, 0))],
            [sds((batch, sl, dim)), sds((batch, sl, qd)), sds((tp_n, batch, sl, 2 * hd)), sds((1, dim), F32)],
            (dz0, dz1, resid, grad_out, gain2, wo_all, kv4, q, pt, cos_t, sin_t),
            scratch=[pltpu.VMEM((hd, seq), BF), pltpu.VMEM((heads * sl, hd), BF), pltpu.VMEM((heads * sl, hd), BF), pltpu.VMEM((seq, heads * sl), BF), pltpu.VMEM((2, seq, sl), F32)],
            flops=2 * own * dim * qd + 8 * own * seq * qd, nbytes=2 * own * heads * seq)
        dkv = lax.psum_scatter(dkv_part, "tp", scatter_dimension=0)

        def wgrad(x, y, bm, by, name):
            m, n = x.shape[1], y.shape[1]
            return run(
                wgrad_kernel, name, (n // by, m // bm),
                [pl.BlockSpec((own, bm), lambda j, i: (0, i)), pl.BlockSpec((own, by), lambda j, i: (0, j))],
                pl.BlockSpec((1, bm, by), lambda j, i: (j, i, 0)), sds((n // by, m, by), F32), (x, y),
                flops=2 * own * m * n, nbytes=4 * m * n)

        g_out = dot_tn(mixed.reshape(own, qd), d_resid.reshape(own, dim))
        g_out = lax.psum_scatter(g_out, "tp", scatter_dimension=0, tiled=True)
        g_query = wgrad(u.reshape(own, dim), d_q.reshape(own, qd), 512, cols, "wgrad_query")
        g_query = lax.psum_scatter(g_query, "tp", scatter_dimension=0)

        extra = 2 * dim // (2 * hd)
        grad_hidden, gkv = run(
            last_kernel, "last", (batch,),
            [pl.BlockSpec((1, sl, 2 * hd), lambda b: (b, 0, 0)), pl.BlockSpec((1, sl, qd), lambda b: (b, 0, 0)), tok_spec, tok_spec, tok_spec, gain_spec,
             const_spec((tp_n, dim, cols)), const_spec((dim, hd)), const_spec((dim, hd)), rope_spec, rope_spec, const_spec((1, dim))],
            [tok_spec, pl.BlockSpec((dim + extra, 2 * hd), lambda b: (0, 0))],
            [sds((batch, sl, dim)), sds((dim + extra, 2 * hd), F32)],
            (dkv, d_q, u, hidden, d_resid, gain1, wq4, w_key, w_value, cos_t, sin_t, gn2),
            scratch=[pltpu.VMEM((1, dim), F32)],
            flops=2 * own * dim * (qd + 4 * hd), nbytes=8 * own * dim)
        gkv = lax.psum(gkv, "tp")
        g_key, g_value = gkv[:dim, :hd], gkv[:dim, hd:]
        g_mlp_norm = gkv[dim : dim + extra // 2].reshape(dim)
        g_attn_norm = gkv[dim + extra // 2 :].reshape(dim)

        def weight_grad(lhs, rhs):
            return sum(dot_tn(a.reshape(4 * rows, -1), b.reshape(4 * rows, -1)) for a, b in zip(lhs, rhs))

        g_down = weight_grad((full0[0], full1[0]), (gcat0, gcat1))
        g_gate = weight_grad((full0[3], full1[3]), (full0[1], full1[1]))
        g_up = weight_grad((full0[3], full1[3]), (full0[2], full1[2]))
        return (hidden_out, grad_hidden, g_attn_norm, g_query, g_key, g_value, g_out, g_mlp_norm, g_gate, g_up, g_down)

    return jax.shard_map(local_layer, mesh=mesh, in_specs=in_specs, out_specs=out_specs, check_vma=False)
```

```python
import functools
import math

import jax
import jax.numpy as jnp
import numpy as np
from jax import lax
from jax.experimental import pallas as pl
from jax.experimental.pallas import tpu as pltpu
from jax.sharding import PartitionSpec as P


EPS = 1e-6
BF = jnp.bfloat16
F32 = jnp.float32
MIB = 1024 * 1024
ANY = pl.BlockSpec(memory_space=pl.ANY)


def dot_nn(a, b):
    return lax.dot_general(a, b, (((1,), (0,)), ((), ())), preferred_element_type=F32)


def dot_nt(a, b):
    return lax.dot_general(a, b, (((1,), (1,)), ((), ())), preferred_element_type=F32)


def dot_tn(a, b):
    return lax.dot_general(a, b, (((0,), (0,)), ((), ())), preferred_element_type=F32)


def const_spec(shape):
    zeros = (0,) * len(shape)
    return pl.BlockSpec(shape, lambda *_: zeros, pipeline_mode=pl.Buffered(1))


def run(kernel, grid, in_specs, out_specs, out_shape, args, scratch=(), prefetch=0, aliases=None, flops=0, nbytes=0, limit=60):
    spec = pltpu.PrefetchScalarGridSpec(num_scalar_prefetch=prefetch, grid=grid, in_specs=in_specs, out_specs=out_specs, scratch_shapes=scratch)
    return pl.pallas_call(
        kernel,
        grid_spec=spec,
        out_shape=out_shape,
        input_output_aliases=aliases or {},
        compiler_params=pltpu.CompilerParams(dimension_semantics=("arbitrary",) * len(grid), vmem_limit_bytes=limit * MIB),
        cost_estimate=pl.CostEstimate(flops=int(flops), bytes_accessed=int(nbytes), transcendentals=0),
    )(*args)


def rope_fwd(x, cos_t, sin_t):
    half = x.shape[-1] // 2
    a, b = x[:, :half], x[:, half:]
    return a * cos_t - b * sin_t, b * cos_t + a * sin_t


def rope_bwd(a, b, cos_t, sin_t):
    return a * cos_t + b * sin_t, b * cos_t - a * sin_t


def pre_kernel(me_ref, h_ref, gain_ref, wk_ref, wv_ref, cos_ref, sin_ref, u_ref, kv_ref):
    x = h_ref[0].astype(F32)
    inv = lax.rsqrt(jnp.mean(x * x, axis=-1, keepdims=True) + EPS)
    u = (x * inv * gain_ref[...]).astype(BF)
    u_ref[0] = u
    hd = wk_ref.shape[1]
    first, second = rope_fwd(dot_nn(u, wk_ref[...]), cos_ref[...], sin_ref[...])
    kv_ref[0, :, : hd // 2] = first.astype(BF)
    kv_ref[0, :, hd // 2 : hd] = second.astype(BF)
    kv_ref[0, :, hd:] = dot_nn(u, wv_ref[...]).astype(BF)


def attn_fwd_kernel(me_ref, pre_ref, val_ref, u_ref, wq_ref, kv_ref, cos_ref, sin_ref, token_ref, q_ref, pt_ref, mix_ref, vt_ref, s_ref):
    b = pl.program_id(0)
    tp_n, _, cols = wq_ref.shape
    hd = kv_ref.shape[-1] // 2
    seq = kv_ref.shape[0] * kv_ref.shape[2]
    sl = u_ref.shape[1]
    heads = tp_n * cols // hd
    u = u_ref[0]
    cos_t, sin_t = cos_ref[...], sin_ref[...]
    keys = kv_ref[:, 0, :, :hd].reshape(seq, hd)
    vt_ref[...] = kv_ref[:, 0, :, hd:].reshape(seq, hd).astype(F32).T.astype(BF)
    for s in range(tp_n):
        qs = dot_nn(u, wq_ref[s])
        for j in range(cols // hd):
            base = (s * (cols // hd) + j) * hd
            first, second = rope_fwd(qs[:, j * hd : (j + 1) * hd], cos_t, sin_t)
            q_ref[0, :, base : base + hd // 2] = first.astype(BF)
            q_ref[0, :, base + hd // 2 : base + hd] = second.astype(BF)
    prefix, valid = pre_ref[b], val_ref[b]
    q_end = lax.broadcasted_iota(jnp.int32, (1, sl), 1) + (me_ref[0] * sl + 1)
    limit = jnp.minimum(valid, jnp.maximum(prefix, q_end))
    visible = lax.broadcasted_iota(jnp.int32, (seq, sl), 0) < limit
    scale = (hd**-0.5) * math.log2(math.e)

    def scores(h):
        return dot_nt(keys, q_ref[0, :, h * hd : (h + 1) * hd])

    s_ref[0] = scores(0)
    for h in range(heads):
        if h + 1 < heads:
            s_ref[(h + 1) % 2] = scores(h + 1)
        sc = jnp.where(visible, s_ref[h % 2], -1e30)
        top = jnp.max(sc, axis=0, keepdims=True)
        e = jnp.exp2((sc - top) * scale)
        p = (e * (1.0 / jnp.sum(e, axis=0, keepdims=True))).astype(BF)
        pt_ref[0, :, h * sl : (h + 1) * sl] = p
        mix_ref[0, :, h * hd : (h + 1) * hd] = dot_nn(vt_ref[...], p).T.astype(BF)


def out_kernel(mix_ref, wo_ref, h_ref, gain_ref, *rest):
    resid_ref, z_ref = rest[-2:]
    x = (h_ref[0].astype(F32) + dot_nn(mix_ref[0], wo_ref[...])).astype(BF)
    resid_ref[0] = x
    x = x.astype(F32)
    inv = lax.rsqrt(jnp.mean(x * x, axis=-1, keepdims=True) + EPS)
    z_ref[0] = (x * inv * gain_ref[...]).astype(BF)


def place_copies(pieces, cats, sems):
    return [pltpu.make_async_copy(src, dst, sems.at[i]) for i, (src, dst) in enumerate(zip(pieces, cats))]


def start_at_first(copies):
    @pl.when(pl.program_id(0) == 0)
    def _():
        for c in copies:
            c.start()


def wait_at_last(copies):
    @pl.when(pl.program_id(0) == pl.num_programs(0) - 1)
    def _():
        for c in copies:
            c.wait()


def dact_near_kernel(me_ref, ga_ref, gb_ref, wd_ref, *rest):
    da_ref, cat0_ref, cat1_ref, own0_ref, own1_ref, sems = rest[-6:]
    half = ga_ref.shape[0] // 2
    rows, dim = half * ga_ref.shape[1], ga_ref.shape[2]
    chip, core = me_ref[0] // 2, me_ref[0] % 2
    src, dst = [], []
    for c, (cat, own) in enumerate(((cat0_ref, own0_ref), (cat1_ref, own1_ref))):
        mine = ga_ref.at[pl.ds(c * half, half)]
        src += [mine, gb_ref.at[pl.ds(c * half, half)], mine]
        dst += [cat.at[chip, core], cat.at[chip, 1 - core], own]
    copies = place_copies(src, dst, sems)
    start_at_first(copies)
    for c in range(2):
        for rel, ref in enumerate((ga_ref, gb_ref)):
            g = ref[c * half : (c + 1) * half].reshape(rows, dim)
            da_ref[c, rel] = dot_nt(g, wd_ref[...]).astype(BF)
    wait_at_last(copies)


def dact_far_kernel(me_ref, ga_ref, gb_ref, wd_ref, *rest):
    da_ref, cat_ref, sems = rest[-3:]
    rows, dim = ga_ref.shape[0] * ga_ref.shape[1], ga_ref.shape[2]
    chip, core = 1 - me_ref[0] // 2, me_ref[0] % 2
    copies = place_copies([ga_ref, gb_ref], [cat_ref.at[chip, core], cat_ref.at[chip, 1 - core]], sems)
    start_at_first(copies)
    for rel, ref in enumerate((ga_ref, gb_ref)):
        da_ref[0, rel] = dot_nt(ref[...].reshape(rows, dim), wd_ref[...]).astype(BF)
    wait_at_last(copies)


def gated(gate, up, da):
    c0 = math.sqrt(2.0 / math.pi)
    c1 = c0 * 0.044715
    x2 = gate * gate
    hh = 0.5 + 0.5 * jnp.tanh(gate * (c0 + c1 * x2))
    gelu = gate * hh
    slope = hh + gelu * ((1.0 - hh) * (2.0 * c0 + 6.0 * c1 * x2))
    return (gelu * up).astype(BF), (da * up * slope).astype(BF), (da * gelu).astype(BF)


def mlp_kernel(other, me_ref, za_ref, zb_ref, da_ref, wg_ref, wu_ref, *rest):
    act_ref, dg_ref, du_ref, cat_ref, sems = rest[-5:]
    rows, dim = za_ref.shape[0] * za_ref.shape[1], za_ref.shape[2]
    core = me_ref[0] % 2
    chip = abs(other - me_ref[0] // 2)
    copies = place_copies([za_ref, zb_ref], [cat_ref.at[chip, core], cat_ref.at[chip, 1 - core]], sems)
    start_at_first(copies)
    step = rows // 2
    for rel, ref in enumerate((za_ref, zb_ref)):
        place = core if rel == 0 else 1 - core
        z = ref[...].reshape(rows, dim)
        for r in range(0, rows, step):
            zr = z[r : r + step]
            out = gated(dot_nn(zr, wg_ref[...]), dot_nn(zr, wu_ref[...]), da_ref[0, rel, r : r + step, :].astype(F32))
            for o_ref, o in zip((act_ref, dg_ref, du_ref), out):
                o_ref[0, place, r : r + step, :] = o
    wait_at_last(copies)


def mlp_fused_kernel(other, me_ref, za_ref, zb_ref, ga_ref, gb_ref, wg_ref, wu_ref, wd_ref, *rest):
    act_ref, dg_ref, du_ref, zcat_ref, gcat_ref, sems = rest[-6:]
    rows, dim = za_ref.shape[0] * za_ref.shape[1], za_ref.shape[2]
    core = me_ref[0] % 2
    chip = abs(other - me_ref[0] // 2)
    here, there = (chip, core), (chip, 1 - core)
    copies = place_copies([za_ref, zb_ref, ga_ref, gb_ref], [zcat_ref.at[here], zcat_ref.at[there], gcat_ref.at[here], gcat_ref.at[there]], sems)
    start_at_first(copies)
    step = rows // 3
    for rel, (z_ref, g_ref) in enumerate(((za_ref, ga_ref), (zb_ref, gb_ref))):
        place = core if rel == 0 else 1 - core
        z, g = z_ref[...].reshape(rows, dim), g_ref[...].reshape(rows, dim)
        for r in range(0, rows, step):
            zr = z[r : r + step]
            out = gated(dot_nn(zr, wg_ref[...]), dot_nn(zr, wu_ref[...]), dot_nt(g[r : r + step], wd_ref[...]))
            for o_ref, o in zip((act_ref, dg_ref, du_ref), out):
                o_ref[0, place, r : r + step, :] = o
    wait_at_last(copies)


def attn_bwd_kernel(me_ref, dz0_ref, dz1_ref, res_ref, go_ref, gain_ref, wo_ref, kv_ref, q_ref, pt_ref, cos_ref, sin_ref, token0_ref, token1_ref, token2_ref,
                    dres_ref, dq_ref, dkv_ref, gn_ref, kt_ref, do_ref, qs_ref, ds_ref, dp_ref):
    b = pl.program_id(0)
    half = pl.num_programs(0) // 2
    hd = kv_ref.shape[-1] // 2
    seq = kv_ref.shape[0] * kv_ref.shape[2]
    sl = q_ref.shape[1]
    heads = q_ref.shape[2] // hd
    x = res_ref[0].astype(F32)
    dz = jnp.where(b < half, dz0_ref[0], dz1_ref[0]).astype(F32)
    inv = lax.rsqrt(jnp.mean(x * x, axis=-1, keepdims=True) + EPS)
    xn = x * inv
    part = jnp.sum(dz * xn, axis=0, keepdims=True)

    @pl.when(b == 0)
    def _():
        gn_ref[...] = part

    @pl.when(b > 0)
    def _():
        gn_ref[...] += part

    dxn = dz * gain_ref[...]
    dx = inv * (dxn - xn * jnp.mean(dxn * xn, axis=-1, keepdims=True))
    dres = (go_ref[0].astype(F32) + dx).astype(BF)
    dres_ref[0] = dres
    keys = kv_ref[:, 0, :, :hd].reshape(seq, hd)
    vals = kv_ref[:, 0, :, hd:].reshape(seq, hd)
    kt_ref[...] = keys.astype(F32).T.astype(BF)
    for h in range(heads):
        do_ref[h * sl : (h + 1) * sl, :] = dot_nt(dres, wo_ref[h * hd : (h + 1) * hd, :]).astype(BF)
        qs_ref[h * sl : (h + 1) * sl, :] = q_ref[0, :, h * hd : (h + 1) * hd]
    scale = hd**-0.5
    cos_t, sin_t = cos_ref[...], sin_ref[...]

    def dprobs(h):
        return dot_nt(vals, do_ref[h * sl : (h + 1) * sl, :])

    dp_ref[0] = dprobs(0)
    for h in range(heads):
        if h + 1 < heads:
            dp_ref[(h + 1) % 2] = dprobs(h + 1)
        p = pt_ref[0, :, h * sl : (h + 1) * sl].astype(F32)
        t = p * dp_ref[h % 2]
        ds = ((t - p * jnp.sum(t, axis=0, keepdims=True)) * scale).astype(BF)
        ds_ref[:, h * sl : (h + 1) * sl] = ds
        dq = dot_nn(kt_ref[...], ds).T
        first, second = rope_bwd(dq[:, : hd // 2], dq[:, hd // 2 :], cos_t, sin_t)
        dq_ref[0, :, h * hd : h * hd + hd // 2] = first.astype(BF)
        dq_ref[0, :, h * hd + hd // 2 : (h + 1) * hd] = second.astype(BF)
    shape = (kv_ref.shape[0], kv_ref.shape[2], hd)
    dkv_ref[:, 0, :, :hd] = dot_nn(ds_ref[...], qs_ref[...]).astype(BF).reshape(shape)
    dkv_ref[:, 0, :, hd:] = dot_nn(pt_ref[0], do_ref[...]).astype(BF).reshape(shape)


def last_kernel(me_ref, dkv_ref, dq_ref, u_ref, h_ref, dres_ref, gain_ref, wq_ref, wk_ref, wv_ref, cos_ref, sin_ref, gm_ref, token0_ref, token1_ref,
                gh_ref, gkv_ref, acc_ref):
    b = pl.program_id(0)
    tp_n, dim, cols = wq_ref.shape
    hd = wk_ref.shape[1]
    raw = dkv_ref[0]
    dk = raw[:, :hd].astype(F32)
    first, second = rope_bwd(dk[:, : hd // 2], dk[:, hd // 2 :], cos_ref[...], sin_ref[...])
    dk = jnp.concatenate([first, second], axis=1).astype(BF)
    dv = raw[:, hd:]
    dn = dot_nt(dk, wk_ref[...]) + dot_nt(dv, wv_ref[...])
    for s in range(tp_n):
        dn = dn + dot_nt(dq_ref[0, :, s * cols : (s + 1) * cols], wq_ref[s])
    x = h_ref[0].astype(F32)
    inv = lax.rsqrt(jnp.mean(x * x, axis=-1, keepdims=True) + EPS)
    xn = x * inv
    part = jnp.sum(dn * xn, axis=0, keepdims=True)
    dxn = dn * gain_ref[...]
    dx = inv * (dxn - xn * jnp.mean(dxn * xn, axis=-1, keepdims=True))
    gh_ref[0] = (dres_ref[0].astype(F32) + dx).astype(BF)
    gk = dot_tn(u_ref[0], jnp.concatenate([dk, dv], axis=1))

    @pl.when(b == 0)
    def _():
        acc_ref[...] = part
        gkv_ref[:dim, :] = gk

    @pl.when(b > 0)
    def _():
        acc_ref[...] += part
        gkv_ref[:dim, :] += gk

    @pl.when(b == pl.num_programs(0) - 1)
    def _():
        width = 2 * hd
        per = dim // width
        for i in range(per):
            gkv_ref[dim + i : dim + i + 1, :] = gm_ref[:, i * width : (i + 1) * width]
            gkv_ref[dim + per + i : dim + per + i + 1, :] = acc_ref[:, i * width : (i + 1) * width]


def wgrad_kernel(x_ref, y_ref, o_ref):
    o_ref[0] = dot_tn(x_ref[...], y_ref[...])


def tie_kernel(x_ref, *rest):
    del x_ref, rest


def tie(x, *tokens):
    return pl.pallas_call(
        tie_kernel,
        name="tie",
        in_specs=[ANY] * (1 + len(tokens)),
        out_specs=ANY,
        out_shape=jax.ShapeDtypeStruct(x.shape, x.dtype),
        input_output_aliases={0: 0},
    )(x, *tokens)


def solution(mesh):
    act_spec = P("dp", "tp", None)
    in_specs = (act_spec, act_spec, P("dp"), P("dp"), P(None), P(None, "tp"), P(None, None), P(None, None), P("tp", None), P(None), P(None, "tp"), P(None, "tp"), P("tp", None))
    out_specs = (act_spec, act_spec, P("dp"), P("dp", "tp"), P("dp", None), P("dp", None), P(("dp", "tp"), None), P("dp"), P("dp", "tp"), P("dp", "tp"), P(("dp", "tp"), None))
    core_flip = [(0, 1), (1, 0), (2, 3), (3, 2)]
    chip_flip = [(0, 2), (2, 0), (1, 3), (3, 1)]

    def to_core(x):
        return lax.ppermute(x, "tp", core_flip)

    def to_chip(x):
        return lax.ppermute(x, "tp", chip_flip)

    def local_layer(hidden, grad_out, prefix_len, valid_len, attn_norm, w_query, w_key, w_value, w_out, mlp_norm, w_gate, w_up, w_down):
        batch, sl, dim = hidden.shape
        half = batch // 2
        rows = half * sl
        hd = w_key.shape[1]
        cols = w_query.shape[1]
        tp_n = mesh.shape["tp"]
        seq = sl * tp_n
        qd = cols * tp_n
        heads = qd // hd
        ffn = w_gate.shape[1]
        own = batch * sl
        me = lax.axis_index("tp").astype(jnp.int32).reshape(1)

        inv_freq = np.exp(np.arange(hd // 2, dtype=np.float32) * np.float32(2.0 / hd) * np.float32(-math.log(10000.0)))
        angles = np.arange(seq, dtype=np.float32)[:, None] * inv_freq[None, :]
        cos_t, sin_t = jnp.asarray(np.cos(angles)), jnp.asarray(np.sin(angles))
        gain1 = (1.0 + attn_norm.astype(F32)).reshape(1, dim)
        gain2 = (1.0 + mlp_norm.astype(F32)).reshape(1, dim)

        def sds(shape, dtype=BF):
            return jax.ShapeDtypeStruct(shape, dtype)

        def block(shape, at, single=False):
            return pl.BlockSpec(shape, at, pipeline_mode=pl.Buffered(1) if single else None)

        tok_spec = block((1, sl, dim), lambda b, *_: (b, 0, 0))
        q_spec = block((1, sl, qd), lambda b, *_: (b, 0, 0))
        kv_spec = block((1, sl, 2 * hd), lambda b, *_: (b, 0, 0))
        kv4_spec = block((tp_n, 1, sl, 2 * hd), lambda b, *_: (0, b, 0, 0))
        pt_spec = block((1, seq, heads * sl), lambda b, *_: (b, 0, 0))
        rope_spec = block((sl, hd // 2), lambda b, m, *_: (m[0], 0), True)
        gain_spec = const_spec((1, dim))
        dma = lambda n: pltpu.SemaphoreType.DMA((n,))

        wq4 = lax.all_gather(w_query, "tp", axis=0)
        g_mate = to_core(grad_out)
        u, kv = run(
            pre_kernel, (batch,),
            [tok_spec, gain_spec, const_spec((dim, hd)), const_spec((dim, hd)), rope_spec, rope_spec],
            [tok_spec, kv_spec], [sds((batch, sl, dim)), sds((batch, sl, 2 * hd))],
            (me, hidden, gain1, w_key, w_value, cos_t, sin_t), prefetch=1,
            flops=4 * own * dim * hd, nbytes=6 * own * dim)
        kv4 = lax.all_gather(kv, "tp", axis=0)
        wo_all = lax.all_gather(w_out, "tp", axis=0, tiled=True)

        bn = 512
        whole_spec = block((batch, sl, dim), lambda n, *_: (0, 0, 0), True)
        half_spec = block((half, sl, dim), lambda n, *_: (0, 0, 0), True)
        cat_shape = (2, 2, half, sl, dim)
        da_near, gcat0, gcat1, go0, go1 = run(
            dact_near_kernel, (ffn // bn,),
            [whole_spec, whole_spec, block((bn, dim), lambda n, *_: (n, 0)), ANY],
            [block((2, 2, rows, bn), lambda n, *_: (0, 0, 0, n))] + [ANY] * 4,
            [sds((2, 2, rows, ffn))] + [sds(cat_shape)] * 2 + [sds((half, sl, dim))] * 2,
            (me, grad_out, g_mate, w_down, kv), prefetch=1, scratch=[dma(6)],
            flops=8 * rows * dim * ffn, nbytes=2 * ffn * dim + 8 * rows * ffn)

        q, pt, mixed = run(
            attn_fwd_kernel, (batch,),
            [tok_spec, const_spec((tp_n, dim, cols)), kv4_spec, rope_spec, rope_spec, ANY],
            [q_spec, pt_spec, q_spec],
            [sds((batch, sl, qd)), sds((batch, seq, heads * sl)), sds((batch, sl, qd))],
            (me, prefix_len, valid_len, u, wq4, kv4, cos_t, sin_t, da_near), prefetch=3,
            scratch=[pltpu.VMEM((hd, seq), BF), pltpu.VMEM((2, seq, sl), F32)],
            flops=2 * own * dim * qd + 4 * own * seq * qd, nbytes=2 * own * heads * seq)

        g_far = [to_chip(tie(go0, mixed))]

        def out_proj(c, prev):
            at = lambda b: (b + c * half, 0, 0)
            extra = [prev] if c else []
            return run(
                out_kernel, (half,),
                [block((1, sl, qd), at), const_spec((qd, dim)), block((1, sl, dim), at), gain_spec] + [ANY] * len(extra),
                [block((1, sl, dim), at), block((1, sl, dim), lambda b: (b, 0, 0))],
                [sds((batch, sl, dim)), sds((half, sl, dim))],
                (mixed, wo_all, hidden, gain2, *extra), aliases={4: 0} if c else None,
                flops=own * dim * qd, nbytes=4 * own * dim)

        resid, z0 = out_proj(0, None)
        resid, z1 = out_proj(1, resid)
        zs = [z0, z1]
        z_mate = [to_core(z) for z in zs]
        z_far = [to_chip(z0)]
        z_far.append(to_chip(z1))
        g_far.append(to_chip(tie(go1, z1)))

        o_shape = (2, 2, rows, ffn)

        def mlp(other, c, za, zb, da, prev, token):
            extra = list(prev) if prev is not None else []
            o_spec = block((1, 2, rows, bn), lambda n, m: (abs(other - m[0] // 2), 0, 0, n))
            w_spec = block((dim, bn), lambda n, *_: (0, n))
            return run(
                functools.partial(mlp_kernel, other), (ffn // bn,),
                [half_spec, half_spec, block((1, 2, rows, bn), lambda n, *_: (c, 0, 0, n)), w_spec, w_spec] + [ANY] * (len(extra) + 1),
                [o_spec] * 3 + [ANY], [sds(o_shape)] * 3 + [sds(cat_shape)],
                (me, za, zb, da, w_gate, w_up, *extra, token),
                prefetch=1, scratch=[dma(2)], aliases={6 + i: i for i in range(4)} if extra else None,
                flops=8 * rows * dim * ffn, nbytes=4 * ffn * dim + 16 * rows * ffn)

        near0 = mlp(0, 0, zs[0], z_mate[0], da_near, None, z1)
        near1 = mlp(0, 1, zs[1], z_mate[1], da_near, None, near0[0])

        ga = tie(g_far[0], near0[0])
        gb = to_core(ga)
        da_far, gcat0 = run(
            dact_far_kernel, (ffn // bn,),
            [half_spec, half_spec, block((bn, dim), lambda n, *_: (n, 0)), ANY, ANY],
            [block((1, 2, rows, bn), lambda n, *_: (0, 0, 0, n)), ANY],
            [sds((1, 2, rows, ffn)), sds(cat_shape)],
            (me, ga, gb, w_down, gcat0, near1[0]), prefetch=1, scratch=[dma(2)], aliases={4: 1},
            flops=4 * rows * dim * ffn, nbytes=2 * ffn * dim + 4 * rows * ffn)
        za = tie(z_far[0], near1[0])
        zb = to_core(za)
        full0 = mlp(1, 0, za, zb, da_far, near0, da_far)

        def gated_grad(full):
            flat = (4 * rows, ffn)
            return (dot_nt(full[1].reshape(flat), w_gate) + dot_nt(full[2].reshape(flat), w_up)).astype(BF)

        def mlp_out(full):
            return dot_nn(full[0].reshape(4 * rows, ffn), w_down).astype(BF)

        def scatter(x):
            return lax.psum_scatter(x.reshape(tp_n, rows, dim), "tp", scatter_dimension=0).reshape(half, sl, dim)

        dz_part0 = gated_grad(full0)
        dz0 = scatter(dz_part0)
        mlp_part0 = mlp_out(full0)
        part0 = scatter(mlp_part0)

        ga, za = tie(g_far[1], full0[0]), tie(z_far[1], full0[0])
        gb, zb = to_core(ga), to_core(za)
        bf = 512
        o_spec = block((1, 2, rows, bf), lambda n, m: (1 - m[0] // 2, 0, 0, n))
        w_spec = block((dim, bf), lambda n, *_: (0, n))
        full1 = run(
            functools.partial(mlp_fused_kernel, 1), (ffn // bf,),
            [half_spec] * 4 + [w_spec, w_spec, block((bf, dim), lambda n, *_: (n, 0))] + [ANY] * 7,
            [o_spec] * 3 + [ANY] * 2, [sds(o_shape)] * 3 + [sds(cat_shape)] * 2,
            (me, za, zb, ga, gb, w_gate, w_up, w_down, *near1, gcat1, dz_part0, mlp_part0),
            prefetch=1, scratch=[dma(4)], aliases={8 + i: i for i in range(5)},
            flops=12 * rows * dim * ffn, nbytes=6 * ffn * dim + 12 * rows * ffn)
        gcat1 = full1[4]
        dz_part1 = gated_grad(full1)
        dz1 = scatter(dz_part1)
        mlp_part1 = mlp_out(full1)
        part1 = scatter(mlp_part1)
        hidden_out = (resid.astype(F32) + jnp.concatenate([part0, part1]).astype(F32)).astype(BF)

        def grad_half(a, b):
            return dot_tn(a.reshape(4 * rows, -1), b.reshape(4 * rows, -1))

        g_down_half = grad_half(full0[0], gcat0)

        d_resid, d_q, dkv_part, gn2 = run(
            attn_bwd_kernel, (batch,),
            [block((1, sl, dim), lambda b, *_: (jnp.minimum(b, half - 1), 0, 0)), block((1, sl, dim), lambda b, *_: (jnp.maximum(b - half, 0), 0, 0)),
             tok_spec, tok_spec, gain_spec, const_spec((qd, dim)), kv4_spec, q_spec, pt_spec, rope_spec, rope_spec, ANY, ANY, ANY],
            [tok_spec, q_spec, kv4_spec, block((1, dim), lambda b, *_: (0, 0))],
            [sds((batch, sl, dim)), sds((batch, sl, qd)), sds((tp_n, batch, sl, 2 * hd)), sds((1, dim), F32)],
            (me, dz0, dz1, resid, grad_out, gain2, wo_all, kv4, q, pt, cos_t, sin_t, mlp_part1, g_down_half, part0), prefetch=1,
            scratch=[pltpu.VMEM((hd, seq), BF), pltpu.VMEM((heads * sl, hd), BF), pltpu.VMEM((heads * sl, hd), BF), pltpu.VMEM((seq, heads * sl), BF), pltpu.VMEM((2, seq, sl), F32)],
            flops=2 * own * dim * qd + 8 * own * seq * qd, nbytes=2 * own * heads * seq)
        dkv = lax.psum_scatter(tie(dkv_part, part1), "tp", scatter_dimension=0)

        g_out = dot_tn(mixed.reshape(own, qd), d_resid.reshape(own, dim))
        g_out_sum = lax.psum_scatter(g_out, "tp", scatter_dimension=0, tiled=True)
        bm = dim // 2
        g_query = run(
            wgrad_kernel, (dim // bm, tp_n),
            [block((own, bm), lambda i, j: (0, i)), block((own, cols), lambda i, j: (0, j))],
            block((1, bm, cols), lambda i, j: (j, i, 0)), sds((tp_n, dim, cols), F32),
            (u.reshape(own, dim), d_q.reshape(own, qd)), flops=2 * own * dim * qd, nbytes=4 * dim * qd)
        g_query_sum = lax.psum_scatter(g_query, "tp", scatter_dimension=0)

        extra = dim // hd
        grad_hidden, gkv = run(
            last_kernel, (batch,),
            [kv_spec, q_spec, tok_spec, tok_spec, tok_spec, gain_spec,
             const_spec((tp_n, dim, cols)), const_spec((dim, hd)), const_spec((dim, hd)), rope_spec, rope_spec, const_spec((1, dim)), ANY, ANY],
            [tok_spec, block((dim + extra, 2 * hd), lambda b, *_: (0, 0))],
            [sds((batch, sl, dim)), sds((dim + extra, 2 * hd), F32)],
            (me, dkv, d_q, u, hidden, d_resid, gain1, wq4, w_key, w_value, cos_t, sin_t, gn2, g_out, g_query), prefetch=1,
            scratch=[pltpu.VMEM((1, dim), F32)],
            flops=2 * own * dim * (qd + 4 * hd), nbytes=8 * own * dim)
        gkv = lax.psum(gkv, "tp")
        g_key, g_value = gkv[:dim, :hd], gkv[:dim, hd:]
        g_mlp_norm = gkv[dim : dim + extra // 2].reshape(dim)
        g_attn_norm = gkv[dim + extra // 2 :].reshape(dim)

        g_down = g_down_half + grad_half(full1[0], gcat1)
        g_gate = grad_half(full0[3], full0[1]) + grad_half(full1[3], full1[1])
        g_up = grad_half(full0[3], full0[2]) + grad_half(full1[3], full1[2])
        return (hidden_out, grad_hidden, g_attn_norm, g_query_sum, g_key, g_value, g_out_sum, g_mlp_norm, g_gate, g_up, g_down)

    return jax.shard_map(local_layer, mesh=mesh, in_specs=in_specs, out_specs=out_specs, check_vma=False)
```

```python
import functools
import math

import jax
import jax.numpy as jnp
import numpy as np
from jax import lax
from jax.experimental import pallas as pl
from jax.experimental.pallas import tpu as pltpu
from jax.sharding import PartitionSpec as P


EPS = 1e-6
BF = jnp.bfloat16
F32 = jnp.float32
MIB = 1024 * 1024
ANY = pl.BlockSpec(memory_space=pl.ANY)


def dot_nn(a, b):
    return lax.dot_general(a, b, (((1,), (0,)), ((), ())), preferred_element_type=F32)


def dot_nt(a, b):
    return lax.dot_general(a, b, (((1,), (1,)), ((), ())), preferred_element_type=F32)


def dot_tn(a, b):
    return lax.dot_general(a, b, (((0,), (0,)), ((), ())), preferred_element_type=F32)


def const_spec(shape):
    zeros = (0,) * len(shape)
    return pl.BlockSpec(shape, lambda *_: zeros, pipeline_mode=pl.Buffered(1))


def run(kernel, grid, in_specs, out_specs, out_shape, args, scratch=(), prefetch=0, aliases=None, flops=0, nbytes=0, limit=60):
    spec = pltpu.PrefetchScalarGridSpec(num_scalar_prefetch=prefetch, grid=grid, in_specs=in_specs, out_specs=out_specs, scratch_shapes=scratch)
    return pl.pallas_call(
        kernel,
        grid_spec=spec,
        out_shape=out_shape,
        input_output_aliases=aliases or {},
        compiler_params=pltpu.CompilerParams(dimension_semantics=("arbitrary",) * len(grid), vmem_limit_bytes=limit * MIB),
        cost_estimate=pl.CostEstimate(flops=int(flops), bytes_accessed=int(nbytes), transcendentals=0),
    )(*args)


def rope_fwd(x, cos_t, sin_t):
    half = x.shape[-1] // 2
    a, b = x[:, :half], x[:, half:]
    return a * cos_t - b * sin_t, b * cos_t + a * sin_t


def rope_bwd(a, b, cos_t, sin_t):
    return a * cos_t + b * sin_t, b * cos_t - a * sin_t


def pre_kernel(me_ref, h_ref, gain_ref, wk_ref, wv_ref, cos_ref, sin_ref, u_ref, kv_ref):
    x = h_ref[0].astype(F32)
    inv = lax.rsqrt(jnp.mean(x * x, axis=-1, keepdims=True) + EPS)
    u = (x * inv * gain_ref[...]).astype(BF)
    u_ref[0] = u
    hd = wk_ref.shape[1]
    first, second = rope_fwd(dot_nn(u, wk_ref[...]), cos_ref[...], sin_ref[...])
    kv_ref[0, :, : hd // 2] = first.astype(BF)
    kv_ref[0, :, hd // 2 : hd] = second.astype(BF)
    kv_ref[0, :, hd:] = dot_nn(u, wv_ref[...]).astype(BF)


def attn_fwd_kernel(me_ref, pre_ref, val_ref, u_ref, w0_ref, w1_ref, w2_ref, w3_ref, k0_ref, k1_ref, k2_ref, k3_ref, cos_ref, sin_ref, token_ref,
                    q_ref, pt_ref, mix_ref, keys_ref, vt_ref, s_ref):
    b = pl.program_id(0)
    cols = w0_ref.shape[1]
    _, hd = keys_ref.shape
    sl = u_ref.shape[1]
    heads = q_ref.shape[2] // hd
    u = u_ref[0]
    me = me_ref[0]
    cos_t, sin_t = cos_ref[...], sin_ref[...]
    place = []
    for r, kv_ref in enumerate((k0_ref, k1_ref, k2_ref, k3_ref)):
        keys_ref[r * sl : (r + 1) * sl, :] = kv_ref[0, :, :hd]
        vt_ref[:, r * sl : (r + 1) * sl] = kv_ref[0, :, hd:].astype(F32).T.astype(BF)
        place.append(lax.broadcasted_iota(jnp.int32, (sl, sl), 0) + (me ^ r) * sl)
    for r, w_ref in enumerate((w0_ref, w1_ref, w2_ref, w3_ref)):
        qs = dot_nn(u, w_ref[...])
        for j in range(cols // hd):
            base = r * cols + j * hd
            first, second = rope_fwd(qs[:, j * hd : (j + 1) * hd], cos_t, sin_t)
            q_ref[0, :, base : base + hd // 2] = first.astype(BF)
            q_ref[0, :, base + hd // 2 : base + hd] = second.astype(BF)
    prefix, valid = pre_ref[b], val_ref[b]
    q_end = lax.broadcasted_iota(jnp.int32, (1, sl), 1) + (me * sl + 1)
    limit = jnp.minimum(valid, jnp.maximum(prefix, q_end))
    visible = jnp.concatenate(place, axis=0) < limit
    scale = (hd**-0.5) * math.log2(math.e)

    def scores(h):
        return dot_nt(keys_ref[...], q_ref[0, :, h * hd : (h + 1) * hd])

    s_ref[0] = scores(0)
    for h in range(heads):
        if h + 1 < heads:
            s_ref[(h + 1) % 2] = scores(h + 1)
        sc = jnp.where(visible, s_ref[h % 2], -1e30)
        top = jnp.max(sc, axis=0, keepdims=True)
        e = jnp.exp2((sc - top) * scale)
        p = (e * (1.0 / jnp.sum(e, axis=0, keepdims=True))).astype(BF)
        pt_ref[0, :, h * sl : (h + 1) * sl] = p
        mix_ref[0, :, h * hd : (h + 1) * hd] = dot_nn(vt_ref[...], p).T.astype(BF)


def fetch_at_first(refs, dst, axis, sems):
    @pl.when(pl.program_id(0) == 0)
    def _():
        at, copies = 0, []
        for i, ref in enumerate(refs):
            n = ref.shape[axis]
            copies.append(pltpu.make_async_copy(ref, dst.at[pl.ds(at, n), :] if axis == 0 else dst.at[:, pl.ds(at, n)], sems.at[i]))
            at += n
        for c in copies:
            c.start()
        for c in copies:
            c.wait()


def out_kernel(mix_ref, w0_ref, w1_ref, w2_ref, w3_ref, h_ref, gain_ref, *rest):
    resid_ref, z_ref, wo_ref, sems = rest[-4:]
    fetch_at_first((w0_ref, w1_ref, w2_ref, w3_ref), wo_ref, 0, sems)
    x = (h_ref[0].astype(F32) + dot_nn(mix_ref[0], wo_ref[...])).astype(BF)
    resid_ref[0] = x
    x = x.astype(F32)
    inv = lax.rsqrt(jnp.mean(x * x, axis=-1, keepdims=True) + EPS)
    z_ref[0] = (x * inv * gain_ref[...]).astype(BF)


def place_copies(pieces, cats, sems):
    return [pltpu.make_async_copy(src, dst, sems.at[i]) for i, (src, dst) in enumerate(zip(pieces, cats))]


def start_at_first(copies):
    @pl.when(pl.program_id(0) == 0)
    def _():
        for c in copies:
            c.start()


def wait_at_last(copies):
    @pl.when(pl.program_id(0) == pl.num_programs(0) - 1)
    def _():
        for c in copies:
            c.wait()


def dact_near_kernel(rel, me_ref, g_ref, wd_ref, *rest):
    outs, sems = rest[-4 if rel else -6 : -1], rest[-1]
    da_ref, cats, owns = outs[0], outs[1:3], outs[3:]
    half = g_ref.shape[0] // 2
    rows, dim = half * g_ref.shape[1], g_ref.shape[2]
    chip = me_ref[0] // 2
    core = abs(rel - me_ref[0] % 2)
    src, dst = [], []
    for c in range(2):
        piece = g_ref.at[pl.ds(c * half, half)]
        src.append(piece)
        dst.append(cats[c].at[chip, core])
        if owns:
            src.append(piece)
            dst.append(owns[c])
    copies = place_copies(src, dst, sems)
    start_at_first(copies)
    da_ref[...] = dot_nt(g_ref[...].reshape(2 * rows, dim), wd_ref[...]).astype(BF).reshape(da_ref.shape)
    wait_at_last(copies)


def dact_far_kernel(me_ref, ga_ref, gb_ref, wd_ref, *rest):
    da_ref, db_ref, cat_ref, sems = rest[-4:]
    rows, dim = ga_ref.shape[0] * ga_ref.shape[1], ga_ref.shape[2]
    chip, core = 1 - me_ref[0] // 2, me_ref[0] % 2
    copies = place_copies([ga_ref, gb_ref], [cat_ref.at[chip, core], cat_ref.at[chip, 1 - core]], sems)
    start_at_first(copies)
    for ref, o_ref in ((ga_ref, da_ref), (gb_ref, db_ref)):
        o_ref[0] = dot_nt(ref[...].reshape(rows, dim), wd_ref[...]).astype(BF)
    wait_at_last(copies)


def gated(gate, up, da):
    c0 = math.sqrt(2.0 / math.pi)
    c1 = c0 * 0.044715
    x2 = gate * gate
    hh = 0.5 + 0.5 * jnp.tanh(gate * (c0 + c1 * x2))
    gelu = gate * hh
    slope = hh + gelu * ((1.0 - hh) * (2.0 * c0 + 6.0 * c1 * x2))
    return (gelu * up).astype(BF), (da * up * slope).astype(BF), (da * gelu).astype(BF)


def mlp_kernel(other, me_ref, za_ref, zb_ref, da_ref, db_ref, wg_ref, wu_ref, *rest):
    act_ref, dg_ref, du_ref, cat_ref, sems = rest[-5:]
    rows, dim = za_ref.shape[0] * za_ref.shape[1], za_ref.shape[2]
    core = me_ref[0] % 2
    chip = abs(other - me_ref[0] // 2)
    copies = place_copies([za_ref, zb_ref], [cat_ref.at[chip, core], cat_ref.at[chip, 1 - core]], sems)
    start_at_first(copies)
    step = rows // 2
    for rel, (ref, d_ref) in enumerate(((za_ref, da_ref), (zb_ref, db_ref))):
        place = core if rel == 0 else 1 - core
        z = ref[...].reshape(rows, dim)
        for r in range(0, rows, step):
            zr = z[r : r + step]
            out = gated(dot_nn(zr, wg_ref[...]), dot_nn(zr, wu_ref[...]), d_ref[0, r : r + step, :].astype(F32))
            for o_ref, o in zip((act_ref, dg_ref, du_ref), out):
                o_ref[0, place, r : r + step, :] = o
    wait_at_last(copies)


def mlp_fused_kernel(other, me_ref, za_ref, zb_ref, ga_ref, gb_ref, wg_ref, wu_ref, wd_ref, *rest):
    act_ref, dg_ref, du_ref, zcat_ref, gcat_ref, sems = rest[-6:]
    rows, dim = za_ref.shape[0] * za_ref.shape[1], za_ref.shape[2]
    core = me_ref[0] % 2
    chip = abs(other - me_ref[0] // 2)
    here, there = (chip, core), (chip, 1 - core)
    copies = place_copies([za_ref, zb_ref, ga_ref, gb_ref], [zcat_ref.at[here], zcat_ref.at[there], gcat_ref.at[here], gcat_ref.at[there]], sems)
    start_at_first(copies)
    step = rows // 3
    for rel, (z_ref, g_ref) in enumerate(((za_ref, ga_ref), (zb_ref, gb_ref))):
        place = core if rel == 0 else 1 - core
        z, g = z_ref[...].reshape(rows, dim), g_ref[...].reshape(rows, dim)
        for r in range(0, rows, step):
            zr = z[r : r + step]
            out = gated(dot_nn(zr, wg_ref[...]), dot_nn(zr, wu_ref[...]), dot_nt(g[r : r + step], wd_ref[...]))
            for o_ref, o in zip((act_ref, dg_ref, du_ref), out):
                o_ref[0, place, r : r + step, :] = o
    wait_at_last(copies)


def attn_bwd_kernel(me_ref, dz0_ref, dz1_ref, res_ref, go_ref, gain_ref, w0_ref, w1_ref, w2_ref, w3_ref, k0_ref, k1_ref, k2_ref, k3_ref,
                    q_ref, pt_ref, cos_ref, sin_ref, token0_ref, token1_ref, token2_ref,
                    dres_ref, dq_ref, dkv_ref, gn_ref, kt_ref, v_ref, do_ref, qs_ref, ds_ref, dp_ref):
    b = pl.program_id(0)
    half = pl.num_programs(0) // 2
    seq, hd = v_ref.shape
    sl = q_ref.shape[1]
    heads = q_ref.shape[2] // hd
    me = me_ref[0]
    x = res_ref[0].astype(F32)
    dz = jnp.where(b < half, dz0_ref[0], dz1_ref[0]).astype(F32)
    inv = lax.rsqrt(jnp.mean(x * x, axis=-1, keepdims=True) + EPS)
    xn = x * inv
    part = jnp.sum(dz * xn, axis=0, keepdims=True)

    @pl.when(b == 0)
    def _():
        gn_ref[...] = part

    @pl.when(b > 0)
    def _():
        gn_ref[...] += part

    dxn = dz * gain_ref[...]
    dx = inv * (dxn - xn * jnp.mean(dxn * xn, axis=-1, keepdims=True))
    dres = (go_ref[0].astype(F32) + dx).astype(BF)
    dres_ref[0] = dres
    for r, kv_ref in enumerate((k0_ref, k1_ref, k2_ref, k3_ref)):
        kt_ref[:, r * sl : (r + 1) * sl] = kv_ref[0, :, :hd].astype(F32).T.astype(BF)
        v_ref[r * sl : (r + 1) * sl, :] = kv_ref[0, :, hd:]
    for r, w_ref in enumerate((w0_ref, w1_ref, w2_ref, w3_ref)):
        dm = dot_nt(dres, w_ref[...]).astype(BF)
        per = w_ref.shape[0] // hd
        for j in range(per):
            h = r * per + j
            do_ref[h * sl : (h + 1) * sl, :] = dm[:, j * hd : (j + 1) * hd]
            qs_ref[h * sl : (h + 1) * sl, :] = q_ref[0, :, h * hd : (h + 1) * hd]
    scale = hd**-0.5
    cos_t, sin_t = cos_ref[...], sin_ref[...]

    def dprobs(h):
        return dot_nt(v_ref[...], do_ref[h * sl : (h + 1) * sl, :])

    dp_ref[0] = dprobs(0)
    for h in range(heads):
        if h + 1 < heads:
            dp_ref[(h + 1) % 2] = dprobs(h + 1)
        p = pt_ref[0, :, h * sl : (h + 1) * sl].astype(F32)
        t = p * dp_ref[h % 2]
        ds = ((t - p * jnp.sum(t, axis=0, keepdims=True)) * scale).astype(BF)
        ds_ref[:, h * sl : (h + 1) * sl] = ds
        dq = dot_nn(kt_ref[...], ds).T
        first, second = rope_bwd(dq[:, : hd // 2], dq[:, hd // 2 :], cos_t, sin_t)
        dq_ref[0, :, h * hd : h * hd + hd // 2] = first.astype(BF)
        dq_ref[0, :, h * hd + hd // 2 : (h + 1) * hd] = second.astype(BF)
    dk = dot_nn(ds_ref[...], qs_ref[...]).astype(BF)
    dv = dot_nn(pt_ref[0], do_ref[...]).astype(BF)
    for r in range(seq // sl):
        dkv_ref[me ^ r, 0, :, :hd] = dk[r * sl : (r + 1) * sl]
        dkv_ref[me ^ r, 0, :, hd:] = dv[r * sl : (r + 1) * sl]


def last_kernel(me_ref, dkv_ref, dq_ref, u_ref, h_ref, dres_ref, gain_ref, w0_ref, w1_ref, w2_ref, w3_ref, wk_ref, wv_ref, cos_ref, sin_ref, gm_ref,
                token0_ref, token1_ref, gh_ref, gkv_ref, acc_ref, w_ref, d_ref, sems):
    b = pl.program_id(0)
    dim, hd = wk_ref.shape
    qd = dq_ref.shape[2]
    fetch_at_first((w0_ref, w1_ref, w2_ref, w3_ref, wk_ref, wv_ref), w_ref, 1, sems)
    raw = dkv_ref[0]
    dk = raw[:, :hd].astype(F32)
    first, second = rope_bwd(dk[:, : hd // 2], dk[:, hd // 2 :], cos_ref[...], sin_ref[...])
    d_ref[:, :qd] = dq_ref[0]
    d_ref[:, qd : qd + hd // 2] = first.astype(BF)
    d_ref[:, qd + hd // 2 : qd + hd] = second.astype(BF)
    d_ref[:, qd + hd :] = raw[:, hd:]
    dn = dot_nt(d_ref[...], w_ref[...])
    gk = dot_tn(u_ref[0], d_ref[:, qd:])
    x = h_ref[0].astype(F32)
    inv = lax.rsqrt(jnp.mean(x * x, axis=-1, keepdims=True) + EPS)
    xn = x * inv
    part = jnp.sum(dn * xn, axis=0, keepdims=True)
    dxn = dn * gain_ref[...]
    dx = inv * (dxn - xn * jnp.mean(dxn * xn, axis=-1, keepdims=True))
    gh_ref[0] = (dres_ref[0].astype(F32) + dx).astype(BF)

    @pl.when(b == 0)
    def _():
        acc_ref[...] = part
        gkv_ref[:dim, :] = gk

    @pl.when(b > 0)
    def _():
        acc_ref[...] += part
        gkv_ref[:dim, :] += gk

    @pl.when(b == pl.num_programs(0) - 1)
    def _():
        width = 2 * hd
        per = dim // width
        for i in range(per):
            gkv_ref[dim + i : dim + i + 1, :] = gm_ref[:, i * width : (i + 1) * width]
            gkv_ref[dim + per + i : dim + per + i + 1, :] = acc_ref[:, i * width : (i + 1) * width]


def block_grad_kernel(n_add, x_ref, y_ref, *rest):
    out = dot_tn(x_ref[...], y_ref[...])
    for ref in rest[:n_add]:
        out = out + ref[...].reshape(out.shape)
    rest[-1][...] = out.reshape(rest[-1].shape)


def wgrad_kernel(x0_ref, x1_ref, y0_ref, y1_ref, *rest):
    rest[-1][...] = dot_tn(x0_ref[...], y0_ref[...]) + dot_tn(x1_ref[...], y1_ref[...])


def tie_kernel(x_ref, *rest):
    del x_ref, rest


def tie(x, *tokens):
    return pl.pallas_call(
        tie_kernel,
        name="tie",
        in_specs=[ANY] * (1 + len(tokens)),
        out_specs=ANY,
        out_shape=jax.ShapeDtypeStruct(x.shape, x.dtype),
        input_output_aliases={0: 0},
    )(x, *tokens)


def solution(mesh):
    act_spec = P("dp", "tp", None)
    in_specs = (act_spec, act_spec, P("dp"), P("dp"), P(None), P(None, "tp"), P(None, None), P(None, None), P("tp", None), P(None), P(None, "tp"), P(None, "tp"), P("tp", None))
    out_specs = (act_spec, act_spec, P("dp"), P("dp", "tp"), P("dp", None), P("dp", None), P(("dp", "tp"), None), P("dp"), P("dp", "tp"), P("dp", "tp"), P(("dp", "tp"), None))
    core_flip = [(0, 1), (1, 0), (2, 3), (3, 2)]
    chip_flip = [(0, 2), (2, 0), (1, 3), (3, 1)]

    def to_core(x):
        return lax.ppermute(x, "tp", core_flip)

    def to_chip(x):
        return lax.ppermute(x, "tp", chip_flip)

    def local_layer(hidden, grad_out, prefix_len, valid_len, attn_norm, w_query, w_key, w_value, w_out, mlp_norm, w_gate, w_up, w_down):
        batch, sl, dim = hidden.shape
        half = batch // 2
        rows = half * sl
        hd = w_key.shape[1]
        cols = w_query.shape[1]
        tp_n = mesh.shape["tp"]
        seq = sl * tp_n
        qd = cols * tp_n
        heads = qd // hd
        ffn = w_gate.shape[1]
        own = batch * sl
        me = lax.axis_index("tp").astype(jnp.int32).reshape(1)

        inv_freq = np.exp(np.arange(hd // 2, dtype=np.float32) * np.float32(2.0 / hd) * np.float32(-math.log(10000.0)))
        angles = np.arange(seq, dtype=np.float32)[:, None] * inv_freq[None, :]
        cos_t, sin_t = jnp.asarray(np.cos(angles)), jnp.asarray(np.sin(angles))
        gain1 = (1.0 + attn_norm.astype(F32)).reshape(1, dim)
        gain2 = (1.0 + mlp_norm.astype(F32)).reshape(1, dim)

        def sds(shape, dtype=BF):
            return jax.ShapeDtypeStruct(shape, dtype)

        def block(shape, at, single=False):
            return pl.BlockSpec(shape, at, pipeline_mode=pl.Buffered(1) if single else None)

        tok_spec = block((1, sl, dim), lambda b, *_: (b, 0, 0))
        q_spec = block((1, sl, qd), lambda b, *_: (b, 0, 0))
        kv_spec = block((1, sl, 2 * hd), lambda b, *_: (b, 0, 0))
        kv4_spec = block((tp_n, 1, sl, 2 * hd), lambda b, *_: (0, b, 0, 0))
        pt_spec = block((1, seq, heads * sl), lambda b, *_: (b, 0, 0))
        rope_spec = block((sl, hd // 2), lambda b, m, *_: (m[0], 0), True)
        gain_spec = const_spec((1, dim))
        dma = lambda n: pltpu.SemaphoreType.DMA((n,))

        wq_far = to_chip(w_query)
        wq_mate = to_core(w_query)
        g_mate = to_core(grad_out)
        u, kv = run(
            pre_kernel, (batch,),
            [tok_spec, gain_spec, const_spec((dim, hd)), const_spec((dim, hd)), rope_spec, rope_spec],
            [tok_spec, kv_spec], [sds((batch, sl, dim)), sds((batch, sl, 2 * hd))],
            (me, hidden, gain1, w_key, w_value, cos_t, sin_t), prefetch=1,
            flops=4 * own * dim * hd, nbytes=6 * own * dim)
        kv_far = to_chip(kv)
        kv_mate = to_core(kv)
        wo_far = to_chip(w_out)
        wo_mate = to_core(w_out)

        bn = 512
        whole_spec = block((batch, sl, dim), lambda n, *_: (0, 0, 0), True)
        half_spec = block((half, sl, dim), lambda n, *_: (0, 0, 0), True)
        cat_shape = (2, 2, half, sl, dim)
        da_shape = (2, rows, ffn)

        def dact_near(rel, g, token, cats):
            return run(
                functools.partial(dact_near_kernel, rel), (ffn // bn,),
                [whole_spec, block((bn, dim), lambda n, *_: (n, 0))] + [ANY] * (1 + len(cats)),
                [block((2, rows, bn), lambda n, *_: (0, 0, n))] + [ANY] * (2 if rel else 4),
                [sds(da_shape)] + [sds(cat_shape)] * 2 + ([] if rel else [sds((half, sl, dim))] * 2),
                (me, g, w_down, token, *cats), prefetch=1, scratch=[dma(2 if rel else 4)], aliases={4: 1, 5: 2} if rel else None,
                flops=4 * rows * dim * ffn, nbytes=2 * ffn * dim + 4 * rows * ffn)

        da_own, gcat0, gcat1, go0, go1 = dact_near(0, grad_out, kv, ())
        wq_far = tie(wq_far, da_own)
        wq_far_mate = to_core(wq_far)
        da_mate, gcat0, gcat1 = dact_near(1, g_mate, da_own, (gcat0, gcat1))
        kv_far = tie(kv_far, da_mate)
        kv_far_mate = to_core(kv_far)
        wqs = (w_query, wq_mate, wq_far, wq_far_mate)
        kvs = (kv, kv_mate, kv_far, kv_far_mate)
        wq_specs = [const_spec((dim, cols))] * 4
        wo_specs = [const_spec((cols, dim))] * 4

        q, pt, mixed = run(
            attn_fwd_kernel, (batch,),
            [tok_spec] + wq_specs + [kv_spec] * 4 + [rope_spec, rope_spec, ANY],
            [q_spec, pt_spec, q_spec],
            [sds((batch, sl, qd)), sds((batch, seq, heads * sl)), sds((batch, sl, qd))],
            (me, prefix_len, valid_len, u, *wqs, *kvs, cos_t, sin_t, da_mate), prefetch=3,
            scratch=[pltpu.VMEM((seq, hd), BF), pltpu.VMEM((hd, seq), BF), pltpu.VMEM((2, seq, sl), F32)],
            flops=2 * own * dim * qd + 4 * own * seq * qd, nbytes=2 * own * heads * seq)
        wo_far = tie(wo_far, mixed)
        wo_far_mate = to_core(wo_far)
        wos = (w_out, wo_mate, wo_far, wo_far_mate)

        g_far = [to_chip(tie(go0, mixed))]

        def out_proj(c, prev):
            at = lambda b: (b + c * half, 0, 0)
            extra = [prev] if c else []
            return run(
                out_kernel, (half,),
                [block((1, sl, qd), at)] + [ANY] * 4 + [block((1, sl, dim), at), gain_spec] + [ANY] * len(extra),
                [block((1, sl, dim), at), block((1, sl, dim), lambda b: (b, 0, 0))],
                [sds((batch, sl, dim)), sds((half, sl, dim))],
                (mixed, *wos, hidden, gain2, *extra), aliases={7: 0} if c else None,
                scratch=[pltpu.VMEM((qd, dim), BF), dma(4)],
                flops=own * dim * qd, nbytes=4 * own * dim)

        resid, z0 = out_proj(0, None)
        resid, z1 = out_proj(1, resid)
        zs = [z0, z1]
        z_mate = [to_core(z) for z in zs]
        z_far = [to_chip(z0)]
        z_far.append(to_chip(z1))
        g_far.append(to_chip(tie(go1, z1)))

        o_shape = (2, 2, rows, ffn)

        def mlp(other, c, za, zb, da, db, prev, token):
            extra = list(prev) if prev is not None else []
            o_spec = block((1, 2, rows, bn), lambda n, m: (abs(other - m[0] // 2), 0, 0, n))
            w_spec = block((dim, bn), lambda n, *_: (0, n))
            d_spec = block((1, rows, bn), lambda n, *_: (c, 0, n))
            return run(
                functools.partial(mlp_kernel, other), (ffn // bn,),
                [half_spec, half_spec, d_spec, d_spec, w_spec, w_spec] + [ANY] * (len(extra) + 1),
                [o_spec] * 3 + [ANY], [sds(o_shape)] * 3 + [sds(cat_shape)],
                (me, za, zb, da, db, w_gate, w_up, *extra, token),
                prefetch=1, scratch=[dma(2)], aliases={7 + i: i for i in range(4)} if extra else None,
                flops=8 * rows * dim * ffn, nbytes=4 * ffn * dim + 16 * rows * ffn)

        near0 = mlp(0, 0, zs[0], z_mate[0], da_own, da_mate, None, z1)
        near1 = mlp(0, 1, zs[1], z_mate[1], da_own, da_mate, None, near0[0])

        ga = tie(g_far[0], near0[0])
        gb = to_core(ga)
        da_far, db_far, gcat0 = run(
            dact_far_kernel, (ffn // bn,),
            [half_spec, half_spec, block((bn, dim), lambda n, *_: (n, 0)), ANY, ANY],
            [block((1, rows, bn), lambda n, *_: (0, 0, n))] * 2 + [ANY],
            [sds((1, rows, ffn))] * 2 + [sds(cat_shape)],
            (me, ga, gb, w_down, gcat0, near1[0]), prefetch=1, scratch=[dma(2)], aliases={4: 2},
            flops=4 * rows * dim * ffn, nbytes=2 * ffn * dim + 4 * rows * ffn)
        za = tie(z_far[0], near1[0])
        zb = to_core(za)
        full0 = mlp(1, 0, za, zb, da_far, db_far, near0, da_far)

        def gated_grad(full):
            flat = (4 * rows, ffn)
            return (dot_nt(full[1].reshape(flat), w_gate) + dot_nt(full[2].reshape(flat), w_up)).astype(BF)

        def mlp_out(full):
            return dot_nn(full[0].reshape(4 * rows, ffn), w_down).astype(BF)

        def scatter(x):
            return lax.psum_scatter(x.reshape(tp_n, rows, dim), "tp", scatter_dimension=0).reshape(half, sl, dim)

        dz_part0 = gated_grad(full0)
        dz0 = scatter(dz_part0)
        mlp_part0 = mlp_out(full0)
        part0 = scatter(mlp_part0)

        ga, za = tie(g_far[1], full0[0]), tie(z_far[1], full0[0])
        gb, zb = to_core(ga), to_core(za)
        bf = 512
        o_spec = block((1, 2, rows, bf), lambda n, m: (1 - m[0] // 2, 0, 0, n))
        w_spec = block((dim, bf), lambda n, *_: (0, n))
        full1 = run(
            functools.partial(mlp_fused_kernel, 1), (ffn // bf,),
            [half_spec] * 4 + [w_spec, w_spec, block((bf, dim), lambda n, *_: (n, 0))] + [ANY] * 7,
            [o_spec] * 3 + [ANY] * 2, [sds(o_shape)] * 3 + [sds(cat_shape)] * 2,
            (me, za, zb, ga, gb, w_gate, w_up, w_down, *near1, gcat1, dz_part0, mlp_part0),
            prefetch=1, scratch=[dma(4)], aliases={8 + i: i for i in range(5)},
            flops=12 * rows * dim * ffn, nbytes=6 * ffn * dim + 12 * rows * ffn)
        gcat1 = full1[4]
        dz_part1 = gated_grad(full1)
        dz1 = scatter(dz_part1)
        mlp_part1 = mlp_out(full1)
        part1 = scatter(mlp_part1)
        hidden_out = (resid.astype(F32) + jnp.concatenate([part0, part1]).astype(F32)).astype(BF)

        def weight_grad(x, y, token):
            x0, x1 = (a.reshape(4 * rows, -1) for a in x)
            y0, y1 = (a.reshape(4 * rows, -1) for a in y)
            m, n = x0.shape[1], y0.shape[1]
            bm, by = 1024, 512
            x_spec = block((4 * rows, bm), lambda i, j: (0, i))
            y_spec = block((4 * rows, by), lambda i, j: (0, j))
            return run(
                wgrad_kernel, (m // bm, n // by), [x_spec, x_spec, y_spec, y_spec, ANY], block((bm, by), lambda i, j: (i, j)),
                sds((m, n), F32), (x0, x1, y0, y1, token), flops=16 * rows * m * n, nbytes=4 * m * n)

        g_down = weight_grad((full0[0], full1[0]), (gcat0, gcat1), mlp_part1)

        d_resid, d_q, dkv_part, gn2 = run(
            attn_bwd_kernel, (batch,),
            [block((1, sl, dim), lambda b, *_: (jnp.minimum(b, half - 1), 0, 0)), block((1, sl, dim), lambda b, *_: (jnp.maximum(b - half, 0), 0, 0)),
             tok_spec, tok_spec, gain_spec] + wo_specs + [kv_spec] * 4 + [q_spec, pt_spec, rope_spec, rope_spec, ANY, ANY, ANY],
            [tok_spec, q_spec, kv4_spec, block((1, dim), lambda b, *_: (0, 0))],
            [sds((batch, sl, dim)), sds((batch, sl, qd)), sds((tp_n, batch, sl, 2 * hd)), sds((1, dim), F32)],
            (me, dz0, dz1, resid, grad_out, gain2, *wos, *kvs, q, pt, cos_t, sin_t, mlp_part1, g_down, part0), prefetch=1,
            scratch=[pltpu.VMEM((hd, seq), BF), pltpu.VMEM((seq, hd), BF), pltpu.VMEM((heads * sl, hd), BF), pltpu.VMEM((heads * sl, hd), BF), pltpu.VMEM((seq, heads * sl), BF), pltpu.VMEM((2, seq, sl), F32)],
            flops=2 * own * dim * qd + 8 * own * seq * qd, nbytes=2 * own * heads * seq)
        dkv = lax.psum_scatter(tie(dkv_part, part1), "tp", scatter_dimension=0)

        mixed2, dres2, u2, dq2 = mixed.reshape(own, qd), d_resid.reshape(own, dim), u.reshape(own, dim), d_q.reshape(own, qd)

        def block_grad(of_query, count, first, stride, adds, token):
            pick = lambda j: (0, first + stride * j)
            full, part = block((own, dim), lambda j: (0, 0), True), block((own, cols), pick)
            o_dims = (dim, cols) if of_query else (cols, dim)
            o_spec = block((1,) + o_dims, lambda j: (j, 0, 0))
            return run(
                functools.partial(block_grad_kernel, len(adds)), (count,),
                ([full, part] if of_query else [part, full]) + [block((1,) + o_dims, lambda j, k=k: (k, 0, 0), True) for _, k in adds] + [ANY],
                o_spec, sds((count,) + o_dims, F32), ((u2, dq2) if of_query else (mixed2, dres2)) + tuple(a for a, _ in adds) + (token,),
                flops=2 * count * own * dim * cols, nbytes=4 * count * dim * cols)

        to_mate = [block_grad(False, 2, 1, 2, (), d_resid)]
        to_mate.append(block_grad(True, 2, 1, 2, (), to_mate[0]))
        from_mate = [to_core(x) for x in to_mate]
        far_sum = [block_grad(False, 1, 2, 1, ((from_mate[0], 1),), to_mate[1])]
        far_sum.append(block_grad(True, 1, 2, 1, ((from_mate[1], 1),), far_sum[0]))
        go_arrived = to_chip(far_sum[0])
        gq_arrived = to_chip(far_sum[1])

        extra = dim // hd
        grad_hidden, gkv = run(
            last_kernel, (batch,),
            [kv_spec, q_spec, tok_spec, tok_spec, tok_spec, gain_spec,
             ] + [ANY] * 6 + [rope_spec, rope_spec, const_spec((1, dim)), ANY, ANY],
            [tok_spec, block((dim + extra, 2 * hd), lambda b, *_: (0, 0))],
            [sds((batch, sl, dim)), sds((dim + extra, 2 * hd), F32)],
            (me, dkv, d_q, u, hidden, d_resid, gain1, *wqs, w_key, w_value, cos_t, sin_t, gn2, *far_sum), prefetch=1,
            scratch=[pltpu.VMEM((1, dim), F32), pltpu.VMEM((dim, qd + 2 * hd), BF), pltpu.VMEM((sl, qd + 2 * hd), BF), dma(6)],
            flops=2 * own * dim * (qd + 4 * hd), nbytes=8 * own * dim)
        gkv = lax.psum(gkv, "tp")
        g_key, g_value = gkv[:dim, :hd], gkv[:dim, hd:]
        g_mlp_norm = gkv[dim : dim + extra // 2].reshape(dim)
        g_attn_norm = gkv[dim + extra // 2 :].reshape(dim)

        g_gate = weight_grad((full0[3], full1[3]), (full0[1], full1[1]), grad_hidden)
        g_up = weight_grad((full0[3], full1[3]), (full0[2], full1[2]), g_gate)
        g_out_sum = block_grad(False, 1, 0, 1, ((from_mate[0], 0), (go_arrived, 0)), g_gate)[0]
        g_query_sum = block_grad(True, 1, 0, 1, ((from_mate[1], 0), (gq_arrived, 0)), g_up)[0]
        return (hidden_out, grad_hidden, g_attn_norm, g_query_sum, g_key, g_value, g_out_sum, g_mlp_norm, g_gate, g_up, g_down)

    return jax.shard_map(local_layer, mesh=mesh, in_specs=in_specs, out_specs=out_specs, check_vma=False)
```

```python
import functools
import math

import jax
import jax.numpy as jnp
import numpy as np
from jax import lax
from jax.experimental import pallas as pl
from jax.experimental.pallas import tpu as pltpu
from jax.sharding import PartitionSpec as P


EPS = 1e-6
BF = jnp.bfloat16
F32 = jnp.float32
MIB = 1024 * 1024
ANY = pl.BlockSpec(memory_space=pl.ANY)


def dot_nn(a, b):
    return lax.dot_general(a, b, (((1,), (0,)), ((), ())), preferred_element_type=F32)


def dot_nt(a, b):
    return lax.dot_general(a, b, (((1,), (1,)), ((), ())), preferred_element_type=F32)


def dot_tn(a, b):
    return lax.dot_general(a, b, (((0,), (0,)), ((), ())), preferred_element_type=F32)


def const_spec(shape):
    zeros = (0,) * len(shape)
    return pl.BlockSpec(shape, lambda *_: zeros, pipeline_mode=pl.Buffered(1))


def run(kernel, grid, in_specs, out_specs, out_shape, args, scratch=(), prefetch=0, aliases=None, flops=0, nbytes=0, limit=60):
    spec = pltpu.PrefetchScalarGridSpec(num_scalar_prefetch=prefetch, grid=grid, in_specs=in_specs, out_specs=out_specs, scratch_shapes=scratch)
    return pl.pallas_call(
        kernel,
        grid_spec=spec,
        out_shape=out_shape,
        input_output_aliases=aliases or {},
        compiler_params=pltpu.CompilerParams(dimension_semantics=("arbitrary",) * len(grid), vmem_limit_bytes=limit * MIB),
        cost_estimate=pl.CostEstimate(flops=int(flops), bytes_accessed=int(nbytes), transcendentals=0),
    )(*args)


def rope_fwd(x, cos_t, sin_t):
    half = x.shape[-1] // 2
    a, b = x[:, :half], x[:, half:]
    return a * cos_t - b * sin_t, b * cos_t + a * sin_t


def rope_bwd(a, b, cos_t, sin_t):
    return a * cos_t + b * sin_t, b * cos_t - a * sin_t


def pre_kernel(me_ref, h_ref, gain_ref, wk_ref, wv_ref, cos_ref, sin_ref, u_ref, kv_ref):
    x = h_ref[0].astype(F32)
    inv = lax.rsqrt(jnp.mean(x * x, axis=-1, keepdims=True) + EPS)
    u = (x * inv * gain_ref[...]).astype(BF)
    u_ref[0] = u
    hd = wk_ref.shape[1]
    first, second = rope_fwd(dot_nn(u, wk_ref[...]), cos_ref[...], sin_ref[...])
    kv_ref[0, :, : hd // 2] = first.astype(BF)
    kv_ref[0, :, hd // 2 : hd] = second.astype(BF)
    kv_ref[0, :, hd:] = dot_nn(u, wv_ref[...]).astype(BF)


def attn_fwd_kernel(me_ref, pre_ref, val_ref, u_ref, w0_ref, w1_ref, w2_ref, w3_ref, k0_ref, k1_ref, k2_ref, k3_ref, cos_ref, sin_ref, token_ref,
                    q_ref, pt_ref, mix_ref, keys_ref, vt_ref, s_ref):
    b = pl.program_id(0)
    cols = w0_ref.shape[1]
    _, hd = keys_ref.shape
    sl = u_ref.shape[1]
    heads = q_ref.shape[2] // hd
    u = u_ref[0]
    me = me_ref[0]
    cos_t, sin_t = cos_ref[...], sin_ref[...]
    place = []
    for r, kv_ref in enumerate((k0_ref, k1_ref, k2_ref, k3_ref)):
        keys_ref[r * sl : (r + 1) * sl, :] = kv_ref[0, :, :hd]
        vt_ref[:, r * sl : (r + 1) * sl] = kv_ref[0, :, hd:].astype(F32).T.astype(BF)
        place.append(lax.broadcasted_iota(jnp.int32, (sl, sl), 0) + (me ^ r) * sl)
    for r, w_ref in enumerate((w0_ref, w1_ref, w2_ref, w3_ref)):
        qs = dot_nn(u, w_ref[...])
        for j in range(cols // hd):
            base = r * cols + j * hd
            first, second = rope_fwd(qs[:, j * hd : (j + 1) * hd], cos_t, sin_t)
            q_ref[0, :, base : base + hd // 2] = first.astype(BF)
            q_ref[0, :, base + hd // 2 : base + hd] = second.astype(BF)
    prefix, valid = pre_ref[b], val_ref[b]
    q_end = lax.broadcasted_iota(jnp.int32, (1, sl), 1) + (me * sl + 1)
    limit = jnp.minimum(valid, jnp.maximum(prefix, q_end))
    visible = jnp.concatenate(place, axis=0) < limit
    scale = (hd**-0.5) * math.log2(math.e)

    def scores(h):
        return dot_nt(keys_ref[...], q_ref[0, :, h * hd : (h + 1) * hd])

    s_ref[0] = scores(0)
    for h in range(heads):
        if h + 1 < heads:
            s_ref[(h + 1) % 2] = scores(h + 1)
        sc = jnp.where(visible, s_ref[h % 2], -1e30)
        top = jnp.max(sc, axis=0, keepdims=True)
        e = jnp.exp2((sc - top) * scale)
        p = (e * (1.0 / jnp.sum(e, axis=0, keepdims=True))).astype(BF)
        pt_ref[0, :, h * sl : (h + 1) * sl] = p
        mix_ref[0, :, h * hd : (h + 1) * hd] = dot_nn(vt_ref[...], p).T.astype(BF)


def fetch_at_first(refs, dst, axis, sems):
    @pl.when(pl.program_id(0) == 0)
    def _():
        at, copies = 0, []
        for i, ref in enumerate(refs):
            n = ref.shape[axis]
            copies.append(pltpu.make_async_copy(ref, dst.at[pl.ds(at, n), :] if axis == 0 else dst.at[:, pl.ds(at, n)], sems.at[i]))
            at += n
        for c in copies:
            c.start()
        for c in copies:
            c.wait()


def out_kernel(mix_ref, w0_ref, w1_ref, w2_ref, w3_ref, h_ref, gain_ref, *rest):
    resid_ref, z_ref, wo_ref, sems = rest[-4:]
    fetch_at_first((w0_ref, w1_ref, w2_ref, w3_ref), wo_ref, 0, sems)
    x = (h_ref[0].astype(F32) + dot_nn(mix_ref[0], wo_ref[...])).astype(BF)
    resid_ref[0] = x
    x = x.astype(F32)
    inv = lax.rsqrt(jnp.mean(x * x, axis=-1, keepdims=True) + EPS)
    z_ref[0] = (x * inv * gain_ref[...]).astype(BF)


def place_copies(pieces, cats, sems):
    return [pltpu.make_async_copy(src, dst, sems.at[i]) for i, (src, dst) in enumerate(zip(pieces, cats))]


def start_at_first(copies):
    @pl.when(pl.program_id(0) == 0)
    def _():
        for c in copies:
            c.start()


def wait_at_last(copies):
    @pl.when(pl.program_id(0) == pl.num_programs(0) - 1)
    def _():
        for c in copies:
            c.wait()


def dact_near_kernel(rel, me_ref, g_ref, wd_ref, *rest):
    outs, sems = rest[-4 if rel else -6 : -1], rest[-1]
    da_ref, cats, owns = outs[0], outs[1:3], outs[3:]
    half = g_ref.shape[0] // 2
    rows, dim = half * g_ref.shape[1], g_ref.shape[2]
    chip = me_ref[0] // 2
    core = abs(rel - me_ref[0] % 2)
    src, dst = [], []
    for c in range(2):
        piece = g_ref.at[pl.ds(c * half, half)]
        src.append(piece)
        dst.append(cats[c].at[chip, core])
        if owns:
            src.append(piece)
            dst.append(owns[c])
    copies = place_copies(src, dst, sems)
    start_at_first(copies)
    da_ref[...] = dot_nt(g_ref[...].reshape(2 * rows, dim), wd_ref[...]).astype(BF).reshape(da_ref.shape)
    wait_at_last(copies)


def dact_far_kernel(me_ref, ga_ref, gb_ref, wd_ref, *rest):
    da_ref, db_ref, cat_ref, sems = rest[-4:]
    rows, dim = ga_ref.shape[0] * ga_ref.shape[1], ga_ref.shape[2]
    chip, core = 1 - me_ref[0] // 2, me_ref[0] % 2
    copies = place_copies([ga_ref, gb_ref], [cat_ref.at[chip, core], cat_ref.at[chip, 1 - core]], sems)
    start_at_first(copies)
    for ref, o_ref in ((ga_ref, da_ref), (gb_ref, db_ref)):
        o_ref[0] = dot_nt(ref[...].reshape(rows, dim), wd_ref[...]).astype(BF)
    wait_at_last(copies)


def gated(gate, up, da):
    c0 = math.sqrt(2.0 / math.pi)
    c1 = c0 * 0.044715
    x2 = gate * gate
    hh = 0.5 + 0.5 * jnp.tanh(gate * (c0 + c1 * x2))
    gelu = gate * hh
    slope = hh + gelu * ((1.0 - hh) * (2.0 * c0 + 6.0 * c1 * x2))
    return (gelu * up).astype(BF), (da * up * slope).astype(BF), (da * gelu).astype(BF)


def mlp_kernel(other, me_ref, za_ref, zb_ref, da_ref, db_ref, wg_ref, wu_ref, *rest):
    act_ref, dg_ref, du_ref, cat_ref, sems = rest[-5:]
    rows, dim = za_ref.shape[0] * za_ref.shape[1], za_ref.shape[2]
    core = me_ref[0] % 2
    chip = abs(other - me_ref[0] // 2)
    copies = place_copies([za_ref, zb_ref], [cat_ref.at[chip, core], cat_ref.at[chip, 1 - core]], sems)
    start_at_first(copies)
    step = rows // 2
    for rel, (ref, d_ref) in enumerate(((za_ref, da_ref), (zb_ref, db_ref))):
        place = core if rel == 0 else 1 - core
        z = ref[...].reshape(rows, dim)
        for r in range(0, rows, step):
            zr = z[r : r + step]
            out = gated(dot_nn(zr, wg_ref[...]), dot_nn(zr, wu_ref[...]), d_ref[0, r : r + step, :].astype(F32))
            for o_ref, o in zip((act_ref, dg_ref, du_ref), out):
                o_ref[0, place, r : r + step, :] = o
    wait_at_last(copies)


def mlp_fused_kernel(other, me_ref, za_ref, zb_ref, ga_ref, gb_ref, wg_ref, wu_ref, wd_ref, *rest):
    act_ref, dg_ref, du_ref, zcat_ref, gcat_ref, sems = rest[-6:]
    rows, dim = za_ref.shape[0] * za_ref.shape[1], za_ref.shape[2]
    core = me_ref[0] % 2
    chip = abs(other - me_ref[0] // 2)
    here, there = (chip, core), (chip, 1 - core)
    copies = place_copies([za_ref, zb_ref, ga_ref, gb_ref], [zcat_ref.at[here], zcat_ref.at[there], gcat_ref.at[here], gcat_ref.at[there]], sems)
    start_at_first(copies)
    step = rows // 3
    for rel, (z_ref, g_ref) in enumerate(((za_ref, ga_ref), (zb_ref, gb_ref))):
        place = core if rel == 0 else 1 - core
        z, g = z_ref[...].reshape(rows, dim), g_ref[...].reshape(rows, dim)
        for r in range(0, rows, step):
            zr = z[r : r + step]
            out = gated(dot_nn(zr, wg_ref[...]), dot_nn(zr, wu_ref[...]), dot_nt(g[r : r + step], wd_ref[...]))
            for o_ref, o in zip((act_ref, dg_ref, du_ref), out):
                o_ref[0, place, r : r + step, :] = o
    wait_at_last(copies)


def attn_bwd_kernel(me_ref, dz0_ref, dz1_ref, res_ref, go_ref, gain_ref, w0_ref, w1_ref, w2_ref, w3_ref, k0_ref, k1_ref, k2_ref, k3_ref,
                    q_ref, pt_ref, cos_ref, sin_ref, token0_ref, token1_ref, token2_ref,
                    dres_ref, dq_ref, dkv_ref, gn_ref, kt_ref, v_ref, do_ref, qs_ref, ds_ref, dp_ref):
    b = pl.program_id(0)
    half = pl.num_programs(0) // 2
    seq, hd = v_ref.shape
    sl = q_ref.shape[1]
    heads = q_ref.shape[2] // hd
    me = me_ref[0]
    x = res_ref[0].astype(F32)
    dz = jnp.where(b < half, dz0_ref[0], dz1_ref[0]).astype(F32)
    inv = lax.rsqrt(jnp.mean(x * x, axis=-1, keepdims=True) + EPS)
    xn = x * inv
    part = jnp.sum(dz * xn, axis=0, keepdims=True)

    @pl.when(b == 0)
    def _():
        gn_ref[...] = part

    @pl.when(b > 0)
    def _():
        gn_ref[...] += part

    dxn = dz * gain_ref[...]
    dx = inv * (dxn - xn * jnp.mean(dxn * xn, axis=-1, keepdims=True))
    dres = (go_ref[0].astype(F32) + dx).astype(BF)
    dres_ref[0] = dres
    scale = hd**-0.5
    for r, kv_ref in enumerate((k0_ref, k1_ref, k2_ref, k3_ref)):
        kt_ref[:, r * sl : (r + 1) * sl] = (kv_ref[0, :, :hd].astype(F32) * scale).T.astype(BF)
        v_ref[r * sl : (r + 1) * sl, :] = kv_ref[0, :, hd:]
    for r, w_ref in enumerate((w0_ref, w1_ref, w2_ref, w3_ref)):
        dm = dot_nt(dres, w_ref[...]).astype(BF)
        per = w_ref.shape[0] // hd
        for j in range(per):
            h = r * per + j
            do_ref[h * sl : (h + 1) * sl, :] = dm[:, j * hd : (j + 1) * hd]
            qs_ref[h * sl : (h + 1) * sl, :] = (q_ref[0, :, h * hd : (h + 1) * hd].astype(F32) * scale).astype(BF)
    cos_t, sin_t = cos_ref[...], sin_ref[...]

    def dprobs(h):
        return dot_nt(v_ref[...], do_ref[h * sl : (h + 1) * sl, :])

    dp_ref[0] = dprobs(0)
    for h in range(heads):
        if h + 1 < heads:
            dp_ref[(h + 1) % 2] = dprobs(h + 1)
        p = pt_ref[0, :, h * sl : (h + 1) * sl].astype(F32)
        t = p * dp_ref[h % 2]
        ds = (t - p * jnp.sum(t, axis=0, keepdims=True)).astype(BF)
        ds_ref[:, h * sl : (h + 1) * sl] = ds
        dq = dot_nn(kt_ref[...], ds).T
        first, second = rope_bwd(dq[:, : hd // 2], dq[:, hd // 2 :], cos_t, sin_t)
        dq_ref[0, :, h * hd : h * hd + hd // 2] = first.astype(BF)
        dq_ref[0, :, h * hd + hd // 2 : (h + 1) * hd] = second.astype(BF)
    dk = dot_nn(ds_ref[...], qs_ref[...]).astype(BF)
    dv = dot_nn(pt_ref[0], do_ref[...]).astype(BF)
    for r in range(seq // sl):
        dkv_ref[me ^ r, 0, :, :hd] = dk[r * sl : (r + 1) * sl]
        dkv_ref[me ^ r, 0, :, hd:] = dv[r * sl : (r + 1) * sl]


def last_kernel(me_ref, dkv_ref, dq_ref, u_ref, h_ref, dres_ref, gain_ref, w0_ref, w1_ref, w2_ref, w3_ref, wk_ref, wv_ref, cos_ref, sin_ref, gm_ref,
                res_ref, p0_ref, p1_ref, token0_ref, gh_ref, gkv_ref, ho_ref, acc_ref, w_ref, d_ref, sems):
    b = pl.program_id(0)
    dim, hd = wk_ref.shape
    qd = dq_ref.shape[2]
    fetch_at_first((w0_ref, w1_ref, w2_ref, w3_ref, wk_ref, wv_ref), w_ref, 1, sems)
    half = pl.num_programs(0) // 2
    ho_ref[0] = (res_ref[0].astype(F32) + jnp.where(b < half, p0_ref[0], p1_ref[0]).astype(F32)).astype(BF)
    raw = dkv_ref[0]
    dk = raw[:, :hd].astype(F32)
    first, second = rope_bwd(dk[:, : hd // 2], dk[:, hd // 2 :], cos_ref[...], sin_ref[...])
    d_ref[:, :qd] = dq_ref[0]
    d_ref[:, qd : qd + hd // 2] = first.astype(BF)
    d_ref[:, qd + hd // 2 : qd + hd] = second.astype(BF)
    d_ref[:, qd + hd :] = raw[:, hd:]
    dn = dot_nt(d_ref[...], w_ref[...])
    gk = dot_tn(u_ref[0], d_ref[:, qd:])
    x = h_ref[0].astype(F32)
    inv = lax.rsqrt(jnp.mean(x * x, axis=-1, keepdims=True) + EPS)
    xn = x * inv
    part = jnp.sum(dn * xn, axis=0, keepdims=True)
    dxn = dn * gain_ref[...]
    dx = inv * (dxn - xn * jnp.mean(dxn * xn, axis=-1, keepdims=True))
    gh_ref[0] = (dres_ref[0].astype(F32) + dx).astype(BF)

    @pl.when(b == 0)
    def _():
        acc_ref[...] = part
        gkv_ref[:dim, :] = gk

    @pl.when(b > 0)
    def _():
        acc_ref[...] += part
        gkv_ref[:dim, :] += gk

    @pl.when(b == pl.num_programs(0) - 1)
    def _():
        width = 2 * hd
        per = dim // width
        for i in range(per):
            gkv_ref[dim + i : dim + i + 1, :] = gm_ref[:, i * width : (i + 1) * width]
            gkv_ref[dim + per + i : dim + per + i + 1, :] = acc_ref[:, i * width : (i + 1) * width]


def block_grad_kernel(*refs):
    x_ref, y_ref, o_ref = refs[-4], refs[-3], refs[-1]
    o_ref[...] = dot_tn(x_ref[...], y_ref[...]).reshape(o_ref.shape)


def pair_grad_kernel(x_ref, y_ref, add_ref, token_ref, far_ref, own_ref):
    out = dot_tn(x_ref[...], y_ref[...]) + add_ref[0]

    @pl.when(pl.program_id(0) == 0)
    def _():
        far_ref[0] = out

    @pl.when(pl.program_id(0) == 1)
    def _():
        own_ref[0] = out


class Flow:
    def __init__(self, bufs, sems, inward, sides):
        self.bufs, self.sems, self.inward, self.sides = bufs, sems, inward, sides

    def copies(self, t, slot):
        out = []
        for i, (hbm, buf) in enumerate(zip(self.sides(t), self.bufs)):
            pair = (hbm, buf.at[slot]) if self.inward else (buf.at[slot], hbm)
            out.append(pltpu.make_async_copy(*pair, self.sems.at[slot, i]))
        return out

    def start(self, t, slot):
        for c in self.copies(t, slot):
            c.start()

    def wait(self, t, slot):
        for c in self.copies(t, slot):
            c.wait()


def gated_grad_kernel(dg_ref, du_ref, wg_ref, wu_ref, *rest):
    o_ref, a1, a2, b1, b2, ob, a_sem, b_sem, o_sem = rest[-9:]
    ni = dg_ref.shape[0] * dg_ref.shape[1]
    bn = b1.shape[1]
    nj = wg_ref.shape[0] // bn
    steps = ni * nj
    cols = lambda t: pl.ds(pl.multiple_of(lax.rem(t, nj) * bn, bn), bn)
    a_flow = Flow((a1, a2), a_sem, True, lambda i: (dg_ref.at[i // 2, i % 2], du_ref.at[i // 2, i % 2]))
    b_flow = Flow((b1, b2), b_sem, True, lambda t: (wg_ref.at[cols(t)], wu_ref.at[cols(t)]))
    o_flow = Flow((ob,), o_sem, False, lambda t: (o_ref.at[t // nj, :, cols(t)],))
    a_flow.start(0, 0)
    b_flow.start(0, 0)

    @pl.loop(0, steps)
    def _(t):
        i, slot = t // nj, lax.rem(t, 2)
        a_slot = lax.rem(i, 2)

        @pl.when(t + 1 < steps)
        def _():
            b_flow.start(t + 1, 1 - slot)

        @pl.when(lax.rem(t, nj) == 0)
        def _():
            a_flow.wait(i, a_slot)

            @pl.when(i + 1 < ni)
            def _():
                a_flow.start(i + 1, 1 - a_slot)

        @pl.when(t >= 2)
        def _():
            o_flow.wait(t - 2, slot)

        b_flow.wait(t, slot)
        ob[slot] = (dot_nt(a1[a_slot], b1[slot]) + dot_nt(a2[a_slot], b2[slot])).astype(BF)
        o_flow.start(t, slot)

    for t in (steps - 2, steps - 1):
        o_flow.wait(t, t % 2)


def weight_grads_kernel(count, first, ni, *refs):
    x_refs, y_refs = refs[:2], refs[2 : 2 + 2 * count]
    o_refs, (x0, x1, y0, y1, ob, x_sem, y_sem, o_sem) = refs[-8 - count : -8], refs[-8:]
    bm, bn = ob.shape[1:]
    nj = y_refs[0].shape[1] // bn
    steps = ni * count * nj
    per = count * nj
    rows = lambda i: pl.ds(pl.multiple_of((first + i) * bm, bm), bm)
    cols = lambda t: pl.ds(pl.multiple_of(lax.rem(t, nj) * bn, bn), bn)
    x_flow = Flow((x0, x1), x_sem, True, lambda i: [r.at[:, rows(i)] for r in x_refs])
    y_flows = [Flow((y0, y1), y_sem, True, lambda t, k=k: [r.at[:, cols(t)] for r in y_refs[2 * k : 2 * k + 2]]) for k in range(count)]
    o_flows = [Flow((ob,), o_sem, False, lambda t, k=k: (o_refs[k].at[rows(t // per), cols(t)],)) for k in range(count)]

    def each(flows, t, act):
        if count == 1:
            act(flows[0])
        else:
            which = lax.rem(t // nj, count)
            for k in range(count):
                pl.when(which == k)(functools.partial(act, flows[k]))

    x_flow.start(0, 0)
    y_flows[0].start(0, 0)

    @pl.loop(0, steps)
    def _(t):
        i, slot = t // per, lax.rem(t, 2)
        x_slot = lax.rem(i, 2)

        @pl.when(t + 1 < steps)
        def _():
            each(y_flows, t + 1, lambda f: f.start(t + 1, 1 - slot))

        @pl.when(lax.rem(t, per) == 0)
        def _():
            x_flow.wait(i, x_slot)

            @pl.when(i + 1 < ni)
            def _():
                x_flow.start(i + 1, 1 - x_slot)

        @pl.when(t >= 2)
        def _():
            o_flows[0].wait(t - 2, slot)

        y_flows[0].wait(t, slot)
        ob[slot] = dot_tn(x0[x_slot], y0[slot]) + dot_tn(x1[x_slot], y1[slot])
        each(o_flows, t, lambda f: f.start(t, slot))

    for t in (steps - 2, steps - 1):
        o_flows[0].wait(t, t % 2)


def tie_kernel(x_ref, *rest):
    del x_ref, rest


def tie(x, *tokens):
    return pl.pallas_call(
        tie_kernel,
        name="tie",
        in_specs=[ANY] * (1 + len(tokens)),
        out_specs=ANY,
        out_shape=jax.ShapeDtypeStruct(x.shape, x.dtype),
        input_output_aliases={0: 0},
    )(x, *tokens)


def solution(mesh):
    act_spec = P("dp", "tp", None)
    in_specs = (act_spec, act_spec, P("dp"), P("dp"), P(None), P(None, "tp"), P(None, None), P(None, None), P("tp", None), P(None), P(None, "tp"), P(None, "tp"), P("tp", None))
    out_specs = (act_spec, act_spec, P("dp"), P("dp", "tp"), P("dp", None), P("dp", None), P(("dp", "tp"), None), P("dp"), P("dp", "tp"), P("dp", "tp"), P(("dp", "tp"), None))
    core_flip = [(0, 1), (1, 0), (2, 3), (3, 2)]
    chip_flip = [(0, 2), (2, 0), (1, 3), (3, 1)]

    def to_core(x):
        return lax.ppermute(x, "tp", core_flip)

    def to_chip(x):
        return lax.ppermute(x, "tp", chip_flip)

    def local_layer(hidden, grad_out, prefix_len, valid_len, attn_norm, w_query, w_key, w_value, w_out, mlp_norm, w_gate, w_up, w_down):
        batch, sl, dim = hidden.shape
        half = batch // 2
        rows = half * sl
        hd = w_key.shape[1]
        cols = w_query.shape[1]
        tp_n = mesh.shape["tp"]
        seq = sl * tp_n
        qd = cols * tp_n
        heads = qd // hd
        ffn = w_gate.shape[1]
        own = batch * sl
        me = lax.axis_index("tp").astype(jnp.int32).reshape(1)

        inv_freq = np.exp(np.arange(hd // 2, dtype=np.float32) * np.float32(2.0 / hd) * np.float32(-math.log(10000.0)))
        angles = np.arange(seq, dtype=np.float32)[:, None] * inv_freq[None, :]
        cos_t, sin_t = jnp.asarray(np.cos(angles)), jnp.asarray(np.sin(angles))
        gain1 = (1.0 + attn_norm.astype(F32)).reshape(1, dim)
        gain2 = (1.0 + mlp_norm.astype(F32)).reshape(1, dim)

        def sds(shape, dtype=BF):
            return jax.ShapeDtypeStruct(shape, dtype)

        def block(shape, at, single=False):
            return pl.BlockSpec(shape, at, pipeline_mode=pl.Buffered(1) if single else None)

        tok_spec = block((1, sl, dim), lambda b, *_: (b, 0, 0))
        q_spec = block((1, sl, qd), lambda b, *_: (b, 0, 0))
        kv_spec = block((1, sl, 2 * hd), lambda b, *_: (b, 0, 0))
        kv4_spec = block((tp_n, 1, sl, 2 * hd), lambda b, *_: (0, b, 0, 0))
        pt_spec = block((1, seq, heads * sl), lambda b, *_: (b, 0, 0))
        rope_spec = block((sl, hd // 2), lambda b, m, *_: (m[0], 0), True)
        gain_spec = const_spec((1, dim))
        dma = lambda n: pltpu.SemaphoreType.DMA((n,))

        wq_far = to_chip(w_query)
        wq_mate = to_core(w_query)
        g_mate = to_core(grad_out)
        u, kv = run(
            pre_kernel, (batch,),
            [tok_spec, gain_spec, const_spec((dim, hd)), const_spec((dim, hd)), rope_spec, rope_spec],
            [tok_spec, kv_spec], [sds((batch, sl, dim)), sds((batch, sl, 2 * hd))],
            (me, hidden, gain1, w_key, w_value, cos_t, sin_t), prefetch=1,
            flops=4 * own * dim * hd, nbytes=6 * own * dim)
        kv_far = to_chip(kv)
        kv_mate = to_core(kv)
        wo_far = to_chip(w_out)
        wo_mate = to_core(w_out)

        bn = 512
        whole_spec = block((batch, sl, dim), lambda n, *_: (0, 0, 0), True)
        half_spec = block((half, sl, dim), lambda n, *_: (0, 0, 0), True)
        cat_shape = (2, 2, half, sl, dim)
        da_shape = (2, rows, ffn)

        def dact_near(rel, g, token, cats):
            return run(
                functools.partial(dact_near_kernel, rel), (ffn // bn,),
                [whole_spec, block((bn, dim), lambda n, *_: (n, 0))] + [ANY] * (1 + len(cats)),
                [block((2, rows, bn), lambda n, *_: (0, 0, n))] + [ANY] * (2 if rel else 4),
                [sds(da_shape)] + [sds(cat_shape)] * 2 + ([] if rel else [sds((half, sl, dim))] * 2),
                (me, g, w_down, token, *cats), prefetch=1, scratch=[dma(2 if rel else 4)], aliases={4: 1, 5: 2} if rel else None,
                flops=4 * rows * dim * ffn, nbytes=2 * ffn * dim + 4 * rows * ffn)

        da_own, gcat0, gcat1, go0, go1 = dact_near(0, grad_out, kv, ())
        wq_far = tie(wq_far, da_own)
        wq_far_mate = to_core(wq_far)
        da_mate, gcat0, gcat1 = dact_near(1, g_mate, da_own, (gcat0, gcat1))
        kv_far = tie(kv_far, da_mate)
        kv_far_mate = to_core(kv_far)
        wqs = (w_query, wq_mate, wq_far, wq_far_mate)
        kvs = (kv, kv_mate, kv_far, kv_far_mate)
        wq_specs = [const_spec((dim, cols))] * 4
        wo_specs = [const_spec((cols, dim))] * 4

        q, pt, mixed = run(
            attn_fwd_kernel, (batch,),
            [tok_spec] + wq_specs + [kv_spec] * 4 + [rope_spec, rope_spec, ANY],
            [q_spec, pt_spec, q_spec],
            [sds((batch, sl, qd)), sds((batch, seq, heads * sl)), sds((batch, sl, qd))],
            (me, prefix_len, valid_len, u, *wqs, *kvs, cos_t, sin_t, da_mate), prefetch=3,
            scratch=[pltpu.VMEM((seq, hd), BF), pltpu.VMEM((hd, seq), BF), pltpu.VMEM((2, seq, sl), F32)],
            flops=2 * own * dim * qd + 4 * own * seq * qd, nbytes=2 * own * heads * seq)
        wo_far = tie(wo_far, mixed)
        wo_far_mate = to_core(wo_far)
        wos = (w_out, wo_mate, wo_far, wo_far_mate)

        g_far = [to_chip(tie(go0, mixed))]

        def out_proj(c, prev):
            at = lambda b: (b + c * half, 0, 0)
            extra = [prev] if c else []
            return run(
                out_kernel, (half,),
                [block((1, sl, qd), at)] + [ANY] * 4 + [block((1, sl, dim), at), gain_spec] + [ANY] * len(extra),
                [block((1, sl, dim), at), block((1, sl, dim), lambda b: (b, 0, 0))],
                [sds((batch, sl, dim)), sds((half, sl, dim))],
                (mixed, *wos, hidden, gain2, *extra), aliases={7: 0} if c else None,
                scratch=[pltpu.VMEM((qd, dim), BF), dma(4)],
                flops=own * dim * qd, nbytes=4 * own * dim)

        resid, z0 = out_proj(0, None)
        resid, z1 = out_proj(1, resid)
        zs = [z0, z1]
        z_mate = [to_core(z) for z in zs]
        z_far = [to_chip(z0)]
        z_far.append(to_chip(z1))
        g_far.append(to_chip(tie(go1, z1)))

        o_shape = (2, 2, rows, ffn)

        def mlp(other, c, za, zb, da, db, prev, token):
            extra = list(prev) if prev is not None else []
            o_spec = block((1, 2, rows, bn), lambda n, m: (abs(other - m[0] // 2), 0, 0, n))
            w_spec = block((dim, bn), lambda n, *_: (0, n))
            d_spec = block((1, rows, bn), lambda n, *_: (c, 0, n))
            return run(
                functools.partial(mlp_kernel, other), (ffn // bn,),
                [half_spec, half_spec, d_spec, d_spec, w_spec, w_spec] + [ANY] * (len(extra) + 1),
                [o_spec] * 3 + [ANY], [sds(o_shape)] * 3 + [sds(cat_shape)],
                (me, za, zb, da, db, w_gate, w_up, *extra, token),
                prefetch=1, scratch=[dma(2)], aliases={7 + i: i for i in range(4)} if extra else None,
                flops=8 * rows * dim * ffn, nbytes=4 * ffn * dim + 16 * rows * ffn)

        near0 = mlp(0, 0, zs[0], z_mate[0], da_own, da_mate, None, z1)
        near1 = mlp(0, 1, zs[1], z_mate[1], da_own, da_mate, None, near0[0])

        ga = tie(g_far[0], near0[0])
        gb = to_core(ga)
        da_far, db_far, gcat0 = run(
            dact_far_kernel, (ffn // bn,),
            [half_spec, half_spec, block((bn, dim), lambda n, *_: (n, 0)), ANY, ANY],
            [block((1, rows, bn), lambda n, *_: (0, 0, n))] * 2 + [ANY],
            [sds((1, rows, ffn))] * 2 + [sds(cat_shape)],
            (me, ga, gb, w_down, gcat0, near1[0]), prefetch=1, scratch=[dma(2)], aliases={4: 2},
            flops=4 * rows * dim * ffn, nbytes=2 * ffn * dim + 4 * rows * ffn)
        za = tie(z_far[0], near1[0])
        zb = to_core(za)
        full0 = mlp(1, 0, za, zb, da_far, db_far, near0, da_far)

        def gated_grad(full):
            bj = 512
            return run(
                gated_grad_kernel, (), [ANY] * 5, ANY, sds((4, rows, dim)), (full[1], full[2], w_gate, w_up, full[0]),
                scratch=[pltpu.VMEM((2, rows, ffn), BF)] * 2 + [pltpu.VMEM((2, bj, ffn), BF)] * 2 + [pltpu.VMEM((2, rows, bj), BF)]
                + [pltpu.SemaphoreType.DMA((2, 2))] * 2 + [pltpu.SemaphoreType.DMA((2, 1))],
                flops=16 * rows * dim * ffn, nbytes=16 * rows * ffn)

        def mlp_out(full):
            return dot_nn(full[0].reshape(4 * rows, ffn), w_down).astype(BF)

        def scatter(x):
            return lax.psum_scatter(x.reshape(tp_n, rows, dim), "tp", scatter_dimension=0).reshape(half, sl, dim)

        dz_part0 = gated_grad(full0)
        dz0 = scatter(dz_part0)
        mlp_part0 = mlp_out(full0)
        part0 = scatter(mlp_part0)

        ga, za = tie(g_far[1], full0[0]), tie(z_far[1], full0[0])
        gb, zb = to_core(ga), to_core(za)
        bf = 512
        o_spec = block((1, 2, rows, bf), lambda n, m: (1 - m[0] // 2, 0, 0, n))
        w_spec = block((dim, bf), lambda n, *_: (0, n))
        full1 = run(
            functools.partial(mlp_fused_kernel, 1), (ffn // bf,),
            [half_spec] * 4 + [w_spec, w_spec, block((bf, dim), lambda n, *_: (n, 0))] + [ANY] * 7,
            [o_spec] * 3 + [ANY] * 2, [sds(o_shape)] * 3 + [sds(cat_shape)] * 2,
            (me, za, zb, ga, gb, w_gate, w_up, w_down, *near1, gcat1, dz_part0, mlp_part0),
            prefetch=1, scratch=[dma(4)], aliases={8 + i: i for i in range(5)},
            flops=12 * rows * dim * ffn, nbytes=6 * ffn * dim + 12 * rows * ffn)
        gcat1 = full1[4]
        dz_part1 = gated_grad(full1)
        dz1 = scatter(dz_part1)
        mlp_part1 = mlp_out(full1)
        part1 = scatter(mlp_part1)

        def weight_grads(x, ys, tokens, first=0, ni=None, prev=None):
            flat = lambda pair: [a.reshape(4 * rows, -1) for a in pair]
            xs, yf = flat(x), [a for y in ys for a in flat(y)]
            m, n = xs[0].shape[1], yf[0].shape[1]
            bm, by = 1024, 512
            extra = [prev] if prev is not None else []
            return run(
                functools.partial(weight_grads_kernel, len(ys), first, ni or m // bm), (),
                [ANY] * (2 + len(yf) + len(extra) + len(tokens)), [ANY] * len(ys), [sds((m, n), F32)] * len(ys),
                (*xs, *yf, *extra, *tokens), aliases={2 + len(yf): 0} if extra else None,
                scratch=[pltpu.VMEM((2, 4 * rows, bm), BF)] * 2 + [pltpu.VMEM((2, 4 * rows, by), BF)] * 2 + [pltpu.VMEM((2, bm, by), F32)]
                + [pltpu.SemaphoreType.DMA((2, 2))] * 2 + [pltpu.SemaphoreType.DMA((2, 1))],
                flops=16 * rows * (ni or m // bm) * bm * n * len(ys), nbytes=4 * m * n)

        down_args = (full0[0], full1[0]), ((gcat0, gcat1),)
        g_down = weight_grads(*down_args, (mlp_part1,), 0, 1)[0]

        d_resid, d_q, dkv_part, gn2 = run(
            attn_bwd_kernel, (batch,),
            [block((1, sl, dim), lambda b, *_: (jnp.minimum(b, half - 1), 0, 0)), block((1, sl, dim), lambda b, *_: (jnp.maximum(b - half, 0), 0, 0)),
             tok_spec, tok_spec, gain_spec] + wo_specs + [kv_spec] * 4 + [q_spec, pt_spec, rope_spec, rope_spec, ANY, ANY, ANY],
            [tok_spec, q_spec, kv4_spec, block((1, dim), lambda b, *_: (0, 0))],
            [sds((batch, sl, dim)), sds((batch, sl, qd)), sds((tp_n, batch, sl, 2 * hd)), sds((1, dim), F32)],
            (me, dz0, dz1, resid, grad_out, gain2, *wos, *kvs, q, pt, cos_t, sin_t, mlp_part1, g_down, part0), prefetch=1,
            scratch=[pltpu.VMEM((hd, seq), BF), pltpu.VMEM((seq, hd), BF), pltpu.VMEM((heads * sl, hd), BF), pltpu.VMEM((heads * sl, hd), BF), pltpu.VMEM((seq, heads * sl), BF), pltpu.VMEM((2, seq, sl), F32)],
            flops=2 * own * dim * qd + 8 * own * seq * qd, nbytes=2 * own * heads * seq)
        dkv = lax.psum_scatter(dkv_part, "tp", scatter_dimension=0)

        mixed2, dres2, u2, dq2 = mixed.reshape(own, qd), d_resid.reshape(own, dim), u.reshape(own, dim), d_q.reshape(own, qd)
        x_spec, y_spec = block((own, dim), lambda j, *_: (0, 0), True), lambda pick: block((own, cols), lambda j, *_: (0, pick(j)))
        g_out = run(
            block_grad_kernel, (tp_n,), [y_spec(lambda j: j), x_spec, ANY],
            block((1, cols, dim), lambda j, m: (m[0] ^ j, 0, 0)), sds((tp_n, cols, dim), F32), (me, mixed2, dres2, dkv_part),
            prefetch=1, flops=2 * own * dim * qd, nbytes=4 * dim * qd)
        g_out_sum = lax.psum_scatter(g_out, "tp", scatter_dimension=0)
        to_mate = run(
            block_grad_kernel, (2,), [x_spec, y_spec(lambda j: 1 + 2 * j), ANY],
            block((1, dim, cols), lambda j: (j, 0, 0)), sds((2, dim, cols), F32), (u2, dq2, g_out),
            flops=own * dim * qd, nbytes=2 * dim * qd)
        from_mate = to_core(to_mate)
        g_down = weight_grads(*down_args, (to_mate,), 1, ffn // 1024 - 1, g_down)[0]
        far_sum, own_sum = run(
            pair_grad_kernel, (2,), [x_spec, y_spec(lambda j: 2 - 2 * j), block((1, dim, cols), lambda j: (1 - j, 0, 0)), ANY],
            [block((1, dim, cols), lambda j: (0, 0, 0))] * 2, [sds((1, dim, cols), F32)] * 2, (u2, dq2, from_mate, g_down),
            flops=own * dim * qd, nbytes=2 * dim * qd)
        arrived = to_chip(far_sum)

        extra = dim // hd
        half_at = [block((1, sl, dim), lambda b, *_: (jnp.minimum(b, half - 1), 0, 0)), block((1, sl, dim), lambda b, *_: (jnp.maximum(b - half, 0), 0, 0))]
        grad_hidden, gkv, hidden_out = run(
            last_kernel, (batch,),
            [kv_spec, q_spec, tok_spec, tok_spec, tok_spec, gain_spec,
             ] + [ANY] * 6 + [rope_spec, rope_spec, const_spec((1, dim)), tok_spec, *half_at, ANY],
            [tok_spec, block((dim + extra, 2 * hd), lambda b, *_: (0, 0)), tok_spec],
            [sds((batch, sl, dim)), sds((dim + extra, 2 * hd), F32), sds((batch, sl, dim))],
            (me, dkv, d_q, u, hidden, d_resid, gain1, *wqs, w_key, w_value, cos_t, sin_t, gn2, resid, part0, part1, far_sum), prefetch=1,
            scratch=[pltpu.VMEM((1, dim), F32), pltpu.VMEM((dim, qd + 2 * hd), BF), pltpu.VMEM((sl, qd + 2 * hd), BF), dma(6)],
            flops=2 * own * dim * (qd + 4 * hd), nbytes=8 * own * dim)
        gkv = lax.psum(gkv, "tp")
        g_key, g_value = gkv[:dim, :hd], gkv[:dim, hd:]
        g_mlp_norm = gkv[dim : dim + extra // 2].reshape(dim)
        g_attn_norm = gkv[dim + extra // 2 :].reshape(dim)

        g_gate, g_up = weight_grads((full0[3], full1[3]), ((full0[1], full1[1]), (full0[2], full1[2])), (grad_hidden,))
        g_query_sum = own_sum[0] + tie(arrived, g_up)[0]
        return (hidden_out, grad_hidden, g_attn_norm, g_query_sum, g_key, g_value, g_out_sum, g_mlp_norm, g_gate, g_up, g_down)

    return jax.shard_map(local_layer, mesh=mesh, in_specs=in_specs, out_specs=out_specs, check_vma=False)
```

```python
import functools
import math

import jax
import jax.numpy as jnp
import numpy as np
from jax import lax
from jax.experimental import pallas as pl
from jax.experimental.pallas import tpu as pltpu
from jax.sharding import PartitionSpec as P


EPS = 1e-6
BF = jnp.bfloat16
F32 = jnp.float32
MIB = 1024 * 1024
ANY = pl.BlockSpec(memory_space=pl.ANY)


def dot_nn(a, b):
    return lax.dot_general(a, b, (((1,), (0,)), ((), ())), preferred_element_type=F32)


def dot_nt(a, b):
    return lax.dot_general(a, b, (((1,), (1,)), ((), ())), preferred_element_type=F32)


def dot_tn(a, b):
    return lax.dot_general(a, b, (((0,), (0,)), ((), ())), preferred_element_type=F32)


def const_spec(shape):
    zeros = (0,) * len(shape)
    return pl.BlockSpec(shape, lambda *_: zeros, pipeline_mode=pl.Buffered(1))


def run(kernel, grid, in_specs, out_specs, out_shape, args, scratch=(), prefetch=0, aliases=None, flops=0, nbytes=0, limit=60):
    spec = pltpu.PrefetchScalarGridSpec(num_scalar_prefetch=prefetch, grid=grid, in_specs=in_specs, out_specs=out_specs, scratch_shapes=scratch)
    return pl.pallas_call(
        kernel,
        grid_spec=spec,
        out_shape=out_shape,
        input_output_aliases=aliases or {},
        compiler_params=pltpu.CompilerParams(dimension_semantics=("arbitrary",) * len(grid), vmem_limit_bytes=limit * MIB),
        cost_estimate=pl.CostEstimate(flops=int(flops), bytes_accessed=int(nbytes), transcendentals=0),
    )(*args)


def rope_fwd(x, cos_t, sin_t):
    half = x.shape[-1] // 2
    a, b = x[:, :half], x[:, half:]
    return a * cos_t - b * sin_t, b * cos_t + a * sin_t


def rope_bwd(a, b, cos_t, sin_t):
    return a * cos_t + b * sin_t, b * cos_t - a * sin_t


def pre_kernel(me_ref, h_ref, gain_ref, wk_ref, wv_ref, cos_ref, sin_ref, u_ref, kv_ref):
    x = h_ref[0].astype(F32)
    inv = lax.rsqrt(jnp.mean(x * x, axis=-1, keepdims=True) + EPS)
    u = (x * inv * gain_ref[...]).astype(BF)
    u_ref[0] = u
    hd = wk_ref.shape[1]
    first, second = rope_fwd(dot_nn(u, wk_ref[...]), cos_ref[...], sin_ref[...])
    kv_ref[0, :, : hd // 2] = first.astype(BF)
    kv_ref[0, :, hd // 2 : hd] = second.astype(BF)
    kv_ref[0, :, hd:] = dot_nn(u, wv_ref[...]).astype(BF)


def attn_fwd_kernel(me_ref, pre_ref, val_ref, u_ref, w0_ref, w1_ref, w2_ref, w3_ref, k0_ref, k1_ref, k2_ref, k3_ref, cos_ref, sin_ref, token_ref,
                    q_ref, pt_ref, mix_ref, keys_ref, vt_ref, s_ref):
    b = pl.program_id(0)
    cols = w0_ref.shape[1]
    _, hd = keys_ref.shape
    sl = u_ref.shape[1]
    heads = q_ref.shape[2] // hd
    u = u_ref[0]
    me = me_ref[0]
    cos_t, sin_t = cos_ref[...], sin_ref[...]
    place = []
    for r, kv_ref in enumerate((k0_ref, k1_ref, k2_ref, k3_ref)):
        keys_ref[r * sl : (r + 1) * sl, :] = kv_ref[0, :, :hd]
        vt_ref[:, r * sl : (r + 1) * sl] = kv_ref[0, :, hd:].astype(F32).T.astype(BF)
        place.append(lax.broadcasted_iota(jnp.int32, (sl, sl), 0) + (me ^ r) * sl)
    for r, w_ref in enumerate((w0_ref, w1_ref, w2_ref, w3_ref)):
        qs = dot_nn(u, w_ref[...])
        for j in range(cols // hd):
            base = r * cols + j * hd
            first, second = rope_fwd(qs[:, j * hd : (j + 1) * hd], cos_t, sin_t)
            q_ref[0, :, base : base + hd // 2] = first.astype(BF)
            q_ref[0, :, base + hd // 2 : base + hd] = second.astype(BF)
    prefix, valid = pre_ref[b], val_ref[b]
    q_end = lax.broadcasted_iota(jnp.int32, (1, sl), 1) + (me * sl + 1)
    limit = jnp.minimum(valid, jnp.maximum(prefix, q_end))
    visible = jnp.concatenate(place, axis=0) < limit
    scale = (hd**-0.5) * math.log2(math.e)

    def scores(h):
        return dot_nt(keys_ref[...], q_ref[0, :, h * hd : (h + 1) * hd])

    s_ref[0] = scores(0)
    for h in range(heads):
        if h + 1 < heads:
            s_ref[(h + 1) % 2] = scores(h + 1)
        sc = jnp.where(visible, s_ref[h % 2], -1e30)
        top = jnp.max(sc, axis=0, keepdims=True)
        e = jnp.exp2((sc - top) * scale)
        p = (e * (1.0 / jnp.sum(e, axis=0, keepdims=True))).astype(BF)
        pt_ref[0, :, h * sl : (h + 1) * sl] = p
        mix_ref[0, :, h * hd : (h + 1) * hd] = dot_nn(vt_ref[...], p).T.astype(BF)


def fetch_at_first(refs, dst, axis, sems):
    @pl.when(pl.program_id(0) == 0)
    def _():
        at, copies = 0, []
        for i, ref in enumerate(refs):
            n = ref.shape[axis]
            copies.append(pltpu.make_async_copy(ref, dst.at[pl.ds(at, n), :] if axis == 0 else dst.at[:, pl.ds(at, n)], sems.at[i]))
            at += n
        for c in copies:
            c.start()
        for c in copies:
            c.wait()


def out_kernel(mix_ref, w0_ref, w1_ref, w2_ref, w3_ref, h_ref, gain_ref, *rest):
    resid_ref, z_ref, wo_ref, sems = rest[-4:]
    fetch_at_first((w0_ref, w1_ref, w2_ref, w3_ref), wo_ref, 0, sems)
    x = (h_ref[0].astype(F32) + dot_nn(mix_ref[0], wo_ref[...])).astype(BF)
    resid_ref[0] = x
    x = x.astype(F32)
    inv = lax.rsqrt(jnp.mean(x * x, axis=-1, keepdims=True) + EPS)
    z_ref[0] = (x * inv * gain_ref[...]).astype(BF)


class Flow:
    def __init__(self, bufs, sems, inward, sides):
        self.bufs, self.sems, self.inward, self.sides = bufs, sems, inward, sides

    def copies(self, t, slot, only):
        out = []
        for i, (hbm, buf) in enumerate(zip(self.sides(t), self.bufs)):
            if only is None or i == only:
                pair = (hbm, buf.at[slot]) if self.inward else (buf.at[slot], hbm)
                out.append(pltpu.make_async_copy(*pair, self.sems.at[slot, i]))
        return out

    def start(self, t, slot, only=None):
        for c in self.copies(t, slot, only):
            c.start()

    def wait(self, t, slot, only=None):
        for c in self.copies(t, slot, only):
            c.wait()


def local_copies(pairs, sems):
    return [pltpu.make_async_copy(src, dst, sems.at[i]) for i, (src, dst) in enumerate(pairs)]


def start_all(copies):
    for c in copies:
        c.start()


def wait_all(copies):
    for c in copies:
        c.wait()


def span(t, n):
    return pl.ds(pl.multiple_of(t * n, n), n)


OWN, MATE, FAR = 0, 1, 2


def dact_kernel(kind, me_ref, *refs):
    n_in, n_out = (2, 2) if kind == FAR else (1, 5 if kind == OWN else 3)
    gs, wd_ref = refs[:n_in], refs[n_in]
    outs, (wb, ob, gv, w_sem, o_sem, g_sem, c_sem) = refs[-7 - n_out : -7], refs[-7:]
    da_ref, homes = outs[0], outs[1:]
    half = gv.shape[0] // 2
    chip, core = me_ref[0] // 2, me_ref[0] % 2
    halves = [gv.at[pl.ds(c * half, half)] for c in range(2)]
    if kind == FAR:
        loads = local_copies(zip(gs, halves), g_sem)
        puts = [(halves[0], homes[0].at[1 - chip, core]), (halves[1], homes[0].at[1 - chip, 1 - core])]
    else:
        loads = local_copies([(gs[0], gv)], g_sem)
        puts = [(halves[c], homes[c].at[chip, core if kind == OWN else 1 - core]) for c in range(2)]
        puts += list(zip(halves, homes[2:]))
    puts = local_copies(puts, c_sem)
    bn = ob.shape[-1]
    steps = wd_ref.shape[0] // bn
    w_flow = Flow((wb,), w_sem, True, lambda t: (wd_ref.at[span(t, bn)],))
    o_flow = Flow((ob,), o_sem, False, lambda t: (da_ref.at[:, :, span(t, bn)],))
    start_all(loads)
    w_flow.start(0, 0)
    wait_all(loads)
    start_all(puts)

    @pl.loop(0, steps)
    def _(t):
        slot = lax.rem(t, 2)

        @pl.when(t + 1 < steps)
        def _():
            w_flow.start(t + 1, 1 - slot)

        @pl.when(t >= 2)
        def _():
            o_flow.wait(t - 2, slot)

        w_flow.wait(t, slot)
        g = gv[...].reshape(2 * half * gv.shape[1], gv.shape[2])
        ob[slot] = dot_nt(g, wb[slot]).astype(BF).reshape(ob.shape[1:])
        o_flow.start(t, slot)

    for t in (steps - 2, steps - 1):
        o_flow.wait(t, t % 2)
    wait_all(puts)


def gated(gate, up, da):
    c0 = math.sqrt(2.0 / math.pi)
    c1 = c0 * 0.044715
    x2 = gate * gate
    hh = 0.5 + 0.5 * jnp.tanh(gate * (c0 + c1 * x2))
    gelu = gate * hh
    slope = hh + gelu * ((1.0 - hh) * (2.0 * c0 + 6.0 * c1 * x2))
    return (gelu * up).astype(BF), (da * up * slope).astype(BF), (da * gelu).astype(BF)


def mlp_kernel(other, at, fused, me_ref, *refs):
    za, zb, da, db, wg_ref, wu_ref = refs[:6]
    n_out, n_scr = (5, 13) if fused else (4, 11)
    outs, scr = refs[-n_scr - n_out : -n_scr], refs[-n_scr:]
    zv, wgb, wub, act_b, dg_b, du_b, in_sem, o_sem, z_sem, c_sem = scr[:10]
    chip = abs(other - me_ref[0] // 2)
    core = me_ref[0] % 2
    rows, bn = act_b.shape[2:]
    dim = zv.shape[-1]
    steps = wg_ref.shape[1] // bn
    if fused:
        wdb, gv, g_sem = scr[10:]
        wd_ref = refs[6]
        in_flow = Flow((wgb, wub, wdb), in_sem, True, lambda t: (wg_ref.at[:, span(t, bn)], wu_ref.at[:, span(t, bn)], wd_ref.at[span(t, bn)]))
    else:
        dv = scr[10]
        in_flow = Flow((wgb, wub, dv.at[:, 0], dv.at[:, 1]), in_sem, True,
                       lambda t: (wg_ref.at[:, span(t, bn)], wu_ref.at[:, span(t, bn)], da.at[at[0], :, span(t, bn)], db.at[at[1], :, span(t, bn)]))
    bufs = (act_b, dg_b, du_b)
    o_flow = Flow([b.at[:, rel] for rel in range(2) for b in bufs], o_sem, False,
                  lambda t: [o.at[chip, abs(rel - core), :, span(t, bn)] for rel in range(2) for o in outs[:3]])
    loads = local_copies([(za, zv.at[0]), (zb, zv.at[1])], z_sem)
    puts = [(zv.at[0], outs[3].at[chip, core]), (zv.at[1], outs[3].at[chip, 1 - core])]
    if fused:
        loads += local_copies([(da, gv.at[0]), (db, gv.at[1])], g_sem)
        puts += [(gv.at[0], outs[4].at[chip, core]), (gv.at[1], outs[4].at[chip, 1 - core])]
    puts = local_copies(puts, c_sem)
    in_flow.start(0, 0)
    start_all(loads)
    wait_all(loads)
    start_all(puts)
    n = rows // (3 if fused else 2)

    @pl.loop(0, steps)
    def _(t):
        slot = lax.rem(t, 2)

        @pl.when(t + 1 < steps)
        def _():
            in_flow.start(t + 1, 1 - slot)

        @pl.when(t >= 2)
        def _():
            o_flow.wait(t - 2, slot)

        in_flow.wait(t, slot)
        for rel in range(2):
            z = zv[rel].reshape(rows, dim)
            for r in range(0, rows, n):
                gate, up = dot_nn(z[r : r + n], wgb[slot]), dot_nn(z[r : r + n], wub[slot])
                if fused:
                    d = dot_nt(gv[rel].reshape(rows, dim)[r : r + n], wdb[slot])
                else:
                    d = dv[slot, rel, r : r + n, :].astype(F32)
                for buf, o in zip(bufs, gated(gate, up, d)):
                    buf[slot, rel, r : r + n, :] = o
        o_flow.start(t, slot)

    for t in (steps - 2, steps - 1):
        o_flow.wait(t, t % 2)
    wait_all(puts)


def attn_bwd_kernel(me_ref, dz0_ref, dz1_ref, res_ref, go_ref, gain_ref, w0_ref, w1_ref, w2_ref, w3_ref, k0_ref, k1_ref, k2_ref, k3_ref,
                    q_ref, pt_ref, cos_ref, sin_ref, token0_ref, token1_ref, token2_ref,
                    dres_ref, dq_ref, dkv_ref, gn_ref, kt_ref, v_ref, do_ref, qs_ref, ds_ref, dp_ref, dk_ref, dv_ref):
    b = pl.program_id(0)
    half = pl.num_programs(0) // 2
    seq, hd = v_ref.shape
    sl = q_ref.shape[1]
    heads = q_ref.shape[2] // hd
    me = me_ref[0]
    x = res_ref[0].astype(F32)
    dz = jnp.where(b < half, dz0_ref[0], dz1_ref[0]).astype(F32)
    inv = lax.rsqrt(jnp.mean(x * x, axis=-1, keepdims=True) + EPS)
    xn = x * inv
    part = jnp.sum(dz * xn, axis=0, keepdims=True)

    @pl.when(b == 0)
    def _():
        gn_ref[...] = part

    @pl.when(b > 0)
    def _():
        gn_ref[...] += part

    dxn = dz * gain_ref[...]
    dx = inv * (dxn - xn * jnp.mean(dxn * xn, axis=-1, keepdims=True))
    dres = (go_ref[0].astype(F32) + dx).astype(BF)
    dres_ref[0] = dres
    scale = hd**-0.5
    for r, kv_ref in enumerate((k0_ref, k1_ref, k2_ref, k3_ref)):
        kt_ref[:, r * sl : (r + 1) * sl] = (kv_ref[0, :, :hd].astype(F32) * scale).T.astype(BF)
        v_ref[r * sl : (r + 1) * sl, :] = kv_ref[0, :, hd:]
    w_refs = (w0_ref, w1_ref, w2_ref, w3_ref)
    per = w0_ref.shape[0] // hd

    def d_mixed(r):
        dm = dot_nt(dres, w_refs[r][...]).astype(BF)
        for j in range(per):
            h = r * per + j
            do_ref[h * sl : (h + 1) * sl, :] = dm[:, j * hd : (j + 1) * hd]
            qs_ref[h * sl : (h + 1) * sl, :] = (q_ref[0, :, h * hd : (h + 1) * hd].astype(F32) * scale).astype(BF)

    cos_t, sin_t = cos_ref[...], sin_ref[...]

    def dprobs(h):
        return dot_nt(v_ref[...], do_ref[h * sl : (h + 1) * sl, :])

    def add_kv(r, first):
        at = pl.ds(r * per * sl, per * sl)
        dk, dv = dot_nn(ds_ref[:, at], qs_ref[at, :]), dot_nn(pt_ref[0, :, at], do_ref[at, :])
        if first:
            dk_ref[...], dv_ref[...] = dk, dv
        else:
            dk_ref[...] += dk
            dv_ref[...] += dv

    d_mixed(0)
    dp_ref[0] = dprobs(0)
    for h in range(heads):
        if h % per == 0:
            if h // per + 1 < len(w_refs):
                d_mixed(h // per + 1)
            if h:
                add_kv(h // per - 1, h == per)
        if h + 1 < heads:
            dp_ref[(h + 1) % 2] = dprobs(h + 1)
        p = pt_ref[0, :, h * sl : (h + 1) * sl].astype(F32)
        t = p * dp_ref[h % 2]
        ds = (t - p * jnp.sum(t, axis=0, keepdims=True)).astype(BF)
        ds_ref[:, h * sl : (h + 1) * sl] = ds
        dq = dot_nn(kt_ref[...], ds).T
        first, second = rope_bwd(dq[:, : hd // 2], dq[:, hd // 2 :], cos_t, sin_t)
        dq_ref[0, :, h * hd : h * hd + hd // 2] = first.astype(BF)
        dq_ref[0, :, h * hd + hd // 2 : (h + 1) * hd] = second.astype(BF)
    at = pl.ds((heads - per) * sl, per * sl)
    dk = (dk_ref[...] + dot_nn(ds_ref[:, at], qs_ref[at, :])).astype(BF)
    dv = (dv_ref[...] + dot_nn(pt_ref[0, :, at], do_ref[at, :])).astype(BF)
    for r in range(seq // sl):
        dkv_ref[me ^ r, 0, :, :hd] = dk[r * sl : (r + 1) * sl]
        dkv_ref[me ^ r, 0, :, hd:] = dv[r * sl : (r + 1) * sl]


def last_kernel(me_ref, dkv_ref, dq_ref, u_ref, h_ref, dres_ref, gain_ref, w0_ref, w1_ref, w2_ref, w3_ref, wk_ref, wv_ref, cos_ref, sin_ref, gm_ref,
                res_ref, p0_ref, p1_ref, token0_ref, gh_ref, gkv_ref, ho_ref, acc_ref, w_ref, d_ref, sems):
    b = pl.program_id(0)
    dim, hd = wk_ref.shape
    qd = dq_ref.shape[2]
    fetch_at_first((w0_ref, w1_ref, w2_ref, w3_ref, wk_ref, wv_ref), w_ref, 1, sems)
    half = pl.num_programs(0) // 2
    ho_ref[0] = (res_ref[0].astype(F32) + jnp.where(b < half, p0_ref[0], p1_ref[0]).astype(F32)).astype(BF)
    raw = dkv_ref[0]
    dk = raw[:, :hd].astype(F32)
    first, second = rope_bwd(dk[:, : hd // 2], dk[:, hd // 2 :], cos_ref[...], sin_ref[...])
    d_ref[:, :qd] = dq_ref[0]
    d_ref[:, qd : qd + hd // 2] = first.astype(BF)
    d_ref[:, qd + hd // 2 : qd + hd] = second.astype(BF)
    d_ref[:, qd + hd :] = raw[:, hd:]
    dn = dot_nt(d_ref[...], w_ref[...])
    gk = dot_tn(u_ref[0], d_ref[:, qd:])
    x = h_ref[0].astype(F32)
    inv = lax.rsqrt(jnp.mean(x * x, axis=-1, keepdims=True) + EPS)
    xn = x * inv
    part = jnp.sum(dn * xn, axis=0, keepdims=True)
    dxn = dn * gain_ref[...]
    dx = inv * (dxn - xn * jnp.mean(dxn * xn, axis=-1, keepdims=True))
    gh_ref[0] = (dres_ref[0].astype(F32) + dx).astype(BF)

    @pl.when(b == 0)
    def _():
        acc_ref[...] = part
        gkv_ref[:dim, :] = gk

    @pl.when(b > 0)
    def _():
        acc_ref[...] += part
        gkv_ref[:dim, :] += gk

    @pl.when(b == pl.num_programs(0) - 1)
    def _():
        width = 2 * hd
        per = dim // width
        for i in range(per):
            gkv_ref[dim + i : dim + i + 1, :] = gm_ref[:, i * width : (i + 1) * width]
            gkv_ref[dim + per + i : dim + per + i + 1, :] = acc_ref[:, i * width : (i + 1) * width]


def block_grad_kernel(*refs):
    x_ref, y_ref, o_ref = refs[-4], refs[-3], refs[-1]
    o_ref[...] = dot_tn(x_ref[...], y_ref[...]).reshape(o_ref.shape)


def pair_grad_kernel(x_ref, y_ref, add_ref, token_ref, far_ref, own_ref):
    out = dot_tn(x_ref[...], y_ref[...]) + add_ref[0]

    @pl.when(pl.program_id(0) == 0)
    def _():
        far_ref[0] = out

    @pl.when(pl.program_id(0) == 1)
    def _():
        own_ref[0] = out


def gated_grad_kernel(dg_ref, du_ref, wg_ref, wu_ref, *rest):
    o_ref, a1, a2, b1, b2, ob, a_sem, b_sem, o_sem = rest[-9:]
    ni = dg_ref.shape[0] * dg_ref.shape[1]
    bn = b1.shape[1]
    nj = wg_ref.shape[0] // bn
    steps = ni * nj
    cols = lambda t: pl.ds(pl.multiple_of(lax.rem(t, nj) * bn, bn), bn)
    a_flow = Flow((a1, a2), a_sem, True, lambda i: (dg_ref.at[i // 2, i % 2], du_ref.at[i // 2, i % 2]))
    b_flow = Flow((b1, b2), b_sem, True, lambda t: (wg_ref.at[cols(t)], wu_ref.at[cols(t)]))
    o_flow = Flow((ob,), o_sem, False, lambda t: (o_ref.at[t // nj, :, cols(t)],))
    for k in range(2):
        a_flow.start(0, 0, k)
        b_flow.start(0, 0, k)
    b_flow.start(1, 1)
    a_flow.start(1, 1)
    for k in range(2):
        a_flow.wait(0, 0, k)
        b_flow.wait(0, 0, k)
        if k == 0:
            first = dot_nt(a1[0], b1[0])
    ob[0] = (first + dot_nt(a2[0], b2[0])).astype(BF)
    o_flow.start(0, 0)

    @pl.loop(1, steps)
    def _(t):
        i, slot = t // nj, lax.rem(t, 2)
        a_slot = lax.rem(i, 2)

        @pl.when(t + 1 < steps)
        def _():
            b_flow.start(t + 1, 1 - slot)

        @pl.when(lax.rem(t, nj) == 0)
        def _():
            a_flow.wait(i, a_slot)

            @pl.when(i + 1 < ni)
            def _():
                a_flow.start(i + 1, 1 - a_slot)

        @pl.when(t >= 2)
        def _():
            o_flow.wait(t - 2, slot)

        b_flow.wait(t, slot)
        ob[slot] = (dot_nt(a1[a_slot], b1[slot]) + dot_nt(a2[a_slot], b2[slot])).astype(BF)
        o_flow.start(t, slot)

    for t in (steps - 2, steps - 1):
        o_flow.wait(t, t % 2)


def weight_grads_kernel(count, first, ni, *refs):
    x_refs, y_refs = refs[:2], refs[2 : 2 + 2 * count]
    o_refs, (x0, x1, y0, y1, ob, x_sem, y_sem, o_sem) = refs[-8 - count : -8], refs[-8:]
    bm, bn = ob.shape[1:]
    nj = y_refs[0].shape[1] // bn
    steps = ni * count * nj
    per = count * nj
    rows = lambda i: pl.ds(pl.multiple_of((first + i) * bm, bm), bm)
    cols = lambda t: pl.ds(pl.multiple_of(lax.rem(t, nj) * bn, bn), bn)
    x_flow = Flow((x0, x1), x_sem, True, lambda i: [r.at[:, rows(i)] for r in x_refs])
    y_flows = [Flow((y0, y1), y_sem, True, lambda t, k=k: [r.at[:, cols(t)] for r in y_refs[2 * k : 2 * k + 2]]) for k in range(count)]
    o_flows = [Flow((ob,), o_sem, False, lambda t, k=k: (o_refs[k].at[rows(t // per), cols(t)],)) for k in range(count)]

    def each(flows, t, act):
        if count == 1:
            act(flows[0])
        else:
            which = lax.rem(t // nj, count)
            for k in range(count):
                pl.when(which == k)(functools.partial(act, flows[k]))

    for k in range(2):
        x_flow.start(0, 0, k)
        y_flows[0].start(0, 0, k)
    y_flows[0].start(1, 1)
    if ni > 1:
        x_flow.start(1, 1)
    for k in range(2):
        x_flow.wait(0, 0, k)
        y_flows[0].wait(0, 0, k)
        if k == 0:
            part = dot_tn(x0[0], y0[0])
    ob[0] = part + dot_tn(x1[0], y1[0])
    o_flows[0].start(0, 0)

    @pl.loop(1, steps)
    def _(t):
        i, slot = t // per, lax.rem(t, 2)
        x_slot = lax.rem(i, 2)

        @pl.when(t + 1 < steps)
        def _():
            each(y_flows, t + 1, lambda f: f.start(t + 1, 1 - slot))

        @pl.when(lax.rem(t, per) == 0)
        def _():
            x_flow.wait(i, x_slot)

            @pl.when(i + 1 < ni)
            def _():
                x_flow.start(i + 1, 1 - x_slot)

        @pl.when(t >= 2)
        def _():
            o_flows[0].wait(t - 2, slot)

        y_flows[0].wait(t, slot)
        ob[slot] = dot_tn(x0[x_slot], y0[slot]) + dot_tn(x1[x_slot], y1[slot])
        each(o_flows, t, lambda f: f.start(t, slot))

    for t in (steps - 2, steps - 1):
        o_flows[0].wait(t, t % 2)


def tie_kernel(x_ref, *rest):
    del x_ref, rest


def tie(x, *tokens):
    return pl.pallas_call(
        tie_kernel,
        name="tie",
        in_specs=[ANY] * (1 + len(tokens)),
        out_specs=ANY,
        out_shape=jax.ShapeDtypeStruct(x.shape, x.dtype),
        input_output_aliases={0: 0},
    )(x, *tokens)


def solution(mesh):
    act_spec = P("dp", "tp", None)
    in_specs = (act_spec, act_spec, P("dp"), P("dp"), P(None), P(None, "tp"), P(None, None), P(None, None), P("tp", None), P(None), P(None, "tp"), P(None, "tp"), P("tp", None))
    out_specs = (act_spec, act_spec, P("dp"), P("dp", "tp"), P("dp", None), P("dp", None), P(("dp", "tp"), None), P("dp"), P("dp", "tp"), P("dp", "tp"), P(("dp", "tp"), None))
    core_flip = [(0, 1), (1, 0), (2, 3), (3, 2)]
    chip_flip = [(0, 2), (2, 0), (1, 3), (3, 1)]

    def to_core(x):
        return lax.ppermute(x, "tp", core_flip)

    def to_chip(x):
        return lax.ppermute(x, "tp", chip_flip)

    def local_layer(hidden, grad_out, prefix_len, valid_len, attn_norm, w_query, w_key, w_value, w_out, mlp_norm, w_gate, w_up, w_down):
        batch, sl, dim = hidden.shape
        half = batch // 2
        rows = half * sl
        hd = w_key.shape[1]
        cols = w_query.shape[1]
        tp_n = mesh.shape["tp"]
        seq = sl * tp_n
        qd = cols * tp_n
        heads = qd // hd
        ffn = w_gate.shape[1]
        own = batch * sl
        me = lax.axis_index("tp").astype(jnp.int32).reshape(1)

        inv_freq = np.exp(np.arange(hd // 2, dtype=np.float32) * np.float32(2.0 / hd) * np.float32(-math.log(10000.0)))
        angles = np.arange(seq, dtype=np.float32)[:, None] * inv_freq[None, :]
        cos_t, sin_t = jnp.asarray(np.cos(angles)), jnp.asarray(np.sin(angles))
        gain1 = (1.0 + attn_norm.astype(F32)).reshape(1, dim)
        gain2 = (1.0 + mlp_norm.astype(F32)).reshape(1, dim)

        def sds(shape, dtype=BF):
            return jax.ShapeDtypeStruct(shape, dtype)

        def block(shape, at, single=False):
            return pl.BlockSpec(shape, at, pipeline_mode=pl.Buffered(1) if single else None)

        tok_spec = block((1, sl, dim), lambda b, *_: (b, 0, 0))
        q_spec = block((1, sl, qd), lambda b, *_: (b, 0, 0))
        kv_spec = block((1, sl, 2 * hd), lambda b, *_: (b, 0, 0))
        kv4_spec = block((tp_n, 1, sl, 2 * hd), lambda b, *_: (0, b, 0, 0))
        pt_spec = block((1, seq, heads * sl), lambda b, *_: (b, 0, 0))
        rope_spec = block((sl, hd // 2), lambda b, m, *_: (m[0], 0), True)
        gain_spec = const_spec((1, dim))
        dma = lambda n: pltpu.SemaphoreType.DMA((n,))

        wq_far = to_chip(w_query)
        wq_mate = to_core(w_query)
        g_mate = to_core(grad_out)
        u, kv = run(
            pre_kernel, (batch,),
            [tok_spec, gain_spec, const_spec((dim, hd)), const_spec((dim, hd)), rope_spec, rope_spec],
            [tok_spec, kv_spec], [sds((batch, sl, dim)), sds((batch, sl, 2 * hd))],
            (me, hidden, gain1, w_key, w_value, cos_t, sin_t), prefetch=1,
            flops=4 * own * dim * hd, nbytes=6 * own * dim)
        kv_far = to_chip(kv)
        kv_mate = to_core(kv)
        wo_far = to_chip(w_out)
        wo_mate = to_core(w_out)

        bn = 512
        cat_shape = (2, 2, half, sl, dim)
        SMEM = pl.BlockSpec(memory_space=pltpu.SMEM)
        pair = (2, rows, bn)

        def dact(kind, gs, homes, tokens, n_out):
            return run(
                functools.partial(dact_kernel, kind), (), [SMEM] + [ANY] * (len(gs) + 1 + len(homes) + len(tokens)), [ANY] * n_out,
                ([sds((2, rows, ffn))] + [sds(cat_shape)] * 2 + [sds((half, sl, dim))] * 2)[: n_out],
                (me, *gs, w_down, *homes, *tokens), aliases={2 + len(gs) + i: 1 + i for i in range(len(homes))},
                scratch=[pltpu.VMEM((2, bn, dim), BF), pltpu.VMEM((2,) + pair, BF), pltpu.VMEM((batch, sl, dim), BF),
                         pltpu.SemaphoreType.DMA((2, 1)), pltpu.SemaphoreType.DMA((2, 1)), dma(2), dma(4)],
                flops=4 * rows * dim * ffn, nbytes=2 * ffn * dim + 4 * rows * ffn)

        da_own, gcat0, gcat1, go0, go1 = dact(OWN, (grad_out,), (), (kv,), 5)
        wq_far = tie(wq_far, da_own)
        wq_far_mate = to_core(wq_far)
        da_mate, gcat0, gcat1 = dact(MATE, (g_mate,), (gcat0, gcat1), (da_own,), 3)
        kv_far = tie(kv_far, da_mate)
        kv_far_mate = to_core(kv_far)
        wqs = (w_query, wq_mate, wq_far, wq_far_mate)
        kvs = (kv, kv_mate, kv_far, kv_far_mate)
        wq_specs = [const_spec((dim, cols))] * 4
        wo_specs = [const_spec((cols, dim))] * 4

        q, pt, mixed = run(
            attn_fwd_kernel, (batch,),
            [tok_spec] + wq_specs + [kv_spec] * 4 + [rope_spec, rope_spec, ANY],
            [q_spec, pt_spec, q_spec],
            [sds((batch, sl, qd)), sds((batch, seq, heads * sl)), sds((batch, sl, qd))],
            (me, prefix_len, valid_len, u, *wqs, *kvs, cos_t, sin_t, da_mate), prefetch=3,
            scratch=[pltpu.VMEM((seq, hd), BF), pltpu.VMEM((hd, seq), BF), pltpu.VMEM((2, seq, sl), F32)],
            flops=2 * own * dim * qd + 4 * own * seq * qd, nbytes=2 * own * heads * seq)
        wo_far = tie(wo_far, mixed)
        wo_far_mate = to_core(wo_far)
        wos = (w_out, wo_mate, wo_far, wo_far_mate)

        g_far = [to_chip(tie(go0, mixed))]

        def out_proj(c, prev):
            at = lambda b: (b + c * half, 0, 0)
            extra = [prev] if c else []
            return run(
                out_kernel, (half,),
                [block((1, sl, qd), at)] + [ANY] * 4 + [block((1, sl, dim), at), gain_spec] + [ANY] * len(extra),
                [block((1, sl, dim), at), block((1, sl, dim), lambda b: (b, 0, 0))],
                [sds((batch, sl, dim)), sds((half, sl, dim))],
                (mixed, *wos, hidden, gain2, *extra), aliases={7: 0} if c else None,
                scratch=[pltpu.VMEM((qd, dim), BF), dma(4)],
                flops=own * dim * qd, nbytes=4 * own * dim)

        resid, z0 = out_proj(0, None)
        resid, z1 = out_proj(1, resid)
        zs = [z0, z1]
        z_mate = [to_core(z) for z in zs]
        z_far = [to_chip(z0)]
        z_far.append(to_chip(z1))
        g_far.append(to_chip(tie(go1, z1)))

        o_shape = (2, 2, rows, ffn)

        def mlp(other, at, fused, za, zb, da, db, prev, tokens):
            n_out = 5 if fused else 4
            weights = (w_gate, w_up, w_down) if fused else (w_gate, w_up)
            sem = lambda k, n: pltpu.SemaphoreType.DMA((k, n))
            scratch = [pltpu.VMEM((2, half, sl, dim), BF)] + [pltpu.VMEM((2, dim, bn), BF)] * 2 + [pltpu.VMEM((2, 2, rows, bn), BF)] * 3
            scratch += [sem(2, 3 if fused else 4), sem(2, 6), dma(2), dma(4)]
            scratch += [pltpu.VMEM((2, bn, dim), BF), pltpu.VMEM((2, half, sl, dim), BF), dma(2)] if fused else [pltpu.VMEM((2, 2, rows, bn), BF)]
            return run(
                functools.partial(mlp_kernel, other, at, fused), (),
                [SMEM] + [ANY] * (4 + len(weights) + len(prev) + len(tokens)), [ANY] * n_out,
                [sds(o_shape)] * 3 + [sds(cat_shape)] * (n_out - 3),
                (me, za, zb, da, db, *weights, *prev, *tokens), scratch=scratch,
                aliases={5 + len(weights) + i: i for i in range(len(prev))},
                flops=(12 if fused else 8) * rows * dim * ffn, nbytes=4 * ffn * dim + 16 * rows * ffn)

        near0 = mlp(0, (0, 0), False, zs[0], z_mate[0], da_own, da_mate, (), (z1,))
        near1 = mlp(0, (1, 1), False, zs[1], z_mate[1], da_own, da_mate, (), (near0[0],))

        ga = tie(g_far[0], near0[0])
        gb = to_core(ga)
        da_far, gcat0 = dact(FAR, (ga, gb), (gcat0,), (near1[0],), 2)
        za = tie(z_far[0], near1[0])
        zb = to_core(za)
        full0 = mlp(1, (0, 1), False, za, zb, da_far, da_far, near0, ())

        def gated_grad(full):
            bj = 512
            return run(
                gated_grad_kernel, (), [ANY] * 5, ANY, sds((4, rows, dim)), (full[1], full[2], w_gate, w_up, full[0]),
                scratch=[pltpu.VMEM((2, rows, ffn), BF)] * 2 + [pltpu.VMEM((2, bj, ffn), BF)] * 2 + [pltpu.VMEM((2, rows, bj), BF)]
                + [pltpu.SemaphoreType.DMA((2, 2))] * 2 + [pltpu.SemaphoreType.DMA((2, 1))],
                flops=16 * rows * dim * ffn, nbytes=16 * rows * ffn)

        def mlp_out(full):
            return dot_nn(full[0].reshape(4 * rows, ffn), w_down).astype(BF)

        def scatter(x):
            return lax.psum_scatter(x.reshape(tp_n, rows, dim), "tp", scatter_dimension=0).reshape(half, sl, dim)

        dz_part0 = gated_grad(full0)
        dz0 = scatter(dz_part0)
        mlp_part0 = mlp_out(full0)
        part0 = scatter(mlp_part0)

        ga, za = tie(g_far[1], full0[0]), tie(z_far[1], full0[0])
        gb = to_core(ga)
        zb = to_core(za)
        full1 = mlp(1, None, True, za, zb, ga, gb, (*near1, gcat1), (dz_part0, mlp_part0))
        gcat1 = full1[4]
        dz_part1 = gated_grad(full1)
        dz1 = scatter(dz_part1)
        mlp_part1 = mlp_out(full1)
        part1 = scatter(mlp_part1)

        def weight_grads(x, ys, tokens, first=0, ni=None, prev=None):
            flat = lambda pair: [a.reshape(4 * rows, -1) for a in pair]
            xs, yf = flat(x), [a for y in ys for a in flat(y)]
            m, n = xs[0].shape[1], yf[0].shape[1]
            bm, by = 1024, 512
            extra = [prev] if prev is not None else []
            return run(
                functools.partial(weight_grads_kernel, len(ys), first, ni or m // bm), (),
                [ANY] * (2 + len(yf) + len(extra) + len(tokens)), [ANY] * len(ys), [sds((m, n), F32)] * len(ys),
                (*xs, *yf, *extra, *tokens), aliases={2 + len(yf): 0} if extra else None,
                scratch=[pltpu.VMEM((2, 4 * rows, bm), BF)] * 2 + [pltpu.VMEM((2, 4 * rows, by), BF)] * 2 + [pltpu.VMEM((2, bm, by), F32)]
                + [pltpu.SemaphoreType.DMA((2, 2))] * 2 + [pltpu.SemaphoreType.DMA((2, 1))],
                flops=16 * rows * (ni or m // bm) * bm * n * len(ys), nbytes=4 * m * n)

        down_args = (full0[0], full1[0]), ((gcat0, gcat1),)
        g_down = weight_grads(*down_args, (mlp_part1,), 0, 1)[0]

        d_resid, d_q, dkv_part, gn2 = run(
            attn_bwd_kernel, (batch,),
            [block((1, sl, dim), lambda b, *_: (jnp.minimum(b, half - 1), 0, 0)), block((1, sl, dim), lambda b, *_: (jnp.maximum(b - half, 0), 0, 0)),
             tok_spec, tok_spec, gain_spec] + wo_specs + [kv_spec] * 4 + [q_spec, pt_spec, rope_spec, rope_spec, ANY, ANY, ANY],
            [tok_spec, q_spec, kv4_spec, block((1, dim), lambda b, *_: (0, 0))],
            [sds((batch, sl, dim)), sds((batch, sl, qd)), sds((tp_n, batch, sl, 2 * hd)), sds((1, dim), F32)],
            (me, dz0, dz1, resid, grad_out, gain2, *wos, *kvs, q, pt, cos_t, sin_t, mlp_part1, g_down, part0), prefetch=1,
            scratch=[pltpu.VMEM((hd, seq), BF), pltpu.VMEM((seq, hd), BF), pltpu.VMEM((heads * sl, hd), BF), pltpu.VMEM((heads * sl, hd), BF), pltpu.VMEM((seq, heads * sl), BF), pltpu.VMEM((2, seq, sl), F32)] + [pltpu.VMEM((seq, hd), F32)] * 2,
            flops=2 * own * dim * qd + 8 * own * seq * qd, nbytes=2 * own * heads * seq)
        dkv = lax.psum_scatter(dkv_part, "tp", scatter_dimension=0)

        mixed2, dres2, u2, dq2 = mixed.reshape(own, qd), d_resid.reshape(own, dim), u.reshape(own, dim), d_q.reshape(own, qd)
        x_spec, y_spec = block((own, dim), lambda j, *_: (0, 0), True), lambda pick: block((own, cols), lambda j, *_: (0, pick(j)))
        g_out = run(
            block_grad_kernel, (tp_n,), [y_spec(lambda j: j), x_spec, ANY],
            block((1, cols, dim), lambda j, m: (m[0] ^ j, 0, 0)), sds((tp_n, cols, dim), F32), (me, mixed2, dres2, dkv_part),
            prefetch=1, flops=2 * own * dim * qd, nbytes=4 * dim * qd)
        g_out_sum = lax.psum_scatter(g_out.reshape(qd, dim), "tp", scatter_dimension=0, tiled=True)
        to_mate = run(
            block_grad_kernel, (2,), [x_spec, y_spec(lambda j: 1 + 2 * j), ANY],
            block((1, dim, cols), lambda j: (j, 0, 0)), sds((2, dim, cols), F32), (u2, dq2, g_out),
            flops=own * dim * qd, nbytes=2 * dim * qd)
        from_mate = to_core(to_mate)
        g_down = weight_grads(*down_args, (to_mate,), 1, ffn // 1024 - 1, g_down)[0]
        far_sum, own_sum = run(
            pair_grad_kernel, (2,), [x_spec, y_spec(lambda j: 2 - 2 * j), block((1, dim, cols), lambda j: (1 - j, 0, 0)), ANY],
            [block((1, dim, cols), lambda j: (0, 0, 0))] * 2, [sds((1, dim, cols), F32)] * 2, (u2, dq2, from_mate, g_down),
            flops=own * dim * qd, nbytes=2 * dim * qd)
        arrived = to_chip(far_sum)

        extra = dim // hd
        half_at = [block((1, sl, dim), lambda b, *_: (jnp.minimum(b, half - 1), 0, 0)), block((1, sl, dim), lambda b, *_: (jnp.maximum(b - half, 0), 0, 0))]
        grad_hidden, gkv, hidden_out = run(
            last_kernel, (batch,),
            [kv_spec, q_spec, tok_spec, tok_spec, tok_spec, gain_spec,
             ] + [ANY] * 6 + [rope_spec, rope_spec, const_spec((1, dim)), tok_spec, *half_at, ANY],
            [tok_spec, block((dim + extra, 2 * hd), lambda b, *_: (0, 0)), tok_spec],
            [sds((batch, sl, dim)), sds((dim + extra, 2 * hd), F32), sds((batch, sl, dim))],
            (me, dkv, d_q, u, hidden, d_resid, gain1, *wqs, w_key, w_value, cos_t, sin_t, gn2, resid, part0, part1, far_sum), prefetch=1,
            scratch=[pltpu.VMEM((1, dim), F32), pltpu.VMEM((dim, qd + 2 * hd), BF), pltpu.VMEM((sl, qd + 2 * hd), BF), dma(6)],
            flops=2 * own * dim * (qd + 4 * hd), nbytes=8 * own * dim)
        gkv = lax.psum(gkv, "tp")
        g_key, g_value = gkv[:dim, :hd], gkv[:dim, hd:]
        g_mlp_norm = gkv[dim : dim + extra // 2].reshape(dim)
        g_attn_norm = gkv[dim + extra // 2 :].reshape(dim)

        g_gate, g_up = weight_grads((full0[3], full1[3]), ((full0[1], full1[1]), (full0[2], full1[2])), (grad_hidden,))
        g_query_sum = own_sum[0] + tie(arrived, g_up)[0]
        return (hidden_out, grad_hidden, g_attn_norm, g_query_sum, g_key, g_value, g_out_sum, g_mlp_norm, g_gate, g_up, g_down)

    return jax.shard_map(local_layer, mesh=mesh, in_specs=in_specs, out_specs=out_specs, check_vma=False)
```

```python
import functools
import math

import jax
import jax.numpy as jnp
import numpy as np
from jax import lax
from jax.experimental import pallas as pl
from jax.experimental.pallas import tpu as pltpu
from jax.sharding import PartitionSpec as P


EPS = 1e-6
BF = jnp.bfloat16
F32 = jnp.float32
MIB = 1024 * 1024
ANY = pl.BlockSpec(memory_space=pl.ANY)


def dot_nn(a, b):
    return lax.dot_general(a, b, (((1,), (0,)), ((), ())), preferred_element_type=F32)


def dot_nt(a, b):
    return lax.dot_general(a, b, (((1,), (1,)), ((), ())), preferred_element_type=F32)


def dot_tn(a, b):
    return lax.dot_general(a, b, (((0,), (0,)), ((), ())), preferred_element_type=F32)


def const_spec(shape):
    zeros = (0,) * len(shape)
    return pl.BlockSpec(shape, lambda *_: zeros, pipeline_mode=pl.Buffered(1))


def run(kernel, grid, in_specs, out_specs, out_shape, args, scratch=(), prefetch=0, aliases=None, flops=0, nbytes=0, limit=63):
    spec = pltpu.PrefetchScalarGridSpec(num_scalar_prefetch=prefetch, grid=grid, in_specs=in_specs, out_specs=out_specs, scratch_shapes=scratch)
    return pl.pallas_call(
        kernel,
        grid_spec=spec,
        out_shape=out_shape,
        input_output_aliases=aliases or {},
        compiler_params=pltpu.CompilerParams(dimension_semantics=("arbitrary",) * len(grid), vmem_limit_bytes=limit * MIB),
        cost_estimate=pl.CostEstimate(flops=int(flops), bytes_accessed=int(nbytes), transcendentals=0),
    )(*args)


def rope_fwd(x, cos_t, sin_t):
    half = x.shape[-1] // 2
    a, b = x[:, :half], x[:, half:]
    return a * cos_t - b * sin_t, b * cos_t + a * sin_t


def rope_bwd(a, b, cos_t, sin_t):
    return a * cos_t + b * sin_t, b * cos_t - a * sin_t


def pre_kernel(me_ref, h_ref, gain_ref, wk_ref, wv_ref, cos_ref, sin_ref, u_ref, kv_ref):
    n, sl, dim = h_ref.shape
    x = h_ref[...].reshape(n * sl, dim).astype(F32)
    inv = lax.rsqrt(jnp.mean(x * x, axis=-1, keepdims=True) + EPS)
    u = (x * inv * gain_ref[...]).astype(BF)
    u_ref[...] = u.reshape(n, sl, dim)
    hd = wk_ref.shape[1]
    k, v = dot_nn(u, wk_ref[...]), dot_nn(u, wv_ref[...])
    for i in range(n):
        first, second = rope_fwd(k[i * sl : (i + 1) * sl], cos_ref[...], sin_ref[...])
        kv_ref[i, :, : hd // 2] = first.astype(BF)
        kv_ref[i, :, hd // 2 : hd] = second.astype(BF)
        kv_ref[i, :, hd:] = v[i * sl : (i + 1) * sl].astype(BF)


def attn_fwd_kernel(me_ref, pre_ref, val_ref, u_ref, w0_ref, w1_ref, w2_ref, w3_ref, k0_ref, k1_ref, k2_ref, k3_ref, cos_ref, sin_ref, token_ref,
                    q_ref, pt_ref, mix_ref, keys_ref, vt_ref, s_ref):
    b = pl.program_id(0)
    cols = w0_ref.shape[1]
    _, hd = keys_ref.shape
    sl = u_ref.shape[1]
    heads = q_ref.shape[2] // hd
    u = u_ref[0]
    me = me_ref[0]
    cos_t, sin_t = cos_ref[...], sin_ref[...]
    place = []
    for r, kv_ref in enumerate((k0_ref, k1_ref, k2_ref, k3_ref)):
        keys_ref[r * sl : (r + 1) * sl, :] = kv_ref[0, :, :hd]
        vt_ref[:, r * sl : (r + 1) * sl] = kv_ref[0, :, hd:].astype(F32).T.astype(BF)
        place.append(lax.broadcasted_iota(jnp.int32, (sl, sl), 0) + (me ^ r) * sl)
    for r, w_ref in enumerate((w0_ref, w1_ref, w2_ref, w3_ref)):
        qs = dot_nn(u, w_ref[...])
        for j in range(cols // hd):
            base = r * cols + j * hd
            first, second = rope_fwd(qs[:, j * hd : (j + 1) * hd], cos_t, sin_t)
            q_ref[0, :, base : base + hd // 2] = first.astype(BF)
            q_ref[0, :, base + hd // 2 : base + hd] = second.astype(BF)
    prefix, valid = pre_ref[b], val_ref[b]
    q_end = lax.broadcasted_iota(jnp.int32, (1, sl), 1) + (me * sl + 1)
    limit = jnp.minimum(valid, jnp.maximum(prefix, q_end))
    visible = jnp.concatenate(place, axis=0) < limit
    scale = (hd**-0.5) * math.log2(math.e)

    def scores(h):
        return dot_nt(keys_ref[...], q_ref[0, :, h * hd : (h + 1) * hd])

    s_ref[0] = scores(0)
    for h in range(heads):
        if h + 1 < heads:
            s_ref[(h + 1) % 2] = scores(h + 1)
        sc = jnp.where(visible, s_ref[h % 2], -1e30)
        top = jnp.max(sc, axis=0, keepdims=True)
        e = jnp.exp2((sc - top) * scale)
        p = (e * (1.0 / jnp.sum(e, axis=0, keepdims=True))).astype(BF)
        pt_ref[0, :, h * sl : (h + 1) * sl] = p
        mix_ref[0, :, h * hd : (h + 1) * hd] = dot_nn(vt_ref[...], p).T.astype(BF)


def weight_copies(refs, dst, axis, sems):
    at, copies = 0, []
    for i, ref in enumerate(refs):
        n = ref.shape[axis]
        copies.append(pltpu.make_async_copy(ref, dst.at[pl.ds(at, n), :] if axis == 0 else dst.at[:, pl.ds(at, n)], sems.at[i]))
        at += n
    return copies


def start_first(*fetch):
    @pl.when(pl.program_id(0) == 0)
    def _():
        for c in weight_copies(*fetch):
            c.start()


def wait_first(*fetch):
    @pl.when(pl.program_id(0) == 0)
    def _():
        for c in weight_copies(*fetch):
            c.wait()


def out_kernel(mix_ref, w0_ref, w1_ref, w2_ref, w3_ref, h_ref, gain_ref, *rest):
    resid_ref, z_ref, wo_ref, sems = rest[-4:]
    fetch = (w0_ref, w1_ref, w2_ref, w3_ref), wo_ref, 0, sems
    start_first(*fetch)
    wait_first(*fetch)
    x = (h_ref[0].astype(F32) + dot_nn(mix_ref[0], wo_ref[...])).astype(BF)
    resid_ref[0] = x
    x = x.astype(F32)
    inv = lax.rsqrt(jnp.mean(x * x, axis=-1, keepdims=True) + EPS)
    z_ref[0] = (x * inv * gain_ref[...]).astype(BF)


class Flow:
    def __init__(self, bufs, sems, inward, sides):
        self.bufs, self.sems, self.inward, self.sides = bufs, sems, inward, sides

    def copies(self, t, slot, only):
        out = []
        for i, (hbm, buf) in enumerate(zip(self.sides(t), self.bufs)):
            if only is None or i == only:
                pair = (hbm, buf.at[slot]) if self.inward else (buf.at[slot], hbm)
                out.append(pltpu.make_async_copy(*pair, self.sems.at[slot, i]))
        return out

    def start(self, t, slot, only=None):
        for c in self.copies(t, slot, only):
            c.start()

    def wait(self, t, slot, only=None):
        for c in self.copies(t, slot, only):
            c.wait()


def local_copies(pairs, sems):
    return [pltpu.make_async_copy(src, dst, sems.at[i]) for i, (src, dst) in enumerate(pairs)]


def start_all(copies):
    for c in copies:
        c.start()


def wait_all(copies):
    for c in copies:
        c.wait()


def span(t, n):
    return pl.ds(pl.multiple_of(t * n, n), n)


OWN, MATE, FAR = 0, 1, 2


def dact_kernel(kind, me_ref, *refs):
    n_in, n_out = (2, 2) if kind == FAR else (1, 5 if kind == OWN else 3)
    gs, wd_ref = refs[:n_in], refs[n_in]
    outs, (wb, ob, gv, w_sem, o_sem, g_sem, c_sem) = refs[-7 - n_out : -7], refs[-7:]
    da_ref, homes = outs[0], outs[1:]
    half = gv.shape[0] // 2
    chip, core = me_ref[0] // 2, me_ref[0] % 2
    halves = [gv.at[pl.ds(c * half, half)] for c in range(2)]
    if kind == FAR:
        loads = local_copies(zip(gs, halves), g_sem)
        puts = [(halves[0], homes[0].at[1 - chip, core]), (halves[1], homes[0].at[1 - chip, 1 - core])]
    else:
        loads = local_copies([(gs[0], gv)], g_sem)
        puts = [(halves[c], homes[c].at[chip, core if kind == OWN else 1 - core]) for c in range(2)]
        puts += list(zip(halves, homes[2:]))
    puts = local_copies(puts, c_sem)
    bn = ob.shape[-1]
    steps = wd_ref.shape[0] // bn
    w_flow = Flow((wb,), w_sem, True, lambda t: (wd_ref.at[span(t, bn)],))
    o_flow = Flow((ob,), o_sem, False, lambda t: (da_ref.at[:, :, span(t, bn)],))
    start_all(loads)
    w_flow.start(0, 0)
    wait_all(loads)
    start_all(puts)

    @pl.loop(0, steps)
    def _(t):
        slot = lax.rem(t, 2)

        @pl.when(t + 1 < steps)
        def _():
            w_flow.start(t + 1, 1 - slot)

        @pl.when(t >= 2)
        def _():
            o_flow.wait(t - 2, slot)

        w_flow.wait(t, slot)
        g = gv[...].reshape(2 * half * gv.shape[1], gv.shape[2])
        ob[slot] = dot_nt(g, wb[slot]).astype(BF).reshape(ob.shape[1:])
        o_flow.start(t, slot)

    for t in (steps - 2, steps - 1):
        o_flow.wait(t, t % 2)
    wait_all(puts)


def gated(gate, up, da):
    c0 = math.sqrt(2.0 / math.pi)
    c1 = c0 * 0.044715
    x2 = gate * gate
    hh = 0.5 + 0.5 * jnp.tanh(gate * (c0 + c1 * x2))
    gelu = gate * hh
    slope = hh + gelu * ((1.0 - hh) * (2.0 * c0 + 6.0 * c1 * x2))
    return (gelu * up).astype(BF), (da * up * slope).astype(BF), (da * gelu).astype(BF)


def mlp_kernel(other, at, fused, me_ref, *refs):
    za, zb, da, db, wg_ref, wu_ref = refs[:6]
    n_out, n_scr = (5, 13) if fused else (4, 11)
    outs, scr = refs[-n_scr - n_out : -n_scr], refs[-n_scr:]
    zv, wgb, wub, act_b, dg_b, du_b, in_sem, o_sem, z_sem, c_sem = scr[:10]
    chip = abs(other - me_ref[0] // 2)
    core = me_ref[0] % 2
    rows, bn = act_b.shape[2:]
    dim = zv.shape[-1]
    steps = wg_ref.shape[1] // bn
    if fused:
        wdb, gv, g_sem = scr[10:]
        wd_ref = refs[6]
        in_flow = Flow((wgb, wub, wdb), in_sem, True, lambda t: (wg_ref.at[:, span(t, bn)], wu_ref.at[:, span(t, bn)], wd_ref.at[span(t, bn)]))
    else:
        dv = scr[10]
        in_flow = Flow((wgb, wub, dv.at[:, 0], dv.at[:, 1]), in_sem, True,
                       lambda t: (wg_ref.at[:, span(t, bn)], wu_ref.at[:, span(t, bn)], da.at[at[0], :, span(t, bn)], db.at[at[1], :, span(t, bn)]))
    bufs = (act_b, dg_b, du_b)
    o_flow = Flow([b.at[:, rel] for rel in range(2) for b in bufs], o_sem, False,
                  lambda t: [o.at[chip, abs(rel - core), :, span(t, bn)] for rel in range(2) for o in outs[:3]])
    loads = local_copies([(za, zv.at[0]), (zb, zv.at[1])], z_sem)
    puts = [(zv.at[0], outs[3].at[chip, core]), (zv.at[1], outs[3].at[chip, 1 - core])]
    if fused:
        loads += local_copies([(da, gv.at[0]), (db, gv.at[1])], g_sem)
        puts += [(gv.at[0], outs[4].at[chip, core]), (gv.at[1], outs[4].at[chip, 1 - core])]
    puts = local_copies(puts, c_sem)
    in_flow.start(0, 0)
    start_all(loads)
    wait_all(loads)
    start_all(puts)
    n = rows // (3 if fused else 2)

    @pl.loop(0, steps)
    def _(t):
        slot = lax.rem(t, 2)

        @pl.when(t + 1 < steps)
        def _():
            in_flow.start(t + 1, 1 - slot)

        @pl.when(t >= 2)
        def _():
            o_flow.wait(t - 2, slot)

        in_flow.wait(t, slot)
        for rel in range(2):
            z = zv[rel].reshape(rows, dim)
            for r in range(0, rows, n):
                gate, up = dot_nn(z[r : r + n], wgb[slot]), dot_nn(z[r : r + n], wub[slot])
                if fused:
                    d = dot_nt(gv[rel].reshape(rows, dim)[r : r + n], wdb[slot])
                else:
                    d = dv[slot, rel, r : r + n, :].astype(F32)
                for buf, o in zip(bufs, gated(gate, up, d)):
                    buf[slot, rel, r : r + n, :] = o
        o_flow.start(t, slot)

    for t in (steps - 2, steps - 1):
        o_flow.wait(t, t % 2)
    wait_all(puts)


def attn_bwd_kernel(me_ref, dz0_ref, dz1_ref, res_ref, go_ref, gain_ref, w0_ref, w1_ref, w2_ref, w3_ref, k0_ref, k1_ref, k2_ref, k3_ref,
                    q_ref, pt_ref, cos_ref, sin_ref, token0_ref, token1_ref, token2_ref,
                    dres_ref, dq_ref, dkv_ref, gn_ref, kt_ref, v_ref, do_ref, qs_ref, ds_ref, dp_ref, dk_ref, dv_ref):
    b = pl.program_id(0)
    half = pl.num_programs(0) // 2
    seq, hd = v_ref.shape
    sl = q_ref.shape[1]
    heads = q_ref.shape[2] // hd
    me = me_ref[0]
    x = res_ref[0].astype(F32)
    dz = jnp.where(b < half, dz0_ref[0], dz1_ref[0]).astype(F32)
    inv = lax.rsqrt(jnp.mean(x * x, axis=-1, keepdims=True) + EPS)
    xn = x * inv
    part = jnp.sum(dz * xn, axis=0, keepdims=True)

    @pl.when(b == 0)
    def _():
        gn_ref[...] = part

    @pl.when(b > 0)
    def _():
        gn_ref[...] += part

    dxn = dz * gain_ref[...]
    dx = inv * (dxn - xn * jnp.mean(dxn * xn, axis=-1, keepdims=True))
    dres = (go_ref[0].astype(F32) + dx).astype(BF)
    dres_ref[0] = dres
    scale = hd**-0.5
    for r, kv_ref in enumerate((k0_ref, k1_ref, k2_ref, k3_ref)):
        kt_ref[:, r * sl : (r + 1) * sl] = (kv_ref[0, :, :hd].astype(F32) * scale).T.astype(BF)
        v_ref[r * sl : (r + 1) * sl, :] = kv_ref[0, :, hd:]
    w_refs = (w0_ref, w1_ref, w2_ref, w3_ref)
    per = w0_ref.shape[0] // hd

    def d_mixed(r):
        dm = dot_nt(dres, w_refs[r][...]).astype(BF)
        for j in range(per):
            h = r * per + j
            do_ref[h * sl : (h + 1) * sl, :] = dm[:, j * hd : (j + 1) * hd]
            qs_ref[h * sl : (h + 1) * sl, :] = (q_ref[0, :, h * hd : (h + 1) * hd].astype(F32) * scale).astype(BF)

    cos_t, sin_t = cos_ref[...], sin_ref[...]

    def dprobs(h):
        return dot_nt(v_ref[...], do_ref[h * sl : (h + 1) * sl, :])

    def add_kv(r, first):
        at = pl.ds(r * per * sl, per * sl)
        dk, dv = dot_nn(ds_ref[:, at], qs_ref[at, :]), dot_nn(pt_ref[0, :, at], do_ref[at, :])
        if first:
            dk_ref[...], dv_ref[...] = dk, dv
        else:
            dk_ref[...] += dk
            dv_ref[...] += dv

    d_mixed(0)
    dp_ref[0] = dprobs(0)
    for h in range(heads):
        if h % per == 0:
            if h // per + 1 < len(w_refs):
                d_mixed(h // per + 1)
            if h:
                add_kv(h // per - 1, h == per)
        if h + 1 < heads:
            dp_ref[(h + 1) % 2] = dprobs(h + 1)
        p = pt_ref[0, :, h * sl : (h + 1) * sl].astype(F32)
        t = p * dp_ref[h % 2]
        ds = (t - p * jnp.sum(t, axis=0, keepdims=True)).astype(BF)
        ds_ref[:, h * sl : (h + 1) * sl] = ds
        dq = dot_nn(kt_ref[...], ds).T
        first, second = rope_bwd(dq[:, : hd // 2], dq[:, hd // 2 :], cos_t, sin_t)
        dq_ref[0, :, h * hd : h * hd + hd // 2] = first.astype(BF)
        dq_ref[0, :, h * hd + hd // 2 : (h + 1) * hd] = second.astype(BF)
    at = pl.ds((heads - per) * sl, per * sl)
    dk = (dk_ref[...] + dot_nn(ds_ref[:, at], qs_ref[at, :])).astype(BF)
    dv = (dv_ref[...] + dot_nn(pt_ref[0, :, at], do_ref[at, :])).astype(BF)
    for r in range(seq // sl):
        dkv_ref[me ^ r, 0, :, :hd] = dk[r * sl : (r + 1) * sl]
        dkv_ref[me ^ r, 0, :, hd:] = dv[r * sl : (r + 1) * sl]


def last_kernel(me_ref, dkv_ref, dq_ref, u_ref, h_ref, dres_ref, gain_ref, w0_ref, w1_ref, w2_ref, w3_ref, wk_ref, wv_ref, cos_ref, sin_ref, gm_ref,
                res_ref, p0_ref, p1_ref, token0_ref, gh_ref, gkv_ref, ho_ref, acc_ref, w_ref, d_ref, sems):
    b = pl.program_id(0)
    dim, hd = wk_ref.shape
    qd = dq_ref.shape[2]
    fetch = (w0_ref, w1_ref, w2_ref, w3_ref, wk_ref, wv_ref), w_ref, 1, sems
    start_first(*fetch)
    half = pl.num_programs(0) // 2
    ho_ref[0] = (res_ref[0].astype(F32) + jnp.where(b < half, p0_ref[0], p1_ref[0]).astype(F32)).astype(BF)
    raw = dkv_ref[0]
    dk = raw[:, :hd].astype(F32)
    first, second = rope_bwd(dk[:, : hd // 2], dk[:, hd // 2 :], cos_ref[...], sin_ref[...])
    d_ref[:, :qd] = dq_ref[0]
    d_ref[:, qd : qd + hd // 2] = first.astype(BF)
    d_ref[:, qd + hd // 2 : qd + hd] = second.astype(BF)
    d_ref[:, qd + hd :] = raw[:, hd:]
    gk = dot_tn(u_ref[0], d_ref[:, qd:])
    wait_first(*fetch)
    dn = dot_nt(d_ref[...], w_ref[...])
    x = h_ref[0].astype(F32)
    inv = lax.rsqrt(jnp.mean(x * x, axis=-1, keepdims=True) + EPS)
    xn = x * inv
    part = jnp.sum(dn * xn, axis=0, keepdims=True)
    dxn = dn * gain_ref[...]
    dx = inv * (dxn - xn * jnp.mean(dxn * xn, axis=-1, keepdims=True))
    gh_ref[0] = (dres_ref[0].astype(F32) + dx).astype(BF)

    @pl.when(b == 0)
    def _():
        acc_ref[...] = part
        gkv_ref[:dim, :] = gk

    @pl.when(b > 0)
    def _():
        acc_ref[...] += part
        gkv_ref[:dim, :] += gk

    @pl.when(b == pl.num_programs(0) - 1)
    def _():
        width = 2 * hd
        per = dim // width
        for i in range(per):
            gkv_ref[dim + i : dim + i + 1, :] = gm_ref[:, i * width : (i + 1) * width]
            gkv_ref[dim + per + i : dim + per + i + 1, :] = acc_ref[:, i * width : (i + 1) * width]


def block_grad_kernel(*refs):
    x_ref, y_ref, o_ref = refs[-4], refs[-3], refs[-1]
    o_ref[...] = dot_tn(x_ref[...], y_ref[...]).reshape(o_ref.shape)


def gated_grad_kernel(dg_ref, du_ref, wg_ref, wu_ref, *rest):
    o_ref, a1, a2, b1, b2, ob, a_sem, b_sem, o_sem = rest[-9:]
    ni = dg_ref.shape[0] * dg_ref.shape[1]
    bn = b1.shape[1]
    nj = wg_ref.shape[0] // bn
    steps = ni * nj
    cols = lambda t: pl.ds(pl.multiple_of(lax.rem(t, nj) * bn, bn), bn)
    a_flow = Flow((a1, a2), a_sem, True, lambda i: (dg_ref.at[i // 2, i % 2], du_ref.at[i // 2, i % 2]))
    b_flow = Flow((b1, b2), b_sem, True, lambda t: (wg_ref.at[cols(t)], wu_ref.at[cols(t)]))
    o_flow = Flow((ob,), o_sem, False, lambda t: (o_ref.at[t // nj, :, cols(t)],))
    for k in range(2):
        a_flow.start(0, 0, k)
        b_flow.start(0, 0, k)
    b_flow.start(1, 1)
    a_flow.start(1, 1)
    for k in range(2):
        a_flow.wait(0, 0, k)
        b_flow.wait(0, 0, k)
        if k == 0:
            first = dot_nt(a1[0], b1[0])
    ob[0] = (first + dot_nt(a2[0], b2[0])).astype(BF)
    o_flow.start(0, 0)

    @pl.loop(1, steps)
    def _(t):
        i, slot = t // nj, lax.rem(t, 2)
        a_slot = lax.rem(i, 2)

        @pl.when(t + 1 < steps)
        def _():
            b_flow.start(t + 1, 1 - slot)

        @pl.when(lax.rem(t, nj) == 0)
        def _():
            a_flow.wait(i, a_slot)

            @pl.when(i + 1 < ni)
            def _():
                a_flow.start(i + 1, 1 - a_slot)

        @pl.when(t >= 2)
        def _():
            o_flow.wait(t - 2, slot)

        b_flow.wait(t, slot)
        ob[slot] = (dot_nt(a1[a_slot], b1[slot]) + dot_nt(a2[a_slot], b2[slot])).astype(BF)
        o_flow.start(t, slot)

    for t in (steps - 2, steps - 1):
        o_flow.wait(t, t % 2)


def weight_grads_kernel(count, first, ni, *refs):
    x_refs, y_refs = refs[:2], refs[2 : 2 + 2 * count]
    o_refs, (x0, x1, y0, y1, ob, x_sem, y_sem, o_sem) = refs[-8 - count : -8], refs[-8:]
    bm, bn = ob.shape[1:]
    nj = y_refs[0].shape[1] // bn
    steps = ni * count * nj
    per = count * nj
    rows = lambda i: pl.ds(pl.multiple_of((first + i) * bm, bm), bm)
    cols = lambda t: pl.ds(pl.multiple_of(lax.rem(t, nj) * bn, bn), bn)
    x_flow = Flow((x0, x1), x_sem, True, lambda i: [r.at[:, rows(i)] for r in x_refs])
    y_flows = [Flow((y0, y1), y_sem, True, lambda t, k=k: [r.at[:, cols(t)] for r in y_refs[2 * k : 2 * k + 2]]) for k in range(count)]
    o_flows = [Flow((ob,), o_sem, False, lambda t, k=k: (o_refs[k].at[rows(t // per), cols(t)],)) for k in range(count)]

    def each(flows, t, act):
        if count == 1:
            act(flows[0])
        else:
            which = lax.rem(t // nj, count)
            for k in range(count):
                pl.when(which == k)(functools.partial(act, flows[k]))

    for k in range(2):
        x_flow.start(0, 0, k)
        y_flows[0].start(0, 0, k)
    y_flows[0].start(1, 1)
    if ni > 1:
        x_flow.start(1, 1)
    for k in range(2):
        x_flow.wait(0, 0, k)
        y_flows[0].wait(0, 0, k)
        if k == 0:
            part = dot_tn(x0[0], y0[0])
    ob[0] = part + dot_tn(x1[0], y1[0])
    o_flows[0].start(0, 0)

    @pl.loop(1, steps)
    def _(t):
        i, slot = t // per, lax.rem(t, 2)
        x_slot = lax.rem(i, 2)

        @pl.when(t + 1 < steps)
        def _():
            each(y_flows, t + 1, lambda f: f.start(t + 1, 1 - slot))

        @pl.when(lax.rem(t, per) == 0)
        def _():
            x_flow.wait(i, x_slot)

            @pl.when(i + 1 < ni)
            def _():
                x_flow.start(i + 1, 1 - x_slot)

        @pl.when(t >= 2)
        def _():
            o_flows[0].wait(t - 2, slot)

        y_flows[0].wait(t, slot)
        ob[slot] = dot_tn(x0[x_slot], y0[slot]) + dot_tn(x1[x_slot], y1[slot])
        each(o_flows, t, lambda f: f.start(t, slot))

    for t in (steps - 2, steps - 1):
        o_flows[0].wait(t, t % 2)


def split_kernel(x_ref, k_ref, v_ref, m_ref, a_ref):
    dim, hd = k_ref.shape
    k_ref[...], v_ref[...] = x_ref[:dim, :hd], x_ref[:dim, hd:]
    for j, o_ref in enumerate((m_ref, a_ref)):
        n = dim // (2 * hd)
        for i in range(n):
            o_ref[:, i * 2 * hd : (i + 1) * 2 * hd] = x_ref[dim + j * n + i : dim + j * n + i + 1, :]


def tie_kernel(x_ref, *rest):
    del x_ref, rest


def tie(x, *tokens):
    return pl.pallas_call(
        tie_kernel,
        name="tie",
        in_specs=[ANY] * (1 + len(tokens)),
        out_specs=ANY,
        out_shape=jax.ShapeDtypeStruct(x.shape, x.dtype),
        input_output_aliases={0: 0},
    )(x, *tokens)


def solution(mesh):
    act_spec = P("dp", "tp", None)
    in_specs = (act_spec, act_spec, P("dp"), P("dp"), P(None), P(None, "tp"), P(None, None), P(None, None), P("tp", None), P(None), P(None, "tp"), P(None, "tp"), P("tp", None))
    out_specs = (act_spec, act_spec, P("dp"), P("dp", "tp"), P("dp", None), P("dp", None), P(("dp", "tp"), None), P("dp"), P("dp", "tp"), P("dp", "tp"), P(("dp", "tp"), None))
    core_flip = [(0, 1), (1, 0), (2, 3), (3, 2)]
    chip_flip = [(0, 2), (2, 0), (1, 3), (3, 1)]

    def to_core(x):
        return lax.ppermute(x, "tp", core_flip)

    def to_chip(x):
        return lax.ppermute(x, "tp", chip_flip)

    def local_layer(hidden, grad_out, prefix_len, valid_len, attn_norm, w_query, w_key, w_value, w_out, mlp_norm, w_gate, w_up, w_down):
        batch, sl, dim = hidden.shape
        half = batch // 2
        rows = half * sl
        hd = w_key.shape[1]
        cols = w_query.shape[1]
        tp_n = mesh.shape["tp"]
        seq = sl * tp_n
        qd = cols * tp_n
        heads = qd // hd
        ffn = w_gate.shape[1]
        own = batch * sl
        me = lax.axis_index("tp").astype(jnp.int32).reshape(1)

        inv_freq = np.exp(np.arange(hd // 2, dtype=np.float32) * np.float32(2.0 / hd) * np.float32(-math.log(10000.0)))
        angles = np.arange(seq, dtype=np.float32)[:, None] * inv_freq[None, :]
        cos_t, sin_t = jnp.asarray(np.cos(angles)), jnp.asarray(np.sin(angles))
        gain1 = (1.0 + attn_norm.astype(F32)).reshape(1, dim)
        gain2 = (1.0 + mlp_norm.astype(F32)).reshape(1, dim)

        def sds(shape, dtype=BF):
            return jax.ShapeDtypeStruct(shape, dtype)

        def block(shape, at, single=False):
            return pl.BlockSpec(shape, at, pipeline_mode=pl.Buffered(1) if single else None)

        tok_spec = block((1, sl, dim), lambda b, *_: (b, 0, 0))
        q_spec = block((1, sl, qd), lambda b, *_: (b, 0, 0))
        kv_spec = block((1, sl, 2 * hd), lambda b, *_: (b, 0, 0))
        kv4_spec = block((tp_n, 1, sl, 2 * hd), lambda b, *_: (0, b, 0, 0))
        pt_spec = block((1, seq, heads * sl), lambda b, *_: (b, 0, 0))
        rope_spec = block((sl, hd // 2), lambda b, m, *_: (m[0], 0), True)
        gain_spec = const_spec((1, dim))
        dma = lambda n: pltpu.SemaphoreType.DMA((n,))

        wq_far = to_chip(w_query)
        wq_mate = to_core(w_query)
        g_mate = to_core(grad_out)
        u, kv = run(
            pre_kernel, (batch // 2,),
            [block((2, sl, dim), lambda b, *_: (b, 0, 0)), gain_spec, const_spec((dim, hd)), const_spec((dim, hd)), rope_spec, rope_spec],
            [block((2, sl, dim), lambda b, *_: (b, 0, 0)), block((2, sl, 2 * hd), lambda b, *_: (b, 0, 0))],
            [sds((batch, sl, dim)), sds((batch, sl, 2 * hd))],
            (me, hidden, gain1, w_key, w_value, cos_t, sin_t), prefetch=1,
            flops=4 * own * dim * hd, nbytes=6 * own * dim)
        kv_far = to_chip(kv)
        kv_mate = to_core(kv)
        wo_far = to_chip(w_out)
        wo_mate = to_core(w_out)

        bn = 512
        cat_shape = (2, 2, half, sl, dim)
        SMEM = pl.BlockSpec(memory_space=pltpu.SMEM)
        pair = (2, rows, bn)

        def dact(kind, gs, homes, tokens, n_out):
            return run(
                functools.partial(dact_kernel, kind), (), [SMEM] + [ANY] * (len(gs) + 1 + len(homes) + len(tokens)), [ANY] * n_out,
                ([sds((2, rows, ffn))] + [sds(cat_shape)] * 2 + [sds((half, sl, dim))] * 2)[: n_out],
                (me, *gs, w_down, *homes, *tokens), aliases={2 + len(gs) + i: 1 + i for i in range(len(homes))},
                scratch=[pltpu.VMEM((2, bn, dim), BF), pltpu.VMEM((2,) + pair, BF), pltpu.VMEM((batch, sl, dim), BF),
                         pltpu.SemaphoreType.DMA((2, 1)), pltpu.SemaphoreType.DMA((2, 1)), dma(2), dma(4)],
                flops=4 * rows * dim * ffn, nbytes=2 * ffn * dim + 4 * rows * ffn)

        da_own, gcat0, gcat1, go0, go1 = dact(OWN, (grad_out,), (), (kv,), 5)
        wq_far = tie(wq_far, da_own)
        wq_far_mate = to_core(wq_far)
        da_mate, gcat0, gcat1 = dact(MATE, (g_mate,), (gcat0, gcat1), (da_own,), 3)
        kv_far = tie(kv_far, da_mate)
        kv_far_mate = to_core(kv_far)
        wqs = (w_query, wq_mate, wq_far, wq_far_mate)
        kvs = (kv, kv_mate, kv_far, kv_far_mate)
        wq_specs = [const_spec((dim, cols))] * 4
        wo_specs = [const_spec((cols, dim))] * 4

        q, pt, mixed = run(
            attn_fwd_kernel, (batch,),
            [tok_spec] + wq_specs + [kv_spec] * 4 + [rope_spec, rope_spec, ANY],
            [q_spec, pt_spec, q_spec],
            [sds((batch, sl, qd)), sds((batch, seq, heads * sl)), sds((batch, sl, qd))],
            (me, prefix_len, valid_len, u, *wqs, *kvs, cos_t, sin_t, da_mate), prefetch=3,
            scratch=[pltpu.VMEM((seq, hd), BF), pltpu.VMEM((hd, seq), BF), pltpu.VMEM((2, seq, sl), F32)],
            flops=2 * own * dim * qd + 4 * own * seq * qd, nbytes=2 * own * heads * seq)
        wo_far = tie(wo_far, mixed)
        wo_far_mate = to_core(wo_far)
        wos = (w_out, wo_mate, wo_far, wo_far_mate)

        g_far = [to_chip(tie(go0, mixed))]

        def out_proj(c, prev):
            at = lambda b: (b + c * half, 0, 0)
            extra = [prev] if c else []
            return run(
                out_kernel, (half,),
                [block((1, sl, qd), at)] + [ANY] * 4 + [block((1, sl, dim), at), gain_spec] + [ANY] * len(extra),
                [block((1, sl, dim), at), block((1, sl, dim), lambda b: (b, 0, 0))],
                [sds((batch, sl, dim)), sds((half, sl, dim))],
                (mixed, *wos, hidden, gain2, *extra), aliases={7: 0} if c else None,
                scratch=[pltpu.VMEM((qd, dim), BF), dma(4)],
                flops=own * dim * qd, nbytes=4 * own * dim)

        resid, z0 = out_proj(0, None)
        resid, z1 = out_proj(1, resid)
        zs = [z0, z1]
        z_mate = [to_core(z) for z in zs]
        z_far = [to_chip(z0)]
        z_far.append(to_chip(z1))
        g_far.append(to_chip(tie(go1, z1)))

        o_shape = (2, 2, rows, ffn)

        def mlp(other, at, fused, za, zb, da, db, prev, tokens):
            n_out = 5 if fused else 4
            weights = (w_gate, w_up, w_down) if fused else (w_gate, w_up)
            sem = lambda k, n: pltpu.SemaphoreType.DMA((k, n))
            scratch = [pltpu.VMEM((2, half, sl, dim), BF)] + [pltpu.VMEM((2, dim, bn), BF)] * 2 + [pltpu.VMEM((2, 2, rows, bn), BF)] * 3
            scratch += [sem(2, 3 if fused else 4), sem(2, 6), dma(2), dma(4)]
            scratch += [pltpu.VMEM((2, bn, dim), BF), pltpu.VMEM((2, half, sl, dim), BF), dma(2)] if fused else [pltpu.VMEM((2, 2, rows, bn), BF)]
            return run(
                functools.partial(mlp_kernel, other, at, fused), (),
                [SMEM] + [ANY] * (4 + len(weights) + len(prev) + len(tokens)), [ANY] * n_out,
                [sds(o_shape)] * 3 + [sds(cat_shape)] * (n_out - 3),
                (me, za, zb, da, db, *weights, *prev, *tokens), scratch=scratch,
                aliases={5 + len(weights) + i: i for i in range(len(prev))},
                flops=(12 if fused else 8) * rows * dim * ffn, nbytes=4 * ffn * dim + 16 * rows * ffn)

        near0 = mlp(0, (0, 0), False, zs[0], z_mate[0], da_own, da_mate, (), (z1,))
        near1 = mlp(0, (1, 1), False, zs[1], z_mate[1], da_own, da_mate, (), (near0[0],))

        ga = tie(g_far[0], near0[0])
        gb = to_core(ga)
        da_far, gcat0 = dact(FAR, (ga, gb), (gcat0,), (near1[0],), 2)
        za = tie(z_far[0], near1[0])
        zb = to_core(za)
        full0 = mlp(1, (0, 1), False, za, zb, da_far, da_far, near0, ())

        def gated_grad(full):
            bj = 512
            return run(
                gated_grad_kernel, (), [ANY] * 5, ANY, sds((4, rows, dim)), (full[1], full[2], w_gate, w_up, full[0]),
                scratch=[pltpu.VMEM((2, rows, ffn), BF)] * 2 + [pltpu.VMEM((2, bj, ffn), BF)] * 2 + [pltpu.VMEM((2, rows, bj), BF)]
                + [pltpu.SemaphoreType.DMA((2, 2))] * 2 + [pltpu.SemaphoreType.DMA((2, 1))],
                flops=16 * rows * dim * ffn, nbytes=16 * rows * ffn)

        def mlp_out(full):
            return dot_nn(full[0].reshape(4 * rows, ffn), w_down).astype(BF)

        def scatter(x):
            return lax.psum_scatter(x.reshape(tp_n, rows, dim), "tp", scatter_dimension=0).reshape(half, sl, dim)

        dz_part0 = gated_grad(full0)
        dz0 = scatter(dz_part0)
        mlp_part0 = mlp_out(full0)
        part0 = scatter(mlp_part0)

        ga, za = tie(g_far[1], full0[0]), tie(z_far[1], full0[0])
        gb = to_core(ga)
        zb = to_core(za)
        full1 = mlp(1, None, True, za, zb, ga, gb, (*near1, gcat1), (dz_part0, mlp_part0))
        gcat1 = full1[4]
        dz_part1 = gated_grad(full1)
        dz1 = scatter(dz_part1)
        mlp_part1 = mlp_out(full1)
        part1 = scatter(mlp_part1)

        def weight_grads(x, ys, tokens, first=0, ni=None, prev=None, by=512):
            flat = lambda pair: [a.reshape(4 * rows, -1) for a in pair]
            xs, yf = flat(x), [a for y in ys for a in flat(y)]
            m, n = xs[0].shape[1], yf[0].shape[1]
            bm = 1024
            extra = [prev] if prev is not None else []
            return run(
                functools.partial(weight_grads_kernel, len(ys), first, ni or m // bm), (),
                [ANY] * (2 + len(yf) + len(extra) + len(tokens)), [ANY] * len(ys), [sds((m, n), F32)] * len(ys),
                (*xs, *yf, *extra, *tokens), aliases={2 + len(yf): 0} if extra else None,
                scratch=[pltpu.VMEM((2, 4 * rows, bm), BF)] * 2 + [pltpu.VMEM((2, 4 * rows, by), BF)] * 2 + [pltpu.VMEM((2, bm, by), F32)]
                + [pltpu.SemaphoreType.DMA((2, 2))] * 2 + [pltpu.SemaphoreType.DMA((2, 1))],
                flops=16 * rows * (ni or m // bm) * bm * n * len(ys), nbytes=4 * m * n)

        down_args = (full0[0], full1[0]), ((gcat0, gcat1),)
        g_down = weight_grads(*down_args, (mlp_part1,), 0, 1)[0]

        d_resid, d_q, dkv_part, gn2 = run(
            attn_bwd_kernel, (batch,),
            [block((1, sl, dim), lambda b, *_: (jnp.minimum(b, half - 1), 0, 0)), block((1, sl, dim), lambda b, *_: (jnp.maximum(b - half, 0), 0, 0)),
             tok_spec, tok_spec, gain_spec] + wo_specs + [kv_spec] * 4 + [q_spec, pt_spec, rope_spec, rope_spec, ANY, ANY, ANY],
            [tok_spec, q_spec, kv4_spec, block((1, dim), lambda b, *_: (0, 0))],
            [sds((batch, sl, dim)), sds((batch, sl, qd)), sds((tp_n, batch, sl, 2 * hd)), sds((1, dim), F32)],
            (me, dz0, dz1, resid, grad_out, gain2, *wos, *kvs, q, pt, cos_t, sin_t, mlp_part1, g_down, part0), prefetch=1,
            scratch=[pltpu.VMEM((hd, seq), BF), pltpu.VMEM((seq, hd), BF), pltpu.VMEM((heads * sl, hd), BF), pltpu.VMEM((heads * sl, hd), BF), pltpu.VMEM((seq, heads * sl), BF), pltpu.VMEM((2, seq, sl), F32)] + [pltpu.VMEM((seq, hd), F32)] * 2,
            flops=2 * own * dim * qd + 8 * own * seq * qd, nbytes=2 * own * heads * seq)
        dkv = lax.psum_scatter(dkv_part, "tp", scatter_dimension=0)

        mixed2, dres2, u2, dq2 = mixed.reshape(own, qd), d_resid.reshape(own, dim), u.reshape(own, dim), d_q.reshape(own, qd)
        x_spec, y_spec = block((own, dim), lambda j, *_: (0, 0), True), lambda pick: block((own, cols), lambda j, *_: (0, pick(j)))
        g_out = run(
            block_grad_kernel, (tp_n,), [y_spec(lambda j: j), x_spec, ANY],
            block((1, cols, dim), lambda j, m: (m[0] ^ j, 0, 0)), sds((tp_n, cols, dim), F32), (me, mixed2, dres2, dkv_part),
            prefetch=1, flops=2 * own * dim * qd, nbytes=4 * dim * qd)
        g_out_sum = lax.psum_scatter(g_out.reshape(qd, dim), "tp", scatter_dimension=0, tiled=True)
        g_query = run(
            block_grad_kernel, (tp_n,), [x_spec, y_spec(lambda j: j), ANY],
            block((1, dim, cols), lambda j, m: (m[0] ^ j, 0, 0)), sds((tp_n, dim, cols), F32), (me, u2, dq2, g_out),
            prefetch=1, flops=2 * own * dim * qd, nbytes=4 * dim * qd)
        g_query_sum = lax.psum_scatter(g_query.reshape(tp_n * dim, cols), "tp", scatter_dimension=0, tiled=True)
        g_down = weight_grads(*down_args, (g_query,), 1, ffn // 1024 - 1, g_down)[0]

        extra = dim // hd
        half_at = [block((1, sl, dim), lambda b, *_: (jnp.minimum(b, half - 1), 0, 0)), block((1, sl, dim), lambda b, *_: (jnp.maximum(b - half, 0), 0, 0))]
        grad_hidden, gkv, hidden_out = run(
            last_kernel, (batch,),
            [kv_spec, q_spec, tok_spec, tok_spec, tok_spec, gain_spec,
             ] + [ANY] * 6 + [rope_spec, rope_spec, const_spec((1, dim)), tok_spec, *half_at, ANY],
            [tok_spec, block((dim + extra, 2 * hd), lambda b, *_: (0, 0)), tok_spec],
            [sds((batch, sl, dim)), sds((dim + extra, 2 * hd), F32), sds((batch, sl, dim))],
            (me, dkv, d_q, u, hidden, d_resid, gain1, *wqs, w_key, w_value, cos_t, sin_t, gn2, resid, part0, part1, g_down), prefetch=1,
            scratch=[pltpu.VMEM((1, dim), F32), pltpu.VMEM((dim, qd + 2 * hd), BF), pltpu.VMEM((sl, qd + 2 * hd), BF), dma(6)],
            flops=2 * own * dim * (qd + 4 * hd), nbytes=8 * own * dim)
        gkv = lax.psum(gkv, "tp")
        whole = lambda shape: block(shape, lambda b: (0,) * len(shape))
        g_key, g_value, g_mlp_norm, g_attn_norm = run(
            split_kernel, (1,), [whole((dim + extra, 2 * hd))], [whole((dim, hd))] * 2 + [whole((1, dim))] * 2,
            [sds((dim, hd), F32)] * 2 + [sds((1, dim), F32)] * 2, (gkv,), nbytes=16 * dim * hd)
        g_mlp_norm, g_attn_norm = g_mlp_norm.reshape(dim), g_attn_norm.reshape(dim)

        g_gate, g_up = weight_grads((full0[3], full1[3]), ((full0[1], full1[1]), (full0[2], full1[2])), (grad_hidden,), by=512)
        return (hidden_out, grad_hidden, g_attn_norm, g_query_sum, g_key, g_value, g_out_sum, g_mlp_norm, g_gate, g_up, g_down)

    return jax.shard_map(local_layer, mesh=mesh, in_specs=in_specs, out_specs=out_specs, check_vma=False)
```

```python
import functools
import math

import jax
import jax.numpy as jnp
import numpy as np
from jax import lax
from jax.experimental import pallas as pl
from jax.experimental.pallas import tpu as pltpu
from jax.sharding import PartitionSpec as P


EPS = 1e-6
BF = jnp.bfloat16
F32 = jnp.float32
MIB = 1024 * 1024
ANY = pl.BlockSpec(memory_space=pl.ANY)


def dot_nn(a, b):
    return lax.dot_general(a, b, (((1,), (0,)), ((), ())), preferred_element_type=F32)


def dot_nt(a, b):
    return lax.dot_general(a, b, (((1,), (1,)), ((), ())), preferred_element_type=F32)


def dot_tn(a, b):
    return lax.dot_general(a, b, (((0,), (0,)), ((), ())), preferred_element_type=F32)


def const_spec(shape):
    zeros = (0,) * len(shape)
    return pl.BlockSpec(shape, lambda *_: zeros, pipeline_mode=pl.Buffered(1))


def run(kernel, grid, in_specs, out_specs, out_shape, args, scratch=(), prefetch=0, aliases=None, flops=0, nbytes=0, limit=63):
    spec = pltpu.PrefetchScalarGridSpec(num_scalar_prefetch=prefetch, grid=grid, in_specs=in_specs, out_specs=out_specs, scratch_shapes=scratch)
    return pl.pallas_call(
        kernel,
        grid_spec=spec,
        out_shape=out_shape,
        input_output_aliases=aliases or {},
        compiler_params=pltpu.CompilerParams(dimension_semantics=("arbitrary",) * len(grid), vmem_limit_bytes=limit * MIB),
        cost_estimate=pl.CostEstimate(flops=int(flops), bytes_accessed=int(nbytes), transcendentals=0),
    )(*args)


def rope_fwd(x, cos_t, sin_t):
    half = x.shape[-1] // 2
    a, b = x[:, :half], x[:, half:]
    return a * cos_t - b * sin_t, b * cos_t + a * sin_t


def rope_bwd(a, b, cos_t, sin_t):
    return a * cos_t + b * sin_t, b * cos_t - a * sin_t


def pre_kernel(me_ref, h_ref, gain_ref, wk_ref, wv_ref, cos_ref, sin_ref, u_ref, kv_ref):
    n, sl, dim = h_ref.shape
    x = h_ref[...].reshape(n * sl, dim).astype(F32)
    inv = lax.rsqrt(jnp.mean(x * x, axis=-1, keepdims=True) + EPS)
    u = (x * inv * gain_ref[...]).astype(BF)
    u_ref[...] = u.reshape(n, sl, dim)
    hd = wk_ref.shape[1]
    k, v = dot_nn(u, wk_ref[...]), dot_nn(u, wv_ref[...])
    for i in range(n):
        first, second = rope_fwd(k[i * sl : (i + 1) * sl], cos_ref[...], sin_ref[...])
        kv_ref[i, :, : hd // 2] = first.astype(BF)
        kv_ref[i, :, hd // 2 : hd] = second.astype(BF)
        kv_ref[i, :, hd:] = v[i * sl : (i + 1) * sl].astype(BF)


def attn_fwd_kernel(me_ref, pre_ref, val_ref, u_ref, w0_ref, w1_ref, w2_ref, w3_ref, k0_ref, k1_ref, k2_ref, k3_ref, cos_ref, sin_ref, token_ref,
                    q_ref, pt_ref, mix_ref, keys_ref, vt_ref, s_ref):
    b = pl.program_id(0)
    cols = w0_ref.shape[1]
    _, hd = keys_ref.shape
    sl = u_ref.shape[1]
    heads = q_ref.shape[2] // hd
    u = u_ref[0]
    me = me_ref[0]
    cos_t, sin_t = cos_ref[...], sin_ref[...]
    place = []
    for r, kv_ref in enumerate((k0_ref, k1_ref, k2_ref, k3_ref)):
        keys_ref[r * sl : (r + 1) * sl, :] = kv_ref[0, :, :hd]
        vt_ref[:, r * sl : (r + 1) * sl] = kv_ref[0, :, hd:].astype(F32).T.astype(BF)
        place.append(lax.broadcasted_iota(jnp.int32, (sl, sl), 0) + (me ^ r) * sl)
    for r, w_ref in enumerate((w0_ref, w1_ref, w2_ref, w3_ref)):
        qs = dot_nn(u, w_ref[...])
        for j in range(cols // hd):
            base = r * cols + j * hd
            first, second = rope_fwd(qs[:, j * hd : (j + 1) * hd], cos_t, sin_t)
            q_ref[0, :, base : base + hd // 2] = first.astype(BF)
            q_ref[0, :, base + hd // 2 : base + hd] = second.astype(BF)
    prefix, valid = pre_ref[b], val_ref[b]
    q_end = lax.broadcasted_iota(jnp.int32, (1, sl), 1) + (me * sl + 1)
    limit = jnp.minimum(valid, jnp.maximum(prefix, q_end))
    visible = jnp.concatenate(place, axis=0) < limit
    scale = (hd**-0.5) * math.log2(math.e)

    def scores(h):
        return dot_nt(keys_ref[...], q_ref[0, :, h * hd : (h + 1) * hd])

    s_ref[0] = scores(0)
    for h in range(heads):
        if h + 1 < heads:
            s_ref[(h + 1) % 2] = scores(h + 1)
        sc = jnp.where(visible, s_ref[h % 2], -1e30)
        top = jnp.max(sc, axis=0, keepdims=True)
        e = jnp.exp2((sc - top) * scale)
        p = (e * (1.0 / jnp.sum(e, axis=0, keepdims=True))).astype(BF)
        pt_ref[0, :, h * sl : (h + 1) * sl] = p
        mix_ref[0, :, h * hd : (h + 1) * hd] = dot_nn(vt_ref[...], p).T.astype(BF)


def weight_copies(refs, dst, axis, sems):
    at, copies = 0, []
    for i, ref in enumerate(refs):
        n = ref.shape[axis]
        copies.append(pltpu.make_async_copy(ref, dst.at[pl.ds(at, n), :] if axis == 0 else dst.at[:, pl.ds(at, n)], sems.at[i]))
        at += n
    return copies


def start_first(*fetch):
    @pl.when(pl.program_id(0) == 0)
    def _():
        for c in weight_copies(*fetch):
            c.start()


def wait_first(*fetch):
    @pl.when(pl.program_id(0) == 0)
    def _():
        for c in weight_copies(*fetch):
            c.wait()


def out_kernel(mix_ref, w0_ref, w1_ref, w2_ref, w3_ref, h_ref, gain_ref, *rest):
    resid_ref, z_ref, wo_ref, sems = rest[-4:]
    fetch = (w0_ref, w1_ref, w2_ref, w3_ref), wo_ref, 0, sems
    start_first(*fetch)
    wait_first(*fetch)
    x = (h_ref[0].astype(F32) + dot_nn(mix_ref[0], wo_ref[...])).astype(BF)
    resid_ref[0] = x
    x = x.astype(F32)
    inv = lax.rsqrt(jnp.mean(x * x, axis=-1, keepdims=True) + EPS)
    z_ref[0] = (x * inv * gain_ref[...]).astype(BF)


class Flow:
    def __init__(self, bufs, sems, inward, sides):
        self.bufs, self.sems, self.inward, self.sides = bufs, sems, inward, sides

    def copies(self, t, slot, only):
        out = []
        for i, (hbm, buf) in enumerate(zip(self.sides(t), self.bufs)):
            if only is None or i == only:
                pair = (hbm, buf.at[slot]) if self.inward else (buf.at[slot], hbm)
                out.append(pltpu.make_async_copy(*pair, self.sems.at[slot, i]))
        return out

    def start(self, t, slot, only=None):
        for c in self.copies(t, slot, only):
            c.start()

    def wait(self, t, slot, only=None):
        for c in self.copies(t, slot, only):
            c.wait()


def local_copies(pairs, sems):
    return [pltpu.make_async_copy(src, dst, sems.at[i]) for i, (src, dst) in enumerate(pairs)]


def start_all(copies):
    for c in copies:
        c.start()


def wait_all(copies):
    for c in copies:
        c.wait()


def span(t, n):
    return pl.ds(t * n if isinstance(t, int) else pl.multiple_of(t * n, n), n)


OWN, MATE, FAR = 0, 1, 2


def dact_kernel(kind, me_ref, *refs):
    n_in, n_out = (2, 2) if kind == FAR else (1, 5 if kind == OWN else 3)
    gs, wd_ref = refs[:n_in], refs[n_in]
    outs, (wb, ob, gv, w_sem, o_sem, g_sem, c_sem) = refs[-7 - n_out : -7], refs[-7:]
    da_ref, homes = outs[0], outs[1:]
    half = gv.shape[0] // 2
    chip, core = me_ref[0] // 2, me_ref[0] % 2
    halves = [gv.at[pl.ds(c * half, half)] for c in range(2)]
    if kind == FAR:
        loads = local_copies(zip(gs, halves), g_sem)
        puts = [(halves[0], homes[0].at[1 - chip, core]), (halves[1], homes[0].at[1 - chip, 1 - core])]
    else:
        loads = local_copies([(gs[0], gv)], g_sem)
        puts = [(halves[c], homes[c].at[chip, core if kind == OWN else 1 - core]) for c in range(2)]
        puts += list(zip(halves, homes[2:]))
    puts = local_copies(puts, c_sem)
    bn = ob.shape[-1]
    steps = wd_ref.shape[0] // bn
    w_flow = Flow((wb,), w_sem, True, lambda t: (wd_ref.at[span(t, bn)],))
    o_flow = Flow((ob,), o_sem, False, lambda t: (da_ref.at[:, :, span(t, bn)],))
    start_all(loads)
    w_flow.start(0, 0)
    wait_all(loads)
    start_all(puts)

    @pl.loop(0, steps)
    def _(t):
        slot = lax.rem(t, 2)

        @pl.when(t + 1 < steps)
        def _():
            w_flow.start(t + 1, 1 - slot)

        @pl.when(t >= 2)
        def _():
            o_flow.wait(t - 2, slot)

        w_flow.wait(t, slot)
        g = gv[...].reshape(2 * half * gv.shape[1], gv.shape[2])
        ob[slot] = dot_nt(g, wb[slot]).astype(BF).reshape(ob.shape[1:])
        o_flow.start(t, slot)

    for t in (steps - 2, steps - 1):
        o_flow.wait(t, t % 2)
    wait_all(puts)


def gated(gate, up, da):
    c0 = math.sqrt(2.0 / math.pi)
    c1 = c0 * 0.044715
    x2 = gate * gate
    hh = 0.5 + 0.5 * jnp.tanh(gate * (c0 + c1 * x2))
    gelu = gate * hh
    slope = hh + gelu * ((1.0 - hh) * (2.0 * c0 + 6.0 * c1 * x2))
    return (gelu * up).astype(BF), (da * up * slope).astype(BF), (da * gelu).astype(BF)


def mlp_kernel(other, at, fused, me_ref, *refs):
    za, zb, da, db, wg_ref, wu_ref = refs[:6]
    n_out, n_scr = (5, 13) if fused else (4, 11)
    outs, scr = refs[-n_scr - n_out : -n_scr], refs[-n_scr:]
    zv, wgb, wub, act_b, dg_b, du_b, in_sem, o_sem, z_sem, c_sem = scr[:10]
    chip = abs(other - me_ref[0] // 2)
    core = me_ref[0] % 2
    rows, bn = act_b.shape[2:]
    dim = zv.shape[-1]
    steps = wg_ref.shape[1] // bn
    if fused:
        wdb, gv, g_sem = scr[10:]
        wd_ref = refs[6]
        in_flow = Flow((wgb, wub, wdb), in_sem, True, lambda t: (wg_ref.at[:, span(t, bn)], wu_ref.at[:, span(t, bn)], wd_ref.at[span(t, bn)]))
    else:
        dv = scr[10]
        in_flow = Flow((wgb, wub, dv.at[:, 0], dv.at[:, 1]), in_sem, True,
                       lambda t: (wg_ref.at[:, span(t, bn)], wu_ref.at[:, span(t, bn)], da.at[at[0], :, span(t, bn)], db.at[at[1], :, span(t, bn)]))
    bufs = (act_b, dg_b, du_b)
    o_flow = Flow([b.at[:, rel] for rel in range(2) for b in bufs], o_sem, False,
                  lambda t: [o.at[chip, abs(rel - core), :, span(t, bn)] for rel in range(2) for o in outs[:3]])
    loads = local_copies([(za, zv.at[0]), (zb, zv.at[1])], z_sem)
    puts = [(zv.at[0], outs[3].at[chip, core]), (zv.at[1], outs[3].at[chip, 1 - core])]
    if fused:
        loads += local_copies([(da, gv.at[0]), (db, gv.at[1])], g_sem)
        puts += [(gv.at[0], outs[4].at[chip, core]), (gv.at[1], outs[4].at[chip, 1 - core])]
    puts = local_copies(puts, c_sem)
    in_flow.start(0, 0)
    start_all(loads)
    wait_all(loads)
    start_all(puts)
    n = rows // (3 if fused else 2)

    @pl.loop(0, steps)
    def _(t):
        slot = lax.rem(t, 2)

        @pl.when(t + 1 < steps)
        def _():
            in_flow.start(t + 1, 1 - slot)

        @pl.when(t >= 2)
        def _():
            o_flow.wait(t - 2, slot)

        in_flow.wait(t, slot)
        for rel in range(2):
            z = zv[rel].reshape(rows, dim)
            for r in range(0, rows, n):
                gate, up = dot_nn(z[r : r + n], wgb[slot]), dot_nn(z[r : r + n], wub[slot])
                if fused:
                    d = dot_nt(gv[rel].reshape(rows, dim)[r : r + n], wdb[slot])
                else:
                    d = dv[slot, rel, r : r + n, :].astype(F32)
                for buf, o in zip(bufs, gated(gate, up, d)):
                    buf[slot, rel, r : r + n, :] = o
        o_flow.start(t, slot)

    for t in (steps - 2, steps - 1):
        o_flow.wait(t, t % 2)
    wait_all(puts)


def attn_bwd_kernel(me_ref, dz0_ref, dz1_ref, res_ref, go_ref, gain_ref, w0_ref, w1_ref, w2_ref, w3_ref, k0_ref, k1_ref, k2_ref, k3_ref,
                    q_ref, pt_ref, cos_ref, sin_ref, token0_ref, token1_ref, token2_ref,
                    dres_ref, dq_ref, dkv_ref, gn_ref, kt_ref, v_ref, do_ref, qs_ref, ds_ref, dp_ref, dk_ref, dv_ref):
    b = pl.program_id(0)
    half = pl.num_programs(0) // 2
    seq, hd = v_ref.shape
    sl = q_ref.shape[1]
    heads = q_ref.shape[2] // hd
    me = me_ref[0]
    x = res_ref[0].astype(F32)
    dz = jnp.where(b < half, dz0_ref[0], dz1_ref[0]).astype(F32)
    inv = lax.rsqrt(jnp.mean(x * x, axis=-1, keepdims=True) + EPS)
    xn = x * inv
    part = jnp.sum(dz * xn, axis=0, keepdims=True)

    @pl.when(b == 0)
    def _():
        gn_ref[...] = part

    @pl.when(b > 0)
    def _():
        gn_ref[...] += part

    dxn = dz * gain_ref[...]
    dx = inv * (dxn - xn * jnp.mean(dxn * xn, axis=-1, keepdims=True))
    dres = (go_ref[0].astype(F32) + dx).astype(BF)
    dres_ref[0] = dres
    scale = hd**-0.5
    for r, kv_ref in enumerate((k0_ref, k1_ref, k2_ref, k3_ref)):
        kt_ref[:, r * sl : (r + 1) * sl] = (kv_ref[0, :, :hd].astype(F32) * scale).T.astype(BF)
        v_ref[r * sl : (r + 1) * sl, :] = kv_ref[0, :, hd:]
    w_refs = (w0_ref, w1_ref, w2_ref, w3_ref)
    per = w0_ref.shape[0] // hd

    def d_mixed(r):
        dm = dot_nt(dres, w_refs[r][...]).astype(BF)
        for j in range(per):
            h = r * per + j
            do_ref[h * sl : (h + 1) * sl, :] = dm[:, j * hd : (j + 1) * hd]
            qs_ref[h * sl : (h + 1) * sl, :] = (q_ref[0, :, h * hd : (h + 1) * hd].astype(F32) * scale).astype(BF)

    cos_t, sin_t = cos_ref[...], sin_ref[...]

    def dprobs(h):
        return dot_nt(v_ref[...], do_ref[h * sl : (h + 1) * sl, :])

    def add_kv(r, first):
        at = pl.ds(r * per * sl, per * sl)
        dk, dv = dot_nn(ds_ref[:, at], qs_ref[at, :]), dot_nn(pt_ref[0, :, at], do_ref[at, :])
        if first:
            dk_ref[...], dv_ref[...] = dk, dv
        else:
            dk_ref[...] += dk
            dv_ref[...] += dv

    d_mixed(0)
    dp_ref[0] = dprobs(0)
    for h in range(heads):
        if h % per == 0:
            if h // per + 1 < len(w_refs):
                d_mixed(h // per + 1)
            if h:
                add_kv(h // per - 1, h == per)
        if h + 1 < heads:
            dp_ref[(h + 1) % 2] = dprobs(h + 1)
        p = pt_ref[0, :, h * sl : (h + 1) * sl].astype(F32)
        t = p * dp_ref[h % 2]
        ds = (t - p * jnp.sum(t, axis=0, keepdims=True)).astype(BF)
        ds_ref[:, h * sl : (h + 1) * sl] = ds
        dq = dot_nn(kt_ref[...], ds).T
        first, second = rope_bwd(dq[:, : hd // 2], dq[:, hd // 2 :], cos_t, sin_t)
        dq_ref[0, :, h * hd : h * hd + hd // 2] = first.astype(BF)
        dq_ref[0, :, h * hd + hd // 2 : (h + 1) * hd] = second.astype(BF)
    at = pl.ds((heads - per) * sl, per * sl)
    dk = (dk_ref[...] + dot_nn(ds_ref[:, at], qs_ref[at, :])).astype(BF)
    dv = (dv_ref[...] + dot_nn(pt_ref[0, :, at], do_ref[at, :])).astype(BF)
    for r in range(seq // sl):
        dkv_ref[me ^ r, 0, :, :hd] = dk[r * sl : (r + 1) * sl]
        dkv_ref[me ^ r, 0, :, hd:] = dv[r * sl : (r + 1) * sl]


def last_kernel(me_ref, dkv_ref, dq_ref, u_ref, h_ref, dres_ref, gain_ref, w0_ref, w1_ref, w2_ref, w3_ref, wk_ref, wv_ref, cos_ref, sin_ref, gm_ref,
                token0_ref, gh_ref, gkv_ref, acc_ref, w_ref, d_ref, sems):
    b = pl.program_id(0)
    dim, hd = wk_ref.shape
    qd = dq_ref.shape[2]
    fetch = (w0_ref, w1_ref, w2_ref, w3_ref, wk_ref, wv_ref), w_ref, 1, sems
    start_first(*fetch)
    wait_first(*fetch)
    raw = dkv_ref[0]
    dk = raw[:, :hd].astype(F32)
    first, second = rope_bwd(dk[:, : hd // 2], dk[:, hd // 2 :], cos_ref[...], sin_ref[...])
    d_ref[:, :qd] = dq_ref[0]
    d_ref[:, qd : qd + hd // 2] = first.astype(BF)
    d_ref[:, qd + hd // 2 : qd + hd] = second.astype(BF)
    d_ref[:, qd + hd :] = raw[:, hd:]
    gk = dot_tn(u_ref[0], d_ref[:, qd:])
    dn = dot_nt(d_ref[...], w_ref[...])
    x = h_ref[0].astype(F32)
    inv = lax.rsqrt(jnp.mean(x * x, axis=-1, keepdims=True) + EPS)
    xn = x * inv
    part = jnp.sum(dn * xn, axis=0, keepdims=True)
    dxn = dn * gain_ref[...]
    dx = inv * (dxn - xn * jnp.mean(dxn * xn, axis=-1, keepdims=True))
    gh_ref[0] = (dres_ref[0].astype(F32) + dx).astype(BF)

    @pl.when(b == 0)
    def _():
        acc_ref[...] = part
        gkv_ref[:dim, :] = gk

    @pl.when(b > 0)
    def _():
        acc_ref[...] += part
        gkv_ref[:dim, :] += gk

    @pl.when(b == pl.num_programs(0) - 1)
    def _():
        width = 2 * hd
        per = dim // width
        for i in range(per):
            gkv_ref[dim + i : dim + i + 1, :] = gm_ref[:, i * width : (i + 1) * width]
            gkv_ref[dim + per + i : dim + per + i + 1, :] = acc_ref[:, i * width : (i + 1) * width]


def block_grad_kernel(*refs):
    x_ref, y_ref, o_ref = refs[-4], refs[-3], refs[-1]
    o_ref[...] = dot_tn(x_ref[...], y_ref[...]).reshape(o_ref.shape)


def gated_grad_kernel(dg_ref, du_ref, wg_ref, wu_ref, *rest):
    o_ref, a1, a2, b1, b2, ob, a_sem, b_sem, o_sem = rest[-9:]
    ni = dg_ref.shape[0] * dg_ref.shape[1]
    bn = b1.shape[1]
    nj = wg_ref.shape[0] // bn
    steps = ni * nj
    cols = lambda t: pl.ds(pl.multiple_of(lax.rem(t, nj) * bn, bn), bn)
    a_flow = Flow((a1, a2), a_sem, True, lambda i: (dg_ref.at[i // 2, i % 2], du_ref.at[i // 2, i % 2]))
    b_flow = Flow((b1, b2), b_sem, True, lambda t: (wg_ref.at[cols(t)], wu_ref.at[cols(t)]))
    o_flow = Flow((ob,), o_sem, False, lambda t: (o_ref.at[t // nj, :, cols(t)],))
    for k in range(2):
        a_flow.start(0, 0, k)
        b_flow.start(0, 0, k)
    b_flow.start(1, 1)
    a_flow.start(1, 1)
    for k in range(2):
        a_flow.wait(0, 0, k)
        b_flow.wait(0, 0, k)
        if k == 0:
            first = dot_nt(a1[0], b1[0])
    ob[0] = (first + dot_nt(a2[0], b2[0])).astype(BF)
    o_flow.start(0, 0)

    @pl.loop(1, steps)
    def _(t):
        i, slot = t // nj, lax.rem(t, 2)
        a_slot = lax.rem(i, 2)

        @pl.when(t + 1 < steps)
        def _():
            b_flow.start(t + 1, 1 - slot)

        @pl.when(lax.rem(t, nj) == 0)
        def _():
            a_flow.wait(i, a_slot)

            @pl.when(i + 1 < ni)
            def _():
                a_flow.start(i + 1, 1 - a_slot)

        @pl.when(t >= 2)
        def _():
            o_flow.wait(t - 2, slot)

        b_flow.wait(t, slot)
        ob[slot] = (dot_nt(a1[a_slot], b1[slot]) + dot_nt(a2[a_slot], b2[slot])).astype(BF)
        o_flow.start(t, slot)

    for t in (steps - 2, steps - 1):
        o_flow.wait(t, t % 2)


def mlp_out_kernel(mine, me_ref, act_ref, wd_ref, *refs):
    outs, (ab, wb, ob, pb, a_sem, w_sem, o_sem, p_sem) = refs[-9 - mine : -8], refs[-8:]
    chip, core = me_ref[0] // 2, me_ref[0] % 2
    core = core if mine else 1 - core
    bn = wb.shape[2]
    nj = wd_ref.shape[1] // bn
    a_flow = Flow((ab,), a_sem, True, lambda i: (act_ref.at[abs(1 - i - chip), core],))
    w_flow = Flow((wb,), w_sem, True, lambda t: (wd_ref.at[:, span(t % nj, bn)],))
    p_flow = Flow((pb,), p_sem, True, lambda t: (refs[0].at[1 - t // nj, :, span(t % nj, bn)],))
    if mine:
        o_flow = Flow((ob,), o_sem, False, lambda t: (outs[t // nj].at[:, span(t % nj, bn)],))
    else:
        o_flow = Flow((ob,), o_sem, False, lambda t: (outs[0].at[1 - t // nj, :, span(t % nj, bn)],))
    steps = 2 * nj
    for i in range(2):
        a_flow.start(i, i)
        w_flow.start(i, i)
        if mine:
            p_flow.start(i, i)
    for t in range(steps):
        slot = t % 2
        if t % nj == 0:
            a_flow.wait(t // nj, t // nj)
        w_flow.wait(t, slot)
        if t >= 2:
            o_flow.wait(t - 2, slot)
        out = dot_nn(ab[t // nj], wb[slot])
        if mine:
            p_flow.wait(t, slot)
            out = out + pb[slot].astype(F32)
        ob[slot] = out.astype(BF)
        o_flow.start(t, slot)
        if t + 2 < steps:
            w_flow.start(t + 2, slot)
            if mine:
                p_flow.start(t + 2, slot)
    for t in (steps - 2, steps - 1):
        o_flow.wait(t, t % 2)


def weight_grads_kernel(count, first, ni, side, *refs):
    x_refs, y_refs = refs[:2], refs[2 : 2 + 2 * count]
    if side:
        res_ref, p0_ref, p1_ref, q1_ref = refs[2 + 2 * count : 6 + 2 * count]
        ho_ref, (rb, sb, tb, hb, s_sem, h_sem) = refs[-15], refs[-6:]
        refs = refs[:-15] + refs[-14:-6]
    o_refs, (x0, x1, y0, y1, ob, x_sem, y_sem, o_sem) = refs[-8 - count : -8], refs[-8:]
    bm, bn = ob.shape[1:]
    nj = y_refs[0].shape[1] // bn
    steps = ni * count * nj
    per = count * nj
    rows = lambda i: pl.ds(pl.multiple_of((first + i) * bm, bm), bm)
    cols = lambda t: pl.ds(pl.multiple_of(lax.rem(t, nj) * bn, bn), bn)
    if side:
        n = rb.shape[1]
        turn = p0_ref.shape[0] // n
        at = lambda t: pl.ds(pl.multiple_of(t * n, n), n)
        later = lambda t: at(jnp.maximum(t - turn, 0))
        side_in = [Flow((rb, sb, tb), s_sem, True, lambda t: (res_ref.at[at(t)], p0_ref.at[at(jnp.minimum(t, turn - 1))], q1_ref.at[later(t)])),
                   Flow((rb, sb, tb), s_sem, True, lambda t: (res_ref.at[at(t)], p1_ref.at[later(t)], q1_ref.at[later(t)]))]
        side_out = Flow((hb,), h_sem, False, lambda t: (ho_ref.at[at(t)],))

        def side_start(t, slot):
            pl.when(t < turn)(lambda: side_in[0].start(t, slot))
            pl.when(t >= turn)(lambda: side_in[1].start(t, slot))

        def side_work(t, slot):
            extra = tb[slot].astype(F32) * jnp.where(t < turn, 0.0, 1.0)
            hb[slot] = (rb[slot].astype(F32) + sb[slot].astype(F32) + extra).astype(BF)

    x_flow = Flow((x0, x1), x_sem, True, lambda i: [r.at[:, rows(i)] for r in x_refs])
    y_flows = [Flow((y0, y1), y_sem, True, lambda t, k=k: [r.at[:, cols(t)] for r in y_refs[2 * k : 2 * k + 2]]) for k in range(count)]
    o_flows = [Flow((ob,), o_sem, False, lambda t, k=k: (o_refs[k].at[rows(t // per), cols(t)],)) for k in range(count)]

    def each(flows, t, act):
        if count == 1:
            act(flows[0])
        else:
            which = lax.rem(t // nj, count)
            for k in range(count):
                pl.when(which == k)(functools.partial(act, flows[k]))

    for k in range(2):
        x_flow.start(0, 0, k)
        y_flows[0].start(0, 0, k)
    y_flows[0].start(1, 1)
    if side:
        side_in[0].start(0, 0)
        side_in[0].start(1, 1)
        side_in[0].wait(0, 0)
        side_work(0, 0)
        side_out.start(0, 0)
    if ni > 1:
        x_flow.start(1, 1)
    for k in range(2):
        x_flow.wait(0, 0, k)
        y_flows[0].wait(0, 0, k)
        if k == 0:
            part = dot_tn(x0[0], y0[0])
    ob[0] = part + dot_tn(x1[0], y1[0])
    o_flows[0].start(0, 0)

    @pl.loop(1, steps)
    def _(t):
        i, slot = t // per, lax.rem(t, 2)
        x_slot = lax.rem(i, 2)

        @pl.when(t + 1 < steps)
        def _():
            each(y_flows, t + 1, lambda f: f.start(t + 1, 1 - slot))
            if side:
                pl.when(t > 0)(lambda: side_start(t + 1, 1 - slot))

        @pl.when(lax.rem(t, per) == 0)
        def _():
            x_flow.wait(i, x_slot)

            @pl.when(i + 1 < ni)
            def _():
                x_flow.start(i + 1, 1 - x_slot)

        @pl.when(t >= 2)
        def _():
            o_flows[0].wait(t - 2, slot)
            if side:
                side_out.wait(t - 2, slot)

        y_flows[0].wait(t, slot)
        if side:
            side_in[0].wait(t, slot)
            side_work(t, slot)
        ob[slot] = dot_tn(x0[x_slot], y0[slot]) + dot_tn(x1[x_slot], y1[slot])
        if side:
            side_out.start(t, slot)
        each(o_flows, t, lambda f: f.start(t, slot))

    for t in (steps - 2, steps - 1):
        o_flows[0].wait(t, t % 2)
        if side:
            side_out.wait(t, t % 2)


def split_kernel(x_ref, k_ref, v_ref, m_ref, a_ref):
    dim, hd = k_ref.shape
    k_ref[...], v_ref[...] = x_ref[:dim, :hd], x_ref[:dim, hd:]
    for j, o_ref in enumerate((m_ref, a_ref)):
        n = dim // (2 * hd)
        for i in range(n):
            o_ref[:, i * 2 * hd : (i + 1) * 2 * hd] = x_ref[dim + j * n + i : dim + j * n + i + 1, :]


def tie_kernel(x_ref, *rest):
    del x_ref, rest


def tie(x, *tokens):
    return pl.pallas_call(
        tie_kernel,
        name="tie",
        in_specs=[ANY] * (1 + len(tokens)),
        out_specs=ANY,
        out_shape=jax.ShapeDtypeStruct(x.shape, x.dtype),
        input_output_aliases={0: 0},
    )(x, *tokens)


def solution(mesh):
    act_spec = P("dp", "tp", None)
    in_specs = (act_spec, act_spec, P("dp"), P("dp"), P(None), P(None, "tp"), P(None, None), P(None, None), P("tp", None), P(None), P(None, "tp"), P(None, "tp"), P("tp", None))
    out_specs = (act_spec, act_spec, P("dp"), P("dp", "tp"), P("dp", None), P("dp", None), P(("dp", "tp"), None), P("dp"), P("dp", "tp"), P("dp", "tp"), P(("dp", "tp"), None))
    core_flip = [(0, 1), (1, 0), (2, 3), (3, 2)]
    chip_flip = [(0, 2), (2, 0), (1, 3), (3, 1)]

    def to_core(x):
        return lax.ppermute(x, "tp", core_flip)

    def to_chip(x):
        return lax.ppermute(x, "tp", chip_flip)

    def local_layer(hidden, grad_out, prefix_len, valid_len, attn_norm, w_query, w_key, w_value, w_out, mlp_norm, w_gate, w_up, w_down):
        batch, sl, dim = hidden.shape
        half = batch // 2
        rows = half * sl
        hd = w_key.shape[1]
        cols = w_query.shape[1]
        tp_n = mesh.shape["tp"]
        seq = sl * tp_n
        qd = cols * tp_n
        heads = qd // hd
        ffn = w_gate.shape[1]
        own = batch * sl
        me = lax.axis_index("tp").astype(jnp.int32).reshape(1)

        inv_freq = np.exp(np.arange(hd // 2, dtype=np.float32) * np.float32(2.0 / hd) * np.float32(-math.log(10000.0)))
        angles = np.arange(seq, dtype=np.float32)[:, None] * inv_freq[None, :]
        cos_t, sin_t = jnp.asarray(np.cos(angles)), jnp.asarray(np.sin(angles))
        gain1 = (1.0 + attn_norm.astype(F32)).reshape(1, dim)
        gain2 = (1.0 + mlp_norm.astype(F32)).reshape(1, dim)

        def sds(shape, dtype=BF):
            return jax.ShapeDtypeStruct(shape, dtype)

        def block(shape, at, single=False):
            return pl.BlockSpec(shape, at, pipeline_mode=pl.Buffered(1) if single else None)

        tok_spec = block((1, sl, dim), lambda b, *_: (b, 0, 0))
        q_spec = block((1, sl, qd), lambda b, *_: (b, 0, 0))
        kv_spec = block((1, sl, 2 * hd), lambda b, *_: (b, 0, 0))
        kv4_spec = block((tp_n, 1, sl, 2 * hd), lambda b, *_: (0, b, 0, 0))
        pt_spec = block((1, seq, heads * sl), lambda b, *_: (b, 0, 0))
        rope_spec = block((sl, hd // 2), lambda b, m, *_: (m[0], 0), True)
        gain_spec = const_spec((1, dim))
        dma = lambda n: pltpu.SemaphoreType.DMA((n,))

        wq_far = to_chip(w_query)
        wq_mate = to_core(w_query)
        g_mate = to_core(grad_out)
        u, kv = run(
            pre_kernel, (batch // 2,),
            [block((2, sl, dim), lambda b, *_: (b, 0, 0)), gain_spec, const_spec((dim, hd)), const_spec((dim, hd)), rope_spec, rope_spec],
            [block((2, sl, dim), lambda b, *_: (b, 0, 0)), block((2, sl, 2 * hd), lambda b, *_: (b, 0, 0))],
            [sds((batch, sl, dim)), sds((batch, sl, 2 * hd))],
            (me, hidden, gain1, w_key, w_value, cos_t, sin_t), prefetch=1,
            flops=4 * own * dim * hd, nbytes=6 * own * dim)
        kv_far = to_chip(kv)
        kv_mate = to_core(kv)
        wo_far = to_chip(w_out)
        wo_mate = to_core(w_out)

        bn = 512
        cat_shape = (2, 2, half, sl, dim)
        SMEM = pl.BlockSpec(memory_space=pltpu.SMEM)
        bd = 1024

        def dact(kind, gs, homes, tokens, n_out):
            return run(
                functools.partial(dact_kernel, kind), (), [SMEM] + [ANY] * (len(gs) + 1 + len(homes) + len(tokens)), [ANY] * n_out,
                ([sds((2, rows, ffn))] + [sds(cat_shape)] * 2 + [sds((half, sl, dim))] * 2)[: n_out],
                (me, *gs, w_down, *homes, *tokens), aliases={2 + len(gs) + i: 1 + i for i in range(len(homes))},
                scratch=[pltpu.VMEM((2, bd, dim), BF), pltpu.VMEM((2, 2, rows, bd), BF), pltpu.VMEM((batch, sl, dim), BF),
                         pltpu.SemaphoreType.DMA((2, 1)), pltpu.SemaphoreType.DMA((2, 1)), dma(2), dma(4)],
                flops=4 * rows * dim * ffn, nbytes=2 * ffn * dim + 4 * rows * ffn)

        da_own, gcat0, gcat1, go0, go1 = dact(OWN, (grad_out,), (), (kv,), 5)
        wq_far = tie(wq_far, da_own)
        wq_far_mate = to_core(wq_far)
        da_mate, gcat0, gcat1 = dact(MATE, (g_mate,), (gcat0, gcat1), (da_own,), 3)
        kv_far = tie(kv_far, da_mate)
        kv_far_mate = to_core(kv_far)
        wqs = (w_query, wq_mate, wq_far, wq_far_mate)
        kvs = (kv, kv_mate, kv_far, kv_far_mate)
        wq_specs = [const_spec((dim, cols))] * 4
        wo_specs = [const_spec((cols, dim))] * 4

        q, pt, mixed = run(
            attn_fwd_kernel, (batch,),
            [tok_spec] + wq_specs + [kv_spec] * 4 + [rope_spec, rope_spec, ANY],
            [q_spec, pt_spec, q_spec],
            [sds((batch, sl, qd)), sds((batch, seq, heads * sl)), sds((batch, sl, qd))],
            (me, prefix_len, valid_len, u, *wqs, *kvs, cos_t, sin_t, da_mate), prefetch=3,
            scratch=[pltpu.VMEM((seq, hd), BF), pltpu.VMEM((hd, seq), BF), pltpu.VMEM((2, seq, sl), F32)],
            flops=2 * own * dim * qd + 4 * own * seq * qd, nbytes=2 * own * heads * seq)
        wo_far = tie(wo_far, mixed)
        wo_far_mate = to_core(wo_far)
        wos = (w_out, wo_mate, wo_far, wo_far_mate)

        g_far = [to_chip(tie(go0, mixed))]

        def out_proj(c, prev):
            at = lambda b: (b + c * half, 0, 0)
            extra = [prev] if c else []
            return run(
                out_kernel, (half,),
                [block((1, sl, qd), at)] + [ANY] * 4 + [block((1, sl, dim), at), gain_spec] + [ANY] * len(extra),
                [block((1, sl, dim), at), block((1, sl, dim), lambda b: (b, 0, 0))],
                [sds((batch, sl, dim)), sds((half, sl, dim))],
                (mixed, *wos, hidden, gain2, *extra), aliases={7: 0} if c else None,
                scratch=[pltpu.VMEM((qd, dim), BF), dma(4)],
                flops=own * dim * qd, nbytes=4 * own * dim)

        resid, z0 = out_proj(0, None)
        resid, z1 = out_proj(1, resid)
        zs = [z0, z1]
        z_mate = [to_core(z) for z in zs]
        z_far = [to_chip(z0)]
        z_far.append(to_chip(z1))
        g_far.append(to_chip(tie(go1, z1)))

        o_shape = (2, 2, rows, ffn)

        def mlp(other, at, fused, za, zb, da, db, prev, tokens):
            n_out = 5 if fused else 4
            weights = (w_gate, w_up, w_down) if fused else (w_gate, w_up)
            sem = lambda k, n: pltpu.SemaphoreType.DMA((k, n))
            scratch = [pltpu.VMEM((2, half, sl, dim), BF)] + [pltpu.VMEM((2, dim, bn), BF)] * 2 + [pltpu.VMEM((2, 2, rows, bn), BF)] * 3
            scratch += [sem(2, 3 if fused else 4), sem(2, 6), dma(2), dma(4)]
            scratch += [pltpu.VMEM((2, bn, dim), BF), pltpu.VMEM((2, half, sl, dim), BF), dma(2)] if fused else [pltpu.VMEM((2, 2, rows, bn), BF)]
            return run(
                functools.partial(mlp_kernel, other, at, fused), (),
                [SMEM] + [ANY] * (4 + len(weights) + len(prev) + len(tokens)), [ANY] * n_out,
                [sds(o_shape)] * 3 + [sds(cat_shape)] * (n_out - 3),
                (me, za, zb, da, db, *weights, *prev, *tokens), scratch=scratch,
                aliases={5 + len(weights) + i: i for i in range(len(prev))},
                flops=(12 if fused else 8) * rows * dim * ffn, nbytes=4 * ffn * dim + 16 * rows * ffn)

        near0 = mlp(0, (0, 0), False, zs[0], z_mate[0], da_own, da_mate, (), (z1,))
        near1 = mlp(0, (1, 1), False, zs[1], z_mate[1], da_own, da_mate, (), (near0[0],))

        ga = tie(g_far[0], near0[0])
        gb = to_core(ga)
        da_far, gcat0 = dact(FAR, (ga, gb), (gcat0,), (near1[0],), 2)
        za = tie(z_far[0], near1[0])
        zb = to_core(za)
        full0 = mlp(1, (0, 1), False, za, zb, da_far, da_far, near0, ())

        def gated_grad(full):
            bj = 512
            return run(
                gated_grad_kernel, (), [ANY] * 5, ANY, sds((4, rows, dim)), (full[1], full[2], w_gate, w_up, full[0]),
                scratch=[pltpu.VMEM((2, rows, ffn), BF)] * 2 + [pltpu.VMEM((2, bj, ffn), BF)] * 2 + [pltpu.VMEM((2, rows, bj), BF)]
                + [pltpu.SemaphoreType.DMA((2, 2))] * 2 + [pltpu.SemaphoreType.DMA((2, 1))],
                flops=16 * rows * dim * ffn, nbytes=16 * rows * ffn)

        def mlp_out(full):
            return dot_nn(full[0].reshape(4 * rows, ffn), w_down).astype(BF)

        def scatter(x):
            return lax.psum_scatter(x.reshape(tp_n, rows, dim), "tp", scatter_dimension=0).reshape(half, sl, dim)

        dz_part0 = gated_grad(full0)
        dz0 = scatter(dz_part0)
        mlp_part0 = mlp_out(full0)
        part0 = scatter(mlp_part0)

        ga, za = tie(g_far[1], full0[0]), tie(z_far[1], full0[0])
        gb = to_core(ga)
        zb = to_core(za)
        full1 = mlp(1, None, True, za, zb, ga, gb, (*near1, gcat1), (dz_part0, mlp_part0))
        gcat1 = full1[4]
        dz_part1 = gated_grad(full1)
        dz1 = scatter(dz_part1)

        def mlp_out_half(mine, adds, token):
            bo = 1024
            dims = [(rows, dim)] * 2 if mine else [(2, rows, dim)]
            dma2 = pltpu.SemaphoreType.DMA((2, 1))
            return run(
                functools.partial(mlp_out_kernel, mine), (), [SMEM] + [ANY] * (3 + len(adds)), [ANY] * len(dims), [sds(d) for d in dims],
                (me, full1[0], w_down, *adds, token),
                scratch=[pltpu.VMEM((2, rows, ffn), BF), pltpu.VMEM((2, ffn, bo), BF), pltpu.VMEM((2, rows, bo), BF), pltpu.VMEM((2, rows, bo), BF), dma2, dma2, dma2, dma2],
                flops=4 * rows * dim * ffn, nbytes=2 * ffn * dim)

        mlp_mate, = mlp_out_half(False, (), dz_part1)
        mlp_from_mate = to_core(mlp_mate)

        def weight_grads(x, ys, tokens, first=0, ni=None, prev=None, by=512, side=()):
            flat = lambda pair: [a.reshape(4 * rows, -1) for a in pair]
            xs, yf = flat(x), [a for y in ys for a in flat(y)]
            m, n = xs[0].shape[1], yf[0].shape[1]
            bm = 1024
            extra = [prev] if prev is not None else []
            return run(
                functools.partial(weight_grads_kernel, len(ys), first, ni or m // bm, bool(side)), (),
                [ANY] * (2 + len(yf) + len(side) + len(extra) + len(tokens)), [ANY] * (len(ys) + bool(side)),
                [sds((m, n), F32)] * len(ys) + [sds(a.shape) for a in side[:1]],
                (*xs, *yf, *side, *extra, *tokens), aliases={2 + len(yf): 0} if extra else None,
                scratch=[pltpu.VMEM((2, 4 * rows, bm), BF)] * 2 + [pltpu.VMEM((2, 4 * rows, by), BF)] * 2 + [pltpu.VMEM((2, bm, by), F32)]
                + [pltpu.SemaphoreType.DMA((2, 2))] * 2 + [pltpu.SemaphoreType.DMA((2, 1))]
                + ([pltpu.VMEM((2, own // (m // bm * len(ys) * n // by), dim), BF)] * 4 + [pltpu.SemaphoreType.DMA((2, 3)), pltpu.SemaphoreType.DMA((2, 1))] if side else []),
                flops=16 * rows * (ni or m // bm) * bm * n * len(ys), nbytes=4 * m * n)

        down_args = (full0[0], full1[0]), ((gcat0, gcat1),)
        g_down = weight_grads(*down_args, (mlp_mate,), 0, 1)[0]
        mlp_far, mlp_own = mlp_out_half(True, (mlp_from_mate,), g_down)
        mlp_arrived = to_chip(mlp_far)

        d_resid, d_q, dkv_part, gn2 = run(
            attn_bwd_kernel, (batch,),
            [block((1, sl, dim), lambda b, *_: (jnp.minimum(b, half - 1), 0, 0)), block((1, sl, dim), lambda b, *_: (jnp.maximum(b - half, 0), 0, 0)),
             tok_spec, tok_spec, gain_spec] + wo_specs + [kv_spec] * 4 + [q_spec, pt_spec, rope_spec, rope_spec, ANY, ANY, ANY],
            [tok_spec, q_spec, kv4_spec, block((1, dim), lambda b, *_: (0, 0))],
            [sds((batch, sl, dim)), sds((batch, sl, qd)), sds((tp_n, batch, sl, 2 * hd)), sds((1, dim), F32)],
            (me, dz0, dz1, resid, grad_out, gain2, *wos, *kvs, q, pt, cos_t, sin_t, mlp_own, g_down, part0), prefetch=1,
            scratch=[pltpu.VMEM((hd, seq), BF), pltpu.VMEM((seq, hd), BF), pltpu.VMEM((heads * sl, hd), BF), pltpu.VMEM((heads * sl, hd), BF), pltpu.VMEM((seq, heads * sl), BF), pltpu.VMEM((2, seq, sl), F32)] + [pltpu.VMEM((seq, hd), F32)] * 2,
            flops=2 * own * dim * qd + 8 * own * seq * qd, nbytes=2 * own * heads * seq)
        dkv = lax.psum_scatter(dkv_part, "tp", scatter_dimension=0)

        mixed2, dres2, u2, dq2 = mixed.reshape(own, qd), d_resid.reshape(own, dim), u.reshape(own, dim), d_q.reshape(own, qd)
        x_spec, y_spec = block((own, dim), lambda j, *_: (0, 0), True), lambda pick: block((own, cols), lambda j, *_: (0, pick(j)))
        g_out = run(
            block_grad_kernel, (tp_n,), [y_spec(lambda j: j), x_spec, ANY],
            block((1, cols, dim), lambda j, m: (m[0] ^ j, 0, 0)), sds((tp_n, cols, dim), F32), (me, mixed2, dres2, dkv_part),
            prefetch=1, flops=2 * own * dim * qd, nbytes=4 * dim * qd)
        g_out_sum = lax.psum_scatter(g_out.reshape(qd, dim), "tp", scatter_dimension=0, tiled=True)
        g_query = run(
            block_grad_kernel, (tp_n,), [x_spec, y_spec(lambda j: j), ANY],
            block((1, dim, cols), lambda j, m: (m[0] ^ j, 0, 0)), sds((tp_n, dim, cols), F32), (me, u2, dq2, g_out),
            prefetch=1, flops=2 * own * dim * qd, nbytes=4 * dim * qd)
        g_query_sum = lax.psum_scatter(g_query.reshape(tp_n * dim, cols), "tp", scatter_dimension=0, tiled=True)
        g_down = weight_grads(*down_args, (g_query,), 1, ffn // 1024 - 1, g_down)[0]

        extra = dim // hd
        grad_hidden, gkv = run(
            last_kernel, (batch,),
            [kv_spec, q_spec, tok_spec, tok_spec, tok_spec, gain_spec] + [ANY] * 6 + [rope_spec, rope_spec, const_spec((1, dim)), ANY],
            [tok_spec, block((dim + extra, 2 * hd), lambda b, *_: (0, 0))],
            [sds((batch, sl, dim)), sds((dim + extra, 2 * hd), F32)],
            (me, dkv, d_q, u, hidden, d_resid, gain1, *wqs, w_key, w_value, cos_t, sin_t, gn2, g_down), prefetch=1,
            scratch=[pltpu.VMEM((1, dim), F32), pltpu.VMEM((dim, qd + 2 * hd), BF), pltpu.VMEM((sl, qd + 2 * hd), BF), dma(6)],
            flops=2 * own * dim * (qd + 4 * hd), nbytes=8 * own * dim)
        gkv = lax.psum(gkv, "tp")
        whole = lambda shape: block(shape, lambda b: (0,) * len(shape))
        g_key, g_value, g_mlp_norm, g_attn_norm = run(
            split_kernel, (1,), [whole((dim + extra, 2 * hd))], [whole((dim, hd))] * 2 + [whole((1, dim))] * 2,
            [sds((dim, hd), F32)] * 2 + [sds((1, dim), F32)] * 2, (gkv,), nbytes=16 * dim * hd)
        g_mlp_norm, g_attn_norm = g_mlp_norm.reshape(dim), g_attn_norm.reshape(dim)

        g_gate, g_up, hidden_out = weight_grads((full0[3], full1[3]), ((full0[1], full1[1]), (full0[2], full1[2])), (grad_hidden,),
                                                side=(resid.reshape(own, dim), part0.reshape(rows, dim), mlp_own, mlp_arrived))
        hidden_out = hidden_out.reshape(batch, sl, dim)
        return (hidden_out, grad_hidden, g_attn_norm, g_query_sum, g_key, g_value, g_out_sum, g_mlp_norm, g_gate, g_up, g_down)

    return jax.shard_map(local_layer, mesh=mesh, in_specs=in_specs, out_specs=out_specs, check_vma=False)
```
